32 devices in a mesh: dp: 8 (over z, x), fsdp: 4 (over y, core).
Axes of the slice: x: 2, y: 2, z: 4, core: 2. Of those that a mesh axis runs over, the one named last changes fastest.
Arguments:
- tokens: bfloat16 [16384, 768], P(('dp', 'fsdp')), may hold values from -6 to 6
- query_weight: bfloat16 [2, 768, 768], P(None, 'fsdp'), may hold values from -0.21875 to 0.21875
- key_weight: bfloat16 [2, 768, 768], P(None, 'fsdp'), may hold values from -0.21875 to 0.21875
- value_weight: bfloat16 [2, 768, 768], P(None, 'fsdp'), may hold values from -0.21875 to 0.21875
- projection: bfloat16 [2, 768, 768], P(None, 'fsdp'), may hold values from -1.75 to 1.75
- router_weight: bfloat16 [2, 768, 8], P(None, 'fsdp'), may hold values from -0.15625 to 0.15625
- attention_gain: bfloat16 [2, 768], P(None, 'fsdp'), may hold values from 0.5 to 1.5
- expert_gain: bfloat16 [2, 768], P(None, 'fsdp'), may hold values from 0.5 to 1.5
- position_bias: bfloat16 [2, 12, 32], P(None, 'fsdp'), may hold values from -4 to 4
- expert_up: bfloat16 [2, 8, 768, 3072], P(None, 'dp'), may hold values from -0.21875 to 0.21875
- expert_down: bfloat16 [2, 8, 3072, 768], P(None, 'dp'), may hold values from -0.15625 to 0.15625
- routes: int32 [16384, 2], P(('dp', 'fsdp')), may hold values from 0 to 7, all different within a row; in each aligned block of 512 rows (0 to 511, 512 to 1023, ...) at most 144 rows name the same one
- cotangent: bfloat16 [16384, 768], P(('dp', 'fsdp')), may hold values from -6 to 6
Outputs:
- output: bfloat16 [16384, 768], P(('dp', 'fsdp'))
- tokens_gradient: float32 [16384, 768], P(('dp', 'fsdp'))
- query_gradient: float32 [2, 768, 768], P(None, 'fsdp')
- key_gradient: float32 [2, 768, 768], P(None, 'fsdp')
- value_gradient: float32 [2, 768, 768], P(None, 'fsdp')
- projection_gradient: float32 [2, 768, 768], P(None, 'fsdp')
- router_gradient: float32 [2, 768, 8], P(None, 'fsdp')
- attention_gain_gradient: float32 [2, 768], P(None, 'fsdp')
- expert_gain_gradient: float32 [2, 768], P(None, 'fsdp')
- position_bias_gradient: float32 [2, 12, 32], P(None, 'fsdp')
- expert_up_gradient: float32 [2, 8, 768, 3072], P(None, 'dp', 'fsdp')
- expert_down_gradient: float32 [2, 8, 3072, 768], P(None, 'dp', 'fsdp')
The draws below stay inside these ranges and needn't reach their ends.
Inputs may be any that keep to these rules, and one draw needn't show every extreme that they name: `routes`: each row names 2 different experts. Within the rows of one device (aligned blocks of 512 rows) no expert is named by more than 144 rows, a bound that some block reaches.
All inputs are finite; a program needn't handle non-finite values.
Results may differ from the reference program's by a relative error of at most 0.025.
Values may be sent and summed in bfloat16 or wider, within the bound.
A program may use at most 256 MiB of HBM per device.

```python
import math
import jax
import jax.numpy as jnp
import numpy as np
from jax import lax

D = 768
HEADS = 12
HEAD = 64
FF = 3072
EXPERTS = 8
TOP = 2
LAYERS = 2
BLOCK = 256
NB = 32
QBLK = 512
TOK_DEV = 512
TOKENS = 16384
CAP = 144


def shard_levels(stream_key, dims, pieces, least, top_value):
    level = 1.0
    for axis_at, blocks in pieces:
        draws = jax.random.uniform(jax.random.fold_in(jax.random.fold_in(stream_key, 6), axis_at), (blocks,), jnp.float32, least / len(pieces), top_value / len(pieces))
        level = level * jnp.repeat(jnp.exp(draws), dims[axis_at] // blocks).reshape((-1,) + (1,) * (len(dims) - 1 - axis_at))
    return level


def assign_block(own_key, own, number, rows, amount, top, bound, slope):
    order = jax.random.permutation(own_key, amount)
    heavy_load, usual = load_shares(amount, rows * top, bound, slope, True), load_shares(amount, rows * top, bound, slope, False)
    places = jnp.arange(amount)

    def named(lengths, offset_by):
        used = int((lengths > 0).sum())
        fixed = max(1, used // 4)
        passed = fixed + (places - fixed + offset_by * (used - fixed)) % max(1, amount - fixed)
        return jnp.zeros((amount,), jnp.int32).at[order[jnp.where(places < fixed, places, passed)]].set(jnp.asarray(lengths, jnp.int32))

    lengths = jnp.where(number % 4 == 0, named(heavy_load, number // 4), named(usual, number - number // 4 - 1))
    mixed = jax.random.permutation(jax.random.fold_in(own, 3), amount)
    giver, taker = mixed[0:amount // 2 * 2:2], mixed[1:amount // 2 * 2:2]
    margin = jnp.minimum(lengths[giver] - 1, bound - lengths[taker]) // 2
    margin = jnp.where((giver == order[0]) | (taker == order[0]) | (lengths[taker] == 0), 0, jnp.maximum(margin, 0))
    passed = jax.random.randint(jax.random.fold_in(own, 4), (amount // 2,), 0, 1 << 20) % (margin + 1)
    lengths = lengths.at[giver].add(-passed).at[taker].add(passed)
    items = jnp.searchsorted(jnp.cumsum(lengths), jnp.arange(rows * top), side="right").astype(jnp.int32)
    grid = items.reshape(top, rows).T
    grid = grid[jax.random.permutation(jax.random.fold_in(own, 1), rows)]
    offset_by = jax.random.randint(jax.random.fold_in(own, 2), (rows, 1), 0, top)
    return jnp.take_along_axis(grid, (jnp.arange(top)[None, :] + offset_by) % top, axis=1)


def load_shares(count, total, reach, lean, full):
    loads = [(1 << 20) // math.isqrt(grade ** lean) + 1 for grade in range(1, count + 1)]
    largest = reach if full else min(reach, max(-(-total // count), total * loads[0] // sum(loads)))
    least = 1 if total - largest >= count - 1 else 0
    given, rest = [largest] + [least] * (count - 1), total - largest - least * (count - 1)
    while rest > 0:
        candidates = [i for i in range(1, count) if given[i] < largest] or [i for i in range(1, count) if given[i] < reach]
        pool, remaining = sum([loads[i] for i in candidates]), rest
        for i in candidates:
            extra = min(reach - given[i], max(1, remaining * loads[i] // pool), rest)
            given[i] = given[i] + extra
            rest = rest - extra
    return np.array(given)


def scatter_about(own_key, extent, width, limit, cuts=(), kind=jnp.bfloat16):
    entries = width * jax.random.normal(own_key, extent, jnp.float32)
    if cuts:
        entries = entries * shard_levels(own_key, extent, cuts, -0.22, 0.18)
    return jnp.clip(entries, -limit, limit).astype(kind)


def setup_inputs(seed: int = 0) -> dict:
    key_of = jax.random.split(jax.random.key(seed), 14)
    tokens = scatter_about(key_of[0], (TOKENS, D), 1.0, 6.0, ((0, 32),))
    query_weight = scatter_about(key_of[1], (LAYERS, D, D), D ** -0.5, 0.21875, ((1, 4),))
    key_weight = scatter_about(key_of[2], (LAYERS, D, D), D ** -0.5, 0.21875, ((1, 4),))
    value_weight = scatter_about(key_of[3], (LAYERS, D, D), D ** -0.5, 0.21875, ((1, 4),))
    projection = scatter_about(key_of[4], (LAYERS, D, D), (max(2, D // 64)) ** -0.5, 1.75, ((1, 4),))
    router_weight = scatter_about(key_of[5], (LAYERS, D, EXPERTS), (2 * D) ** -0.5, 0.15625, ((1, 4),))
    attention_gain = jnp.clip(1.0 + 0.1 * jax.random.normal(key_of[6], (LAYERS, D), jnp.float32), 0.5, 1.5).astype(jnp.bfloat16)
    expert_gain = jnp.clip(1.0 + 0.1 * jax.random.normal(key_of[7], (LAYERS, D), jnp.float32), 0.5, 1.5).astype(jnp.bfloat16)
    position_bias = scatter_about(key_of[8], (LAYERS, HEADS, NB), 1.0, 4.0, ((1, 4),))
    expert_up = scatter_about(key_of[9], (LAYERS, EXPERTS, D, FF), D ** -0.5, 0.21875, ((1, 8),))
    expert_down = scatter_about(key_of[10], (LAYERS, EXPERTS, FF, D), (FF // 2) ** -0.5, 0.15625, ((1, 8),))
    routes_keys = jax.random.split(jax.random.fold_in(key_of[11], 1), TOKENS // TOK_DEV)
    routes_turns = jax.random.permutation(jax.random.fold_in(key_of[11], 3), TOKENS // TOK_DEV)
    routes = jax.vmap(lambda own, number: assign_block(jax.random.fold_in(key_of[11], 2), own, number, TOK_DEV, EXPERTS, TOP, CAP, 1))(routes_keys, routes_turns).reshape((TOKENS, TOP))
    cotangent = scatter_about(key_of[12], (TOKENS, D), 1.0, 6.0, ((0, 32),))
    return {"tokens": tokens, "query_weight": query_weight, "key_weight": key_weight, "value_weight": value_weight, "projection": projection, "router_weight": router_weight, "attention_gain": attention_gain, "expert_gain": expert_gain, "position_bias": position_bias, "expert_up": expert_up, "expert_down": expert_down, "routes": routes, "cotangent": cotangent}


@jax.custom_vjp
def low(v):
    return lax.optimization_barrier(v.astype(jnp.bfloat16)).astype(jnp.float32)

@jax.custom_vjp
def low_back(v):
    return v

def low_keep(v):
    return (low(v), None)

def low_pass(kept, grad):
    return (grad,)

def back_keep(v):
    return (v, None)

def back_low(kept, grad):
    return (low(grad),)
low.defvjp(low_keep, low_pass)
low_back.defvjp(back_keep, back_low)
epsilon = 1e-06
edges = (1, 2, 3, 4, 5, 6, 7, 8, 12, 16, 24, 32, 64, 128, 256)
masked = -1000000000.0
highest = lax.Precision.HIGHEST

def norm_rows(values, gain):
    scale = lax.rsqrt(lax.optimization_barrier(jnp.mean(values * values, axis=-1, keepdims=True)) + epsilon)
    return values * scale * gain

def pair_layout(start, rows, length, block, buckets):
    queries = start + jnp.arange(rows, dtype=jnp.int32)
    places = jnp.arange(length, dtype=jnp.int32)
    offset = places[None, :] - queries[:, None]
    distance = jnp.abs(offset)
    bucket = jnp.zeros((rows, length), jnp.int32)
    for edge in edges:
        bucket = bucket + (distance >= edge).astype(jnp.int32)
    bucket = bucket + buckets // 2 * (offset > 0).astype(jnp.int32)
    allowed = places[None, :] // block <= queries[:, None] // block
    selector = (bucket[:, :, None] == jnp.arange(buckets, dtype=jnp.int32)[None, None, :]).astype(jnp.float32)
    return (selector, allowed)

def smooth_gate(values):
    return jax.nn.gelu(values, approximate=True)

def product(left, right):
    return jnp.dot(left, right, precision=highest, preferred_element_type=jnp.float32)

def attention(query, key, value, bias):
    sequences = TOKENS // TOK_DEV
    starts = jnp.arange(TOK_DEV // QBLK, dtype=jnp.int32) * QBLK
    scale = HEAD ** (-0.5)

    def one_sequence(parts):
        queries, keys, values = parts

        def one_block(start):
            rows = lax.dynamic_slice_in_dim(queries, start, QBLK, 0)
            selector, allowed = pair_layout(start, QBLK, TOK_DEV, BLOCK, NB)
            raw = low_back(jnp.einsum('qhe,khe->hqk', rows, keys, precision=highest))
            table = jnp.einsum('hb,qkb->hqk', bias, selector, precision=highest)
            scores = jnp.where(allowed[None, :, :], scale * raw + table, masked)
            shares = low(jax.nn.softmax(scores, axis=-1))
            return low(low_back(jnp.einsum('hqk,khe->qhe', shares, values, precision=highest)))
        return lax.map(jax.checkpoint(one_block), starts)
    shaped = (query.reshape(sequences, TOK_DEV, HEADS, HEAD), key.reshape(sequences, TOK_DEV, HEADS, HEAD), value.reshape(sequences, TOK_DEV, HEADS, HEAD))
    mixed = lax.map(one_sequence, shaped)
    return mixed.reshape(TOKENS, HEADS * HEAD)

def expert_tables(routes):
    devices = TOKENS // TOK_DEV
    flat = routes.reshape(devices, TOK_DEV * TOP)
    selector = flat[:, :, None] == jnp.arange(EXPERTS, dtype=jnp.int32)[None, None, :]
    running = jnp.cumsum(selector.astype(jnp.int32), axis=1)
    rank = lax.optimization_barrier(jnp.sum(jnp.where(selector, running, 0), axis=2)) - 1
    slot = jnp.arange(devices, dtype=jnp.int32)[:, None] * CAP + rank
    assign = jnp.arange(devices * TOK_DEV * TOP, dtype=jnp.int32).reshape(devices, TOK_DEV * TOP)
    anchor = jnp.zeros((EXPERTS, devices * CAP), jnp.int32).at[flat, slot].set(assign)
    filled = jnp.zeros((EXPERTS, devices * CAP), jnp.float32).at[flat, slot].set(1.0)
    return (anchor, filled, flat.reshape(-1), slot.reshape(-1))

def expert_apply(parts):
    rows, up_matrix, down_matrix = parts
    inner = low_back(product(rows, up_matrix))
    activity = low(smooth_gate(inner))
    return low(low_back(product(activity, down_matrix)))

def forward(tokens, query_weight, key_weight, value_weight, projection, router_weight, attention_gain, expert_gain, position_bias, expert_up, expert_down, routes, tables):
    anchor, filled, flat_expert, slot = tables
    route_select = routes[:, :, None] == jnp.arange(EXPERTS, dtype=jnp.int32)[None, None, :]
    hidden = tokens
    for layer in range(LAYERS):
        normed = low(norm_rows(hidden, attention_gain[layer]))
        query = low(low_back(product(normed, query_weight[layer])))
        key = low(low_back(product(normed, key_weight[layer])))
        value = low(low_back(product(normed, value_weight[layer])))
        mixed = attention(query, key, value, position_bias[layer])
        hidden = hidden + low_back(product(mixed, projection[layer]))
        normed = low(norm_rows(hidden, expert_gain[layer]))
        logits = low_back(product(normed, router_weight[layer]))
        picked = lax.optimization_barrier(jnp.sum(jnp.where(route_select, logits[:, None, :], 0.0), axis=-1))
        gates = jax.nn.softmax(picked, axis=-1)
        rows = low_back(normed[anchor // TOP]) * filled[:, :, None]
        results = lax.map(jax.checkpoint(expert_apply), (rows, expert_up[layer], expert_down[layer]))
        routed = results[flat_expert, slot].reshape(TOKENS, TOP, HEADS * HEAD)
        hidden = hidden + lax.optimization_barrier(jnp.sum(gates[:, :, None] * routed, axis=1))
    return hidden

def reference(tokens, query_weight, key_weight, value_weight, projection, router_weight, attention_gain, expert_gain, position_bias, expert_up, expert_down, routes, cotangent):
    tables = expert_tables(routes)
    primals = tuple((item.astype(jnp.float32) for item in (tokens, query_weight, key_weight, value_weight, projection, router_weight, attention_gain, expert_gain, position_bias, expert_up, expert_down)))

    def run(*values):
        return forward(*values, routes, tables)
    result, pullback = jax.vjp(run, *primals)
    changes = pullback(cotangent.astype(jnp.float32))
    return (result.astype(jnp.bfloat16), changes[0], changes[1], changes[2], changes[3], changes[4], changes[5], changes[6], changes[7], changes[8], changes[9], changes[10])
```

```python
import functools

import jax
import jax.numpy as jnp
from jax import lax
from jax.experimental import pallas as pl
from jax.experimental.pallas import tpu as pltpu
from jax.sharding import PartitionSpec as P

EXP_DEV = 1
TOP = 2
BLOCK = 256
NB = 32
LANES = 128


epsilon = 1e-06
edges = (1, 2, 3, 4, 5, 6, 7, 8, 12, 16, 24, 32, 64, 128, 256)
highest = lax.Precision.HIGHEST
contract_first = (((0,), (0,)), ((), ()))
contract_last = (((1,), (1,)), ((), ()))
root = 0.7978845608028654
cubic = 0.044715


def dot(left, right):
    return jnp.dot(left, right, preferred_element_type=jnp.float32)


def dot_last(left, right):
    return lax.dot_general(left, right, contract_last, preferred_element_type=jnp.float32)


def dot_first(left, right):
    return lax.dot_general(left, right, contract_first, preferred_element_type=jnp.float32)


def low(values):
    return values.astype(jnp.bfloat16)


def row_scale(values):
    return lax.rsqrt(jnp.mean(values * values, axis=-1, keepdims=True) + epsilon)


def norm_back(values, scale, gain, back):
    lifted = back * gain
    inner = jnp.mean(lifted * values, axis=-1, keepdims=True)
    rows = scale * lifted - scale * scale * scale * values * inner
    return rows, jnp.sum(back * values * scale, axis=0)


def smooth_pair(values):
    tail = jnp.tanh(root * (values + cubic * values * values * values))
    half = 0.5 * (1.0 + tail)
    slope = half + 0.5 * values * (1.0 - tail * tail) * root * (1.0 + 3.0 * cubic * values * values)
    return values * half, slope


def offset_selector(length):
    offset = jnp.arange(2 * length, dtype=jnp.int32) - (length - 1)
    distance = jnp.abs(offset)
    bucket = jnp.zeros_like(offset)
    for edge in edges:
        bucket = bucket + (distance >= edge).astype(jnp.int32)
    bucket = bucket + NB // 2 * (offset > 0).astype(jnp.int32)
    return (bucket[:, None] == jnp.arange(NB, dtype=jnp.int32)[None, :]).astype(jnp.float32)


def lane_of(half, heads):
    lanes = lax.broadcasted_iota(jnp.int32, (1, LANES), 1)
    size = LANES // heads
    return (lanes >= half * size) & (lanes < (half + 1) * size)


def bias_tile(table, start, block, keys):
    span = table.shape[1]
    length = span // 2
    spread = jnp.broadcast_to(table, (block, span))
    shift = (start - (length - 1)) % span
    return pltpu.roll(spread, shift, 1, stride=1, stride_axis=0)[:, :keys]


def attend(pair, scale, q_ref, k_ref, v_ref, table_ref, mixed_ref, log_ref):
    length = q_ref.shape[0]
    for start in range(0, length, BLOCK):
        keys = start + BLOCK
        rows = pl.ds(start, BLOCK)
        query = q_ref[rows, :]
        key = k_ref[pl.ds(0, keys), :]
        value = v_ref[pl.ds(0, keys), :]
        mixed = None
        for half in range(pair):
            lane = lane_of(half, pair)
            table = table_ref[0, half : half + 1, :]
            raw = dot_last(jnp.where(lane, query, jnp.zeros_like(query)), key)
            scores = scale * raw + bias_tile(table, start, BLOCK, keys)
            peak = jnp.max(scores, axis=-1, keepdims=True)
            lifted = jnp.exp(scores - peak)
            total = jnp.sum(lifted, axis=-1, keepdims=True)
            shares = low(lifted * (1.0 / total))
            part = dot(shares, value)
            tops = jnp.broadcast_to(peak + jnp.log(total), part.shape)
            mixed = part if mixed is None else jnp.where(lane, part, mixed)
            logs = tops if half == 0 else jnp.where(lane, tops, logs)
        mixed_ref[rows, :] = low(mixed)
        log_ref[rows, :] = logs


def attend_back(
    pair,
    scale,
    q_ref,
    k_ref,
    v_ref,
    table_ref,
    log_ref,
    back_ref,
    dq_ref,
    dk_ref,
    dv_ref,
    sums_ref,
    key_sum,
    value_sum,
):
    length = q_ref.shape[0]
    size = LANES // pair
    span = 2 * length
    order = list(range(0, length, BLOCK))[::-1]
    for turn, start in enumerate(order):
        keys = start + BLOCK
        rows = pl.ds(start, BLOCK)
        query = q_ref[rows, :]
        back = back_ref[rows, :]
        key = k_ref[pl.ds(0, keys), :]
        value = v_ref[pl.ds(0, keys), :]
        back_query = None
        for half in range(pair):
            lane = lane_of(half, pair)
            table = table_ref[0, half : half + 1, :]
            query_half = jnp.where(lane, query, jnp.zeros_like(query))
            back_half = jnp.where(lane, back, jnp.zeros_like(back))
            raw = dot_last(query_half, key)
            scores = scale * raw + bias_tile(table, start, BLOCK, keys)
            shares = jnp.exp(scores - log_ref[rows, half * size : half * size + 1])
            back_shares = dot_last(back_half, value)
            weighted = shares * back_shares
            back_scores = weighted - shares * jnp.sum(weighted, axis=-1, keepdims=True)
            back_raw = low(scale * back_scores)
            part = dot(back_raw, key)
            back_query = part if back_query is None else jnp.where(lane, part, back_query)
            key_part = dot_first(back_raw, query_half)
            value_part = dot_first(low(shares), back_half)
            if turn == 0 and half == 0:
                key_sum[pl.ds(0, keys), :] = key_part
                value_sum[pl.ds(0, keys), :] = value_part
            else:
                key_sum[pl.ds(0, keys), :] += key_part
                value_sum[pl.ds(0, keys), :] += value_part
            first = length - 1 - start
            lines = jnp.zeros((8, span), jnp.float32)
            wide = jnp.concatenate(
                [back_scores, jnp.zeros((BLOCK, span - keys), jnp.float32)], axis=1
            )
            for tile in range(BLOCK // 8):
                piece = wide[tile * 8 : tile * 8 + 8, :]
                lines = lines + pltpu.roll(piece, (first - tile * 8) % span, 1)
            line = lines[0:1, :]
            for step in range(1, 8):
                line = line + pltpu.roll(lines[step : step + 1, :], span - step, 1)
            if turn == 0:
                sums_ref[0, half : half + 1, :] = line
            else:
                sums_ref[0, half : half + 1, :] += line
        dq_ref[rows, :] = low(back_query)
    dk_ref[...] = low(key_sum[...])
    dv_ref[...] = low(value_sum[...])


def attention_specs(length, heads, size):
    pair = LANES // size
    groups = heads // pair

    def column(offset):
        return pl.BlockSpec((length, LANES), lambda g: (0, g + offset))

    table = pl.BlockSpec((1, pair, 2 * length), lambda g: (g, 0, 0))
    return pair, groups, column, table


def attention_forward(joined, table, heads):
    length, width = joined.shape[0], joined.shape[1] // 3
    size = width // heads
    pair, groups, column, table_spec = attention_specs(length, heads, size)
    return pl.pallas_call(
        functools.partial(attend, pair, size**-0.5),
        grid=(groups,),
        out_shape=(
            jax.ShapeDtypeStruct((length, width), jnp.bfloat16),
            jax.ShapeDtypeStruct((length, width), jnp.float32),
        ),
        in_specs=[column(0), column(groups), column(2 * groups), table_spec],
        out_specs=(column(0), column(0)),
        compiler_params=pltpu.CompilerParams(vmem_limit_bytes=32 << 20),
        cost_estimate=pl.CostEstimate(
            flops=4 * length * length * width,
            bytes_accessed=length * width * 12,
            transcendentals=length * length * heads,
        ),
        name="attend",
    )(joined, joined, joined, table.reshape(groups, pair, 2 * length))


def attention_backward(joined, table, log_total, back_mixed, heads):
    length, width = back_mixed.shape
    size = width // heads
    pair, groups, column, table_spec = attention_specs(length, heads, size)
    rows = jax.ShapeDtypeStruct((length, width), jnp.bfloat16)
    back_query, back_key, back_value, sums = pl.pallas_call(
        functools.partial(attend_back, pair, size**-0.5),
        grid=(groups,),
        out_shape=(
            rows,
            rows,
            rows,
            jax.ShapeDtypeStruct((groups, pair, 2 * length), jnp.float32),
        ),
        in_specs=[
            column(0),
            column(groups),
            column(2 * groups),
            table_spec,
            column(0),
            column(0),
        ],
        out_specs=(column(0), column(0), column(0), table_spec),
        scratch_shapes=[pltpu.VMEM((length, LANES), jnp.float32)] * 2,
        compiler_params=pltpu.CompilerParams(vmem_limit_bytes=32 << 20),
        cost_estimate=pl.CostEstimate(
            flops=10 * length * length * width,
            bytes_accessed=length * width * 20,
            transcendentals=length * length * heads,
        ),
        name="attend_back",
    )(joined, joined, joined, table.reshape(groups, pair, 2 * length), log_total, back_mixed)
    return back_query, back_key, back_value, sums.reshape(heads, 2 * length)


def plan_routes(routes, experts, capacity):
    length = routes.shape[0]
    flat = routes.reshape(-1)
    selector = flat[:, None] == jnp.arange(experts, dtype=jnp.int32)[None, :]
    running = jnp.cumsum(selector.astype(jnp.int32), axis=0)
    rank = jnp.sum(jnp.where(selector, running, 0), axis=1) - 1
    slot = (flat * capacity + rank).reshape(length, TOP).T.reshape(-1)
    place = jnp.arange(experts * capacity, dtype=jnp.int32)
    taken = slot[None, :] == place[:, None]
    pick = low(taken)
    both = sum(pick[:, choice * length : (choice + 1) * length] for choice in range(TOP))
    chosen = routes[:, :, None] == jnp.arange(experts, dtype=jnp.int32)[None, None, :]
    return taken, pick, both, chosen


def exchange(values):
    return lax.all_to_all(values, "dp", split_axis=0, concat_axis=0, tiled=True)


def exchange_rows(values, experts):
    rows, width = values.shape
    return exchange(values.reshape(experts, rows // experts, width)).reshape(rows, width)


def exchange_numbers(values, experts):
    return exchange(values.reshape(experts, 1, -1)).reshape(-1)


def pack_small(router, attention_gain, expert_gain, bias):
    rows = router.shape[0]
    flat = bias.reshape(-1)
    column = jnp.concatenate([flat, jnp.zeros((rows - flat.shape[0],), flat.dtype)])
    block = jnp.concatenate(
        [router, attention_gain[:, None], expert_gain[:, None], column[:, None]], axis=1
    )
    return jnp.pad(block, ((0, 0), (0, -block.shape[1] % LANES)))


def unpack_small(block, experts, shards, heads):
    router = block[:, :experts]
    attention_gain = block[:, experts]
    expert_gain = block[:, experts + 1]
    column = block[:, experts + 2].reshape(shards, -1)
    bias = column[:, : heads // shards * NB].reshape(heads, NB)
    return router, attention_gain, expert_gain, bias


def per_device(
    tokens,
    query_weight,
    key_weight,
    value_weight,
    projection,
    router_weight,
    attention_gain,
    expert_gain,
    position_bias,
    expert_up,
    expert_down,
    routes,
    cotangent,
):
    layers = query_weight.shape[0]
    length, width = tokens.shape
    shards = lax.axis_size("fsdp")
    owners = lax.axis_size("dp")
    experts = owners * EXP_DEV
    heads = position_bias.shape[1] * shards
    capacity = max(2, 9 * length * TOP // (8 * experts))
    taken, pick, both, chosen = plan_routes(routes, experts, capacity)
    offsets = offset_selector(length)

    mixers = []
    for layer in range(layers):
        small = pack_small(
            router_weight[layer], attention_gain[layer], expert_gain[layer], position_bias[layer]
        )
        first = jnp.concatenate(
            [query_weight[layer], key_weight[layer], value_weight[layer], small], axis=1
        )
        first = lax.all_gather(first, "fsdp", axis=0, tiled=True)
        second = lax.all_gather(projection[layer], "fsdp", axis=0, tiled=True)
        router, gain_attention, gain_expert, bias = unpack_small(
            first[:, 3 * width :], experts, shards, heads
        )
        table = lax.dot_general(
            bias.astype(jnp.float32), offsets, contract_last, precision=highest
        )
        mixers.append(
            (
                first[:, : 3 * width],
                second,
                router,
                gain_attention.astype(jnp.float32),
                gain_expert.astype(jnp.float32),
                table,
            )
        )

    early = exchange_rows(low(dot(both, cotangent)), experts)

    hidden = tokens.astype(jnp.float32)
    saved = []
    for layer in range(layers):
        joined_weight, projection_full, router, gain_attention, gain_expert, table = mixers[layer]
        up_matrix, down_matrix = expert_up[layer, 0], expert_down[layer, 0]
        scale = row_scale(hidden)
        normed = low(hidden * scale * gain_attention)
        joined = low(dot(normed, joined_weight))
        mixed, log_total = attention_forward(joined, table, heads)
        middle = hidden + dot(mixed, projection_full)
        scale_expert = row_scale(middle)
        normed_expert = low(middle * scale_expert * gain_expert)
        logits = dot(normed_expert, router)
        picked = jnp.sum(jnp.where(chosen, logits[:, None, :], 0.0), axis=-1)
        gates = jax.nn.softmax(picked, axis=-1)
        gate_line = gates.T.reshape(-1)
        received = exchange_rows(low(dot(both, normed_expert)), experts)
        inner = dot(received, up_matrix)
        activity, slope = smooth_pair(inner)
        activity = low(activity)
        result = low(dot(activity, down_matrix))
        if layer == layers - 1:
            gate_places = exchange_numbers(
                jnp.sum(jnp.where(taken, gate_line[None, :], 0.0), axis=1), experts
            )
            back_places = jnp.sum(early.astype(jnp.float32) * result.astype(jnp.float32), axis=1)
            back_places = exchange_numbers(back_places, experts)
            back_sent = low(gate_places[:, None] * early.astype(jnp.float32))
            back_inner = low(dot_last(back_sent, down_matrix) * slope)
            back_rows = exchange_rows(low(dot_last(back_inner, up_matrix)), experts)
            last = (back_places, back_sent, back_inner, back_rows)
        returned = exchange_rows(result, experts)
        routed = low(dot_first(pick, returned)).reshape(TOP, length, width)
        update = sum(
            gates[:, choice : choice + 1] * routed[choice].astype(jnp.float32)
            for choice in range(TOP)
        )
        saved.append(
            (
                hidden,
                scale,
                normed,
                joined,
                mixed,
                log_total,
                middle,
                scale_expert,
                normed_expert,
                gates,
                received,
                activity,
                slope,
                routed,
            )
        )
        hidden = middle + update
    output = low(hidden)

    back_out = cotangent.astype(jnp.float32)
    mixer_results = [None] * layers
    expert_results = [None] * layers
    for layer in range(layers - 1, -1, -1):
        joined_weight, projection_full, router, gain_attention, gain_expert, table = mixers[layer]
        up_matrix, down_matrix = expert_up[layer, 0], expert_down[layer, 0]
        (
            hidden,
            scale,
            normed,
            joined,
            mixed,
            log_total,
            middle,
            scale_expert,
            normed_expert,
            gates,
            received,
            activity,
            slope,
            routed,
        ) = saved[layer]
        if layer == layers - 1:
            back_places, back_sent, back_inner, back_rows = last
            back_gates = jnp.sum(jnp.where(taken, back_places[:, None], 0.0), axis=0)
            back_gates = back_gates.reshape(TOP, length).T
        else:
            back_gates = jnp.stack(
                [
                    jnp.sum(back_out * routed[choice].astype(jnp.float32), axis=-1)
                    for choice in range(TOP)
                ],
                axis=1,
            )
            gated = jnp.concatenate(
                [low(gates[:, choice : choice + 1] * back_out) for choice in range(TOP)], axis=0
            )
            back_sent = exchange_rows(low(dot(pick, gated)), experts)
            back_inner = low(dot_last(back_sent, down_matrix) * slope)
            back_rows = exchange_rows(low(dot_last(back_inner, up_matrix)), experts)
        down_change = dot_first(activity, back_sent)
        up_change = dot_first(received, back_inner)
        expert_results[layer] = tuple(
            lax.psum_scatter(low(change), "fsdp", scatter_dimension=0, tiled=True).astype(
                jnp.float32
            )
            for change in (up_change, down_change)
        )
        back_picked = gates * (back_gates - jnp.sum(gates * back_gates, axis=-1, keepdims=True))
        back_logits = low(jnp.sum(jnp.where(chosen, back_picked[:, :, None], 0.0), axis=1))
        router_change = dot_first(normed_expert, back_logits)
        back_expert = dot_first(both, back_rows) + dot_last(back_logits, router)
        rows, expert_gain_change = norm_back(middle, scale_expert, gain_expert, back_expert)
        back_middle = back_out + rows
        back_attended = low(back_middle)
        back_mixed = low(dot_last(back_attended, projection_full))
        back_query, back_key, back_value, sums = attention_backward(
            joined, table, log_total, back_mixed, heads
        )
        bias_change = jnp.dot(sums, offsets, precision=highest)
        projection_change = dot_first(mixed, back_attended)
        parts = (back_query, back_key, back_value)
        changes = [low(dot_first(normed, part)) for part in parts]
        back_normed = sum(
            dot_last(part, joined_weight[:, index * width : (index + 1) * width])
            for index, part in enumerate(parts)
        )
        rows, attention_gain_change = norm_back(hidden, scale, gain_attention, back_normed)
        back_out = back_middle + rows
        column = jnp.pad(
            bias_change.reshape(shards, -1), ((0, 0), (0, (width - heads * NB) // shards))
        ).reshape(-1)
        small = jnp.concatenate(
            [
                router_change,
                attention_gain_change[:, None],
                expert_gain_change[:, None],
                column[:, None],
            ],
            axis=1,
        )
        small = jnp.pad(small, ((0, 0), (0, -small.shape[1] % LANES)))
        packed = jnp.concatenate(changes + [low(projection_change), low(small)], axis=1)
        shard = lax.psum_scatter(packed, "fsdp", scatter_dimension=0, tiled=True)
        mixer_results[layer] = lax.psum(shard, "dp").astype(jnp.float32)

    stacked = jnp.stack(mixer_results)
    router_gradient = stacked[:, :, 4 * width : 4 * width + experts]
    tail = 4 * width + experts
    bias_gradient = stacked[:, : position_bias.shape[1] * NB, tail + 2].reshape(
        position_bias.shape
    )
    up_stack = jnp.stack([expert_results[layer][0] for layer in range(layers)])[:, None]
    down_stack = jnp.stack([expert_results[layer][1] for layer in range(layers)])[:, None]
    return (
        output,
        back_out,
        stacked[:, :, :width],
        stacked[:, :, width : 2 * width],
        stacked[:, :, 2 * width : 3 * width],
        stacked[:, :, 3 * width : 4 * width],
        router_gradient,
        stacked[:, :, tail],
        stacked[:, :, tail + 1],
        bias_gradient,
        up_stack,
        down_stack,
    )


def solution(mesh):
    return jax.shard_map(
        per_device,
        mesh=mesh,
        in_specs=(
            P(("dp", "fsdp"), None),
            P(None, "fsdp", None),
            P(None, "fsdp", None),
            P(None, "fsdp", None),
            P(None, "fsdp", None),
            P(None, "fsdp", None),
            P(None, "fsdp"),
            P(None, "fsdp"),
            P(None, "fsdp", None),
            P(None, "dp", None, None),
            P(None, "dp", None, None),
            P(("dp", "fsdp"), None),
            P(("dp", "fsdp"), None),
        ),
        out_specs=(
            P(("dp", "fsdp"), None),
            P(("dp", "fsdp"), None),
            P(None, "fsdp", None),
            P(None, "fsdp", None),
            P(None, "fsdp", None),
            P(None, "fsdp", None),
            P(None, "fsdp", None),
            P(None, "fsdp"),
            P(None, "fsdp"),
            P(None, "fsdp", None),
            P(None, "dp", "fsdp", None),
            P(None, "dp", "fsdp", None),
        ),
        check_vma=False,
    )
```

```python
import functools

import jax
import jax.numpy as jnp
from jax import lax
from jax.experimental import pallas as pl
from jax.experimental.pallas import tpu as pltpu
from jax.sharding import PartitionSpec as P

EXP_DEV = 1
TOP = 2
BLOCK = 256
NB = 32
LANES = 128


epsilon = 1e-06
edges = (1, 2, 3, 4, 5, 6, 7, 8, 12, 16, 24, 32, 64, 128, 256)
highest = lax.Precision.HIGHEST
contract_first = (((0,), (0,)), ((), ()))
contract_last = (((1,), (1,)), ((), ()))
root = 0.7978845608028654
cubic = 0.044715


def dot(left, right):
    return jnp.dot(left, right, preferred_element_type=jnp.float32)


def dot_last(left, right):
    return lax.dot_general(left, right, contract_last, preferred_element_type=jnp.float32)


def dot_first(left, right):
    return lax.dot_general(left, right, contract_first, preferred_element_type=jnp.float32)


def low(values):
    return values.astype(jnp.bfloat16)


def row_scale(values):
    return lax.rsqrt(jnp.mean(values * values, axis=-1, keepdims=True) + epsilon)


def norm_back(values, scale, gain, back):
    lifted = back * gain
    inner = jnp.mean(lifted * values, axis=-1, keepdims=True)
    rows = scale * lifted - scale * scale * scale * values * inner
    return rows, jnp.sum(back * values * scale, axis=0)


def smooth_pair(values):
    tail = jnp.tanh(root * (values + cubic * values * values * values))
    half = 0.5 * (1.0 + tail)
    slope = half + 0.5 * values * (1.0 - tail * tail) * root * (1.0 + 3.0 * cubic * values * values)
    return values * half, slope


def offset_selector(length):
    offset = jnp.arange(2 * length, dtype=jnp.int32) - (length - 1)
    distance = jnp.abs(offset)
    bucket = jnp.zeros_like(offset)
    for edge in edges:
        bucket = bucket + (distance >= edge).astype(jnp.int32)
    bucket = bucket + NB // 2 * (offset > 0).astype(jnp.int32)
    return (bucket[:, None] == jnp.arange(NB, dtype=jnp.int32)[None, :]).astype(jnp.float32)


def lane_of(half, heads):
    lanes = lax.broadcasted_iota(jnp.int32, (1, LANES), 1)
    size = LANES // heads
    return (lanes >= half * size) & (lanes < (half + 1) * size)


def bias_tile(table, start, block, keys):
    span = table.shape[1]
    length = span // 2
    spread = jnp.broadcast_to(table, (block, span))
    shift = (start - (length - 1)) % span
    return pltpu.roll(spread, shift, 1, stride=1, stride_axis=0)[:, :keys]


def attend(pair, scale, q_ref, k_ref, v_ref, table_ref, mixed_ref, log_ref):
    length = q_ref.shape[0]
    for start in range(0, length, BLOCK):
        keys = start + BLOCK
        rows = pl.ds(start, BLOCK)
        query = q_ref[rows, :]
        key = k_ref[pl.ds(0, keys), :]
        value = v_ref[pl.ds(0, keys), :]
        mixed = None
        for half in range(pair):
            lane = lane_of(half, pair)
            table = table_ref[0, half : half + 1, :]
            raw = dot_last(jnp.where(lane, query, jnp.zeros_like(query)), key)
            scores = scale * raw + bias_tile(table, start, BLOCK, keys)
            peak = jnp.max(scores, axis=-1, keepdims=True)
            lifted = jnp.exp(scores - peak)
            total = jnp.sum(lifted, axis=-1, keepdims=True)
            shares = low(lifted * (1.0 / total))
            part = dot(shares, value)
            tops = jnp.broadcast_to(peak + jnp.log(total), part.shape)
            mixed = part if mixed is None else jnp.where(lane, part, mixed)
            logs = tops if half == 0 else jnp.where(lane, tops, logs)
        mixed_ref[rows, :] = low(mixed)
        log_ref[rows, :] = logs


def attend_back(
    pair,
    scale,
    q_ref,
    k_ref,
    v_ref,
    table_ref,
    log_ref,
    back_ref,
    dq_ref,
    dk_ref,
    dv_ref,
    sums_ref,
    key_sum,
    value_sum,
):
    length = q_ref.shape[0]
    size = LANES // pair
    span = 2 * length
    order = list(range(0, length, BLOCK))[::-1]
    for turn, start in enumerate(order):
        keys = start + BLOCK
        rows = pl.ds(start, BLOCK)
        query = q_ref[rows, :]
        back = back_ref[rows, :]
        key = k_ref[pl.ds(0, keys), :]
        value = v_ref[pl.ds(0, keys), :]
        back_query = None
        for half in range(pair):
            lane = lane_of(half, pair)
            table = table_ref[0, half : half + 1, :]
            query_half = jnp.where(lane, query, jnp.zeros_like(query))
            back_half = jnp.where(lane, back, jnp.zeros_like(back))
            raw = dot_last(query_half, key)
            scores = scale * raw + bias_tile(table, start, BLOCK, keys)
            shares = jnp.exp(scores - log_ref[rows, half * size : half * size + 1])
            back_shares = dot_last(back_half, value)
            weighted = shares * back_shares
            back_scores = weighted - shares * jnp.sum(weighted, axis=-1, keepdims=True)
            back_raw = low(scale * back_scores)
            part = dot(back_raw, key)
            back_query = part if back_query is None else jnp.where(lane, part, back_query)
            key_part = dot_first(back_raw, query_half)
            value_part = dot_first(low(shares), back_half)
            if turn == 0 and half == 0:
                key_sum[pl.ds(0, keys), :] = key_part
                value_sum[pl.ds(0, keys), :] = value_part
            else:
                key_sum[pl.ds(0, keys), :] += key_part
                value_sum[pl.ds(0, keys), :] += value_part
            first = length - 1 - start
            lines = jnp.zeros((8, span), jnp.float32)
            wide = jnp.concatenate(
                [back_scores, jnp.zeros((BLOCK, span - keys), jnp.float32)], axis=1
            )
            for tile in range(BLOCK // 8):
                piece = wide[tile * 8 : tile * 8 + 8, :]
                lines = lines + pltpu.roll(piece, (first - tile * 8) % span, 1)
            line = lines[0:1, :]
            for step in range(1, 8):
                line = line + pltpu.roll(lines[step : step + 1, :], span - step, 1)
            if turn == 0:
                sums_ref[0, half : half + 1, :] = line
            else:
                sums_ref[0, half : half + 1, :] += line
        dq_ref[rows, :] = low(back_query)
    dk_ref[...] = low(key_sum[...])
    dv_ref[...] = low(value_sum[...])


def attention_specs(length, heads, size):
    pair = LANES // size
    groups = heads // pair

    def column(offset):
        return pl.BlockSpec((length, LANES), lambda g: (0, g + offset))

    table = pl.BlockSpec((1, pair, 2 * length), lambda g: (g, 0, 0))
    return pair, groups, column, table


def attention_forward(joined, table, heads):
    length, width = joined.shape[0], joined.shape[1] // 3
    size = width // heads
    pair, groups, column, table_spec = attention_specs(length, heads, size)
    return pl.pallas_call(
        functools.partial(attend, pair, size**-0.5),
        grid=(groups,),
        out_shape=(
            jax.ShapeDtypeStruct((length, width), jnp.bfloat16),
            jax.ShapeDtypeStruct((length, width), jnp.float32),
        ),
        in_specs=[column(0), column(groups), column(2 * groups), table_spec],
        out_specs=(column(0), column(0)),
        compiler_params=pltpu.CompilerParams(vmem_limit_bytes=32 << 20),
        cost_estimate=pl.CostEstimate(
            flops=4 * length * length * width,
            bytes_accessed=length * width * 12,
            transcendentals=length * length * heads,
        ),
        name="attend",
    )(joined, joined, joined, table.reshape(groups, pair, 2 * length))


def attention_backward(joined, table, log_total, back_mixed, heads):
    length, width = back_mixed.shape
    size = width // heads
    pair, groups, column, table_spec = attention_specs(length, heads, size)
    rows = jax.ShapeDtypeStruct((length, width), jnp.bfloat16)
    back_query, back_key, back_value, sums = pl.pallas_call(
        functools.partial(attend_back, pair, size**-0.5),
        grid=(groups,),
        out_shape=(
            rows,
            rows,
            rows,
            jax.ShapeDtypeStruct((groups, pair, 2 * length), jnp.float32),
        ),
        in_specs=[
            column(0),
            column(groups),
            column(2 * groups),
            table_spec,
            column(0),
            column(0),
        ],
        out_specs=(column(0), column(0), column(0), table_spec),
        scratch_shapes=[pltpu.VMEM((length, LANES), jnp.float32)] * 2,
        compiler_params=pltpu.CompilerParams(vmem_limit_bytes=32 << 20),
        cost_estimate=pl.CostEstimate(
            flops=10 * length * length * width,
            bytes_accessed=length * width * 20,
            transcendentals=length * length * heads,
        ),
        name="attend_back",
    )(joined, joined, joined, table.reshape(groups, pair, 2 * length), log_total, back_mixed)
    return back_query, back_key, back_value, sums.reshape(heads, 2 * length)


def mesh_copy(source, target, sends, receives, where, device):
    return pltpu.make_async_remote_copy(
        src_ref=source,
        dst_ref=target,
        send_sem=sends.at[where],
        recv_sem=receives.at[where],
        device_id=device,
        device_id_type=pl.DeviceIdType.MESH,
    )


def reduce_mixer(
    owners,
    chunks,
    q_ref,
    k_ref,
    v_ref,
    p_ref,
    small_ref,
    out_ref,
    core_in,
    side_out,
    side_in,
    keep,
    owner_in,
    small_in,
    part,
    whole_in,
    core_send,
    core_recv,
    side_send,
    side_recv,
    owner_send,
    owner_recv,
    small_send,
    small_recv,
    whole_send,
    whole_recv,
):
    me = lax.axis_index("dp")
    place = lax.axis_index("fsdp")
    core, side = lax.rem(place, 2), place // 2
    partner = 2 * side + (1 - core)
    across = 2 * (1 - side) + core
    refs = (q_ref, k_ref, v_ref, p_ref, small_ref)
    rows = q_ref.shape[1]
    spare = small_ref.shape[1]
    main = 4 * rows
    block = main // owners
    columns = q_ref.shape[2] // chunks
    spans = [(index * rows, ref.shape[1]) for index, ref in enumerate(refs)]

    barrier = pltpu.get_barrier_semaphore()
    for other in (partner, across):
        pl.semaphore_signal(
            barrier, inc=1, device_id={"fsdp": other}, device_id_type=pl.DeviceIdType.MESH
        )
    for step in range(1, owners):
        pl.semaphore_signal(
            barrier,
            inc=1,
            device_id={"dp": lax.rem(me + step, owners)},
            device_id_type=pl.DeviceIdType.MESH,
        )
    pl.semaphore_wait(barrier, owners + 1)

    waits = []
    core_copies = [[] for _ in range(chunks)]
    for chunk in range(chunks):
        lanes = pl.ds(chunk * columns, columns)
        for turn in range(2):
            there = 1 - side if turn == 0 else side
            for index, (start, count) in enumerate(spans):
                copy = mesh_copy(
                    refs[index].at[2 * there + 1 - core, :, lanes],
                    core_in.at[turn, pl.ds(start, count), lanes],
                    core_send,
                    core_recv,
                    (chunk * 2 + turn) * 5 + index,
                    {"fsdp": partner},
                )
                copy.start()
                core_copies[chunk].append(copy)

    side_copies = []
    for chunk in range(chunks):
        lanes = pl.ds(chunk * columns, columns)
        for copy in core_copies[chunk]:
            copy.wait()
        for turn in range(2):
            there = 1 - side if turn == 0 else side
            target = side_out if turn == 0 else keep
            for index, (start, count) in enumerate(spans):
                at = pl.ds(start, count)
                total = refs[index][2 * there + core, :, lanes].astype(jnp.float32)
                total = total + core_in[turn, at, lanes].astype(jnp.float32)
                target[at, lanes] = low(total)
            if turn == 0:
                copy = mesh_copy(
                    side_out.at[:, lanes],
                    side_in.at[:, lanes],
                    side_send,
                    side_recv,
                    chunk,
                    {"fsdp": across},
                )
                copy.start()
                side_copies.append(copy)

    owner_copies = []
    for chunk in range(chunks):
        lanes = pl.ds(chunk * columns, columns)
        side_copies[chunk].wait()
        keep[:, lanes] = low(
            keep[:, lanes].astype(jnp.float32) + side_in[:, lanes].astype(jnp.float32)
        )
        copies = []
        for step in range(1, owners):
            other = lax.rem(me + step, owners)
            where = chunk * owners + step
            at = pl.ds(pl.multiple_of(other * block, block), block)
            copies.append(
                mesh_copy(
                    keep.at[at, lanes],
                    owner_in.at[step, :, lanes],
                    owner_send,
                    owner_recv,
                    where,
                    {"dp": other},
                )
            )
            copies.append(
                mesh_copy(
                    keep.at[pl.ds(main, spare), lanes],
                    small_in.at[me, :, lanes],
                    small_send,
                    small_recv,
                    where,
                    {"dp": other},
                )
            )
            copies[-2].start()
            copies[-1].start()
        owner_copies.append(copies)

    mine = pl.ds(pl.multiple_of(me * block, block), block)
    whole_copies = []
    for chunk in range(chunks):
        lanes = pl.ds(chunk * columns, columns)
        for copy in owner_copies[chunk]:
            copy.wait()
        total = keep[mine, lanes].astype(jnp.float32)
        for step in range(1, owners):
            total = total + owner_in[step, :, lanes].astype(jnp.float32)
        part[:, lanes] = low(total)
        out_ref[mine, lanes] = low(total).astype(jnp.float32)
        copies = []
        for step in range(1, owners):
            copy = mesh_copy(
                part.at[:, lanes],
                whole_in.at[me, :, lanes],
                whole_send,
                whole_recv,
                chunk * owners + step,
                {"dp": lax.rem(me + step, owners)},
            )
            copy.start()
            copies.append(copy)
        whole_copies.append(copies)
        small_in[me, :, lanes] = keep[pl.ds(main, spare), lanes]
        narrow = small_in[0, :, lanes].astype(jnp.float32)
        for other in range(1, owners):
            narrow = narrow + small_in[other, :, lanes].astype(jnp.float32)
        out_ref[pl.ds(main, spare), lanes] = narrow

    for chunk in range(chunks):
        lanes = pl.ds(chunk * columns, columns)
        for copy in whole_copies[chunk]:
            copy.wait()
        for step in range(1, owners):
            other = lax.rem(me + step, owners)
            at = pl.ds(pl.multiple_of(other * block, block), block)
            out_ref[at, lanes] = whole_in[other, :, lanes].astype(jnp.float32)


def reduce_in_kernel(changes, small, owners):
    shards, rows, width = changes[0].shape
    spare = small.shape[1]
    main = 4 * rows
    total = main + spare
    block = main // owners
    chunks = 3
    low_type = jnp.bfloat16
    space = pl.BlockSpec(memory_space=pltpu.VMEM)
    return pl.pallas_call(
        functools.partial(reduce_mixer, owners, chunks),
        out_shape=jax.ShapeDtypeStruct((total, width), jnp.float32),
        in_specs=[space] * 5,
        out_specs=space,
        scratch_shapes=[
            pltpu.VMEM((2, total, width), low_type),
            pltpu.VMEM((total, width), low_type),
            pltpu.VMEM((total, width), low_type),
            pltpu.VMEM((total, width), low_type),
            pltpu.VMEM((owners, block, width), low_type),
            pltpu.VMEM((owners, spare, width), low_type),
            pltpu.VMEM((block, width), low_type),
            pltpu.VMEM((owners, block, width), low_type),
        ]
        + [pltpu.SemaphoreType.DMA((10 * chunks,))] * 2
        + [pltpu.SemaphoreType.DMA((chunks,))] * 2
        + [pltpu.SemaphoreType.DMA((chunks * owners,))] * 6,
        compiler_params=pltpu.CompilerParams(
            collective_id=1, has_side_effects=True, vmem_limit_bytes=40 << 20
        ),
        name="reduce_mixer",
    )(*changes, small)


def plan_routes(routes, experts, capacity):
    length = routes.shape[0]
    flat = routes.reshape(-1)
    selector = flat[:, None] == jnp.arange(experts, dtype=jnp.int32)[None, :]
    running = jnp.cumsum(selector.astype(jnp.int32), axis=0)
    rank = jnp.sum(jnp.where(selector, running, 0), axis=1) - 1
    slot = (flat * capacity + rank).reshape(length, TOP).T.reshape(-1)
    place = jnp.arange(experts * capacity, dtype=jnp.int32)
    taken = slot[None, :] == place[:, None]
    pick = low(taken)
    both = sum(pick[:, choice * length : (choice + 1) * length] for choice in range(TOP))
    chosen = routes[:, :, None] == jnp.arange(experts, dtype=jnp.int32)[None, None, :]
    return taken, pick, both, chosen


def exchange(values):
    return lax.all_to_all(values, "dp", split_axis=0, concat_axis=0, tiled=True)


def exchange_rows(values, experts):
    rows, width = values.shape
    return exchange(values.reshape(experts, rows // experts, width)).reshape(rows, width)


def exchange_numbers(values, experts):
    return exchange(values.reshape(experts, 1, -1)).reshape(-1)


def pack_small(router, attention_gain, expert_gain, bias):
    rows = router.shape[0]
    flat = bias.reshape(-1)
    column = jnp.concatenate([flat, jnp.zeros((rows - flat.shape[0],), flat.dtype)])
    block = jnp.concatenate(
        [router, attention_gain[:, None], expert_gain[:, None], column[:, None]], axis=1
    )
    return jnp.pad(block, ((0, 0), (0, -block.shape[1] % LANES)))


def unpack_small(block, experts, shards, heads):
    router = block[:, :experts]
    attention_gain = block[:, experts]
    expert_gain = block[:, experts + 1]
    column = block[:, experts + 2].reshape(shards, -1)
    bias = column[:, : heads // shards * NB].reshape(heads, NB)
    return router, attention_gain, expert_gain, bias


def per_device(
    tokens,
    query_weight,
    key_weight,
    value_weight,
    projection,
    router_weight,
    attention_gain,
    expert_gain,
    position_bias,
    expert_up,
    expert_down,
    routes,
    cotangent,
):
    layers = query_weight.shape[0]
    length, width = tokens.shape
    shards = lax.axis_size("fsdp")
    owners = lax.axis_size("dp")
    experts = owners * EXP_DEV
    heads = position_bias.shape[1] * shards
    capacity = max(2, 9 * length * TOP // (8 * experts))
    taken, pick, both, chosen = plan_routes(routes, experts, capacity)
    offsets = offset_selector(length)

    mixers = []
    for layer in range(layers):
        small = pack_small(
            router_weight[layer], attention_gain[layer], expert_gain[layer], position_bias[layer]
        )
        first = jnp.concatenate(
            [query_weight[layer], key_weight[layer], value_weight[layer], small], axis=1
        )
        first = lax.all_gather(first, "fsdp", axis=0, tiled=True)
        second = lax.all_gather(projection[layer], "fsdp", axis=0, tiled=True)
        router, gain_attention, gain_expert, bias = unpack_small(
            first[:, 3 * width :], experts, shards, heads
        )
        table = lax.dot_general(
            bias.astype(jnp.float32), offsets, contract_last, precision=highest
        )
        mixers.append(
            (
                first[:, : 3 * width],
                second,
                router,
                gain_attention.astype(jnp.float32),
                gain_expert.astype(jnp.float32),
                table,
            )
        )

    early = exchange_rows(low(dot(both, cotangent)), experts)

    hidden = tokens.astype(jnp.float32)
    saved = []
    for layer in range(layers):
        joined_weight, projection_full, router, gain_attention, gain_expert, table = mixers[layer]
        up_matrix, down_matrix = expert_up[layer, 0], expert_down[layer, 0]
        scale = row_scale(hidden)
        normed = low(hidden * scale * gain_attention)
        joined = low(dot(normed, joined_weight))
        mixed, log_total = attention_forward(joined, table, heads)
        if layer == 0:
            mixed, early = lax.optimization_barrier((mixed, early))
        middle = hidden + dot(mixed, projection_full)
        scale_expert = row_scale(middle)
        normed_expert = low(middle * scale_expert * gain_expert)
        logits = dot(normed_expert, router)
        picked = jnp.sum(jnp.where(chosen, logits[:, None, :], 0.0), axis=-1)
        gates = jax.nn.softmax(picked, axis=-1)
        gate_line = gates.T.reshape(-1)
        received = exchange_rows(low(dot(both, normed_expert)), experts)
        if layer == layers - 1:
            gate_places = exchange_numbers(
                jnp.sum(jnp.where(taken, gate_line[None, :], 0.0), axis=1), experts
            )
            received, gate_places = lax.optimization_barrier((received, gate_places))
        inner = dot(received, up_matrix)
        activity, slope = smooth_pair(inner)
        activity = low(activity)
        result = low(dot(activity, down_matrix))
        if layer == layers - 1:
            back_places = jnp.sum(early.astype(jnp.float32) * result.astype(jnp.float32), axis=1)
            back_places = exchange_numbers(back_places, experts)
            back_sent = low(gate_places[:, None] * early.astype(jnp.float32))
            back_inner = low(dot_last(back_sent, down_matrix) * slope)
            back_rows = exchange_rows(low(dot_last(back_inner, up_matrix)), experts)
            last = (back_places, back_sent, back_inner, back_rows)
        returned = exchange_rows(result, experts)
        routed = low(dot_first(pick, returned)).reshape(TOP, length, width)
        update = sum(
            gates[:, choice : choice + 1] * routed[choice].astype(jnp.float32)
            for choice in range(TOP)
        )
        saved.append(
            (
                hidden,
                scale,
                normed,
                joined,
                mixed,
                log_total,
                middle,
                scale_expert,
                normed_expert,
                gates,
                received,
                activity,
                slope,
                routed,
            )
        )
        hidden = middle + update
    output = low(hidden)

    back_out = cotangent.astype(jnp.float32)
    mixer_results = [None] * layers
    expert_results = [None] * layers
    for layer in range(layers - 1, -1, -1):
        joined_weight, projection_full, router, gain_attention, gain_expert, table = mixers[layer]
        up_matrix, down_matrix = expert_up[layer, 0], expert_down[layer, 0]
        (
            hidden,
            scale,
            normed,
            joined,
            mixed,
            log_total,
            middle,
            scale_expert,
            normed_expert,
            gates,
            received,
            activity,
            slope,
            routed,
        ) = saved[layer]
        if layer == layers - 1:
            back_places, back_sent, back_inner, back_rows = last
            back_gates = jnp.sum(jnp.where(taken, back_places[:, None], 0.0), axis=0)
            back_gates = back_gates.reshape(TOP, length).T
        else:
            back_gates = jnp.stack(
                [
                    jnp.sum(back_out * routed[choice].astype(jnp.float32), axis=-1)
                    for choice in range(TOP)
                ],
                axis=1,
            )
            gated = jnp.concatenate(
                [low(gates[:, choice : choice + 1] * back_out) for choice in range(TOP)], axis=0
            )
            back_sent = exchange_rows(low(dot(pick, gated)), experts)
            back_inner = low(dot_last(back_sent, down_matrix) * slope)
            back_rows = exchange_rows(low(dot_last(back_inner, up_matrix)), experts)
        down_change = low(dot_first(activity, back_sent))
        up_change = low(dot_first(received, back_inner))
        back_rows, down_change, up_change = lax.optimization_barrier(
            (back_rows, down_change, up_change)
        )
        expert_results[layer] = tuple(
            lax.psum_scatter(change, "fsdp", scatter_dimension=0, tiled=True).astype(jnp.float32)
            for change in (up_change, down_change)
        )
        back_picked = gates * (back_gates - jnp.sum(gates * back_gates, axis=-1, keepdims=True))
        back_logits = low(jnp.sum(jnp.where(chosen, back_picked[:, :, None], 0.0), axis=1))
        router_change = dot_first(normed_expert, back_logits)
        back_expert = dot_first(both, back_rows) + dot_last(back_logits, router)
        rows, expert_gain_change = norm_back(middle, scale_expert, gain_expert, back_expert)
        back_middle = back_out + rows
        back_attended = low(back_middle)
        back_mixed = low(dot_last(back_attended, projection_full))
        back_query, back_key, back_value, sums = attention_backward(
            joined, table, log_total, back_mixed, heads
        )
        bias_change = jnp.dot(sums, offsets, precision=highest)
        projection_change = dot_first(mixed, back_attended)
        parts = (back_query, back_key, back_value)
        changes = [low(dot_first(normed, part)) for part in parts]
        back_normed = sum(
            dot_last(part, joined_weight[:, index * width : (index + 1) * width])
            for index, part in enumerate(parts)
        )
        rows, attention_gain_change = norm_back(hidden, scale, gain_attention, back_normed)
        back_out = back_middle + rows
        changes = [
            change.reshape(shards, width // shards, width)
            for change in changes + [low(projection_change)]
        ]
        small = jnp.concatenate(
            [
                change.reshape(shards, -1)
                for change in (
                    router_change,
                    attention_gain_change,
                    expert_gain_change,
                    bias_change,
                )
            ],
            axis=1,
        )
        small = low(jnp.pad(small, ((0, 0), (0, -small.shape[1] % (16 * width)))))
        small = small.reshape(shards, -1, width)
        if layer == 0 and shards == 4 and owners == 8:
            mixer_results[layer] = reduce_in_kernel(changes, small, owners)
        else:
            packed = jnp.concatenate(changes + [small], axis=1)
            shard = lax.psum_scatter(packed, "fsdp", scatter_dimension=0)
            mixer_results[layer] = lax.psum(shard, "dp").astype(jnp.float32)

    rows = width // shards
    counts = (rows * experts, rows, rows, heads // shards * NB)
    smalls = []
    for result in mixer_results:
        flat = result[4 * rows :].reshape(-1)
        ends = [sum(counts[: index + 1]) for index in range(4)]
        smalls.append([flat[end - count : end] for end, count in zip(ends, counts)])
    small_gradients = [jnp.stack([small[index] for small in smalls]) for index in range(4)]
    router_gradient = small_gradients[0].reshape(layers, rows, experts)
    bias_gradient = small_gradients[3].reshape(position_bias.shape)
    mixer_gradients = [
        jnp.stack([result[index * rows : (index + 1) * rows] for result in mixer_results])
        for index in range(4)
    ]
    up_stack = jnp.stack([expert_results[layer][0] for layer in range(layers)])[:, None]
    down_stack = jnp.stack([expert_results[layer][1] for layer in range(layers)])[:, None]
    return (
        output,
        back_out,
        *mixer_gradients,
        router_gradient,
        small_gradients[1],
        small_gradients[2],
        bias_gradient,
        up_stack,
        down_stack,
    )


def solution(mesh):
    return jax.shard_map(
        per_device,
        mesh=mesh,
        in_specs=(
            P(("dp", "fsdp"), None),
            P(None, "fsdp", None),
            P(None, "fsdp", None),
            P(None, "fsdp", None),
            P(None, "fsdp", None),
            P(None, "fsdp", None),
            P(None, "fsdp"),
            P(None, "fsdp"),
            P(None, "fsdp", None),
            P(None, "dp", None, None),
            P(None, "dp", None, None),
            P(("dp", "fsdp"), None),
            P(("dp", "fsdp"), None),
        ),
        out_specs=(
            P(("dp", "fsdp"), None),
            P(("dp", "fsdp"), None),
            P(None, "fsdp", None),
            P(None, "fsdp", None),
            P(None, "fsdp", None),
            P(None, "fsdp", None),
            P(None, "fsdp", None),
            P(None, "fsdp"),
            P(None, "fsdp"),
            P(None, "fsdp", None),
            P(None, "dp", "fsdp", None),
            P(None, "dp", "fsdp", None),
        ),
        check_vma=False,
    )
```

```python
import functools

import jax
import jax.numpy as jnp
from jax import lax
from jax.experimental import pallas as pl
from jax.experimental.pallas import tpu as pltpu
from jax.sharding import PartitionSpec as P

EXP_DEV = 1
TOP = 2
BLOCK = 256
NB = 32
LANES = 128


epsilon = 1e-06
edges = (1, 2, 3, 4, 5, 6, 7, 8, 12, 16, 24, 32, 64, 128, 256)
highest = lax.Precision.HIGHEST
contract_first = (((0,), (0,)), ((), ()))
contract_last = (((1,), (1,)), ((), ()))
root = 0.7978845608028654
cubic = 0.044715


def dot(left, right):
    return jnp.dot(left, right, preferred_element_type=jnp.float32)


def dot_last(left, right):
    return lax.dot_general(left, right, contract_last, preferred_element_type=jnp.float32)


def dot_first(left, right):
    return lax.dot_general(left, right, contract_first, preferred_element_type=jnp.float32)


def low(values):
    return values.astype(jnp.bfloat16)


def row_scale(values):
    return lax.rsqrt(jnp.mean(values * values, axis=-1, keepdims=True) + epsilon)


def norm_back(values, scale, gain, back):
    lifted = back * gain
    inner = jnp.mean(lifted * values, axis=-1, keepdims=True)
    rows = scale * lifted - scale * scale * scale * values * inner
    return rows, jnp.sum(back * values * scale, axis=0)


def smooth_pair(values):
    tail = jnp.tanh(root * (values + cubic * values * values * values))
    half = 0.5 * (1.0 + tail)
    slope = half + 0.5 * values * (1.0 - tail * tail) * root * (1.0 + 3.0 * cubic * values * values)
    return values * half, slope


def offset_selector(length):
    offset = jnp.arange(2 * length, dtype=jnp.int32) - (length - 1)
    distance = jnp.abs(offset)
    bucket = jnp.zeros_like(offset)
    for edge in edges:
        bucket = bucket + (distance >= edge).astype(jnp.int32)
    bucket = bucket + NB // 2 * (offset > 0).astype(jnp.int32)
    return (bucket[:, None] == jnp.arange(NB, dtype=jnp.int32)[None, :]).astype(jnp.float32)


def lane_of(half, heads):
    lanes = lax.broadcasted_iota(jnp.int32, (1, LANES), 1)
    size = LANES // heads
    return (lanes >= half * size) & (lanes < (half + 1) * size)


def bias_tile(table, start, block, keys):
    span = table.shape[1]
    length = span // 2
    spread = jnp.broadcast_to(table, (block, span))
    shift = (start - (length - 1)) % span
    return pltpu.roll(spread, shift, 1, stride=1, stride_axis=0)[:, :keys]


def attend(pair, scale, q_ref, k_ref, v_ref, table_ref, mixed_ref, log_ref):
    length = q_ref.shape[0]
    for start in range(0, length, BLOCK):
        keys = start + BLOCK
        rows = pl.ds(start, BLOCK)
        query = q_ref[rows, :]
        key = k_ref[pl.ds(0, keys), :]
        value = v_ref[pl.ds(0, keys), :]
        mixed = None
        for half in range(pair):
            lane = lane_of(half, pair)
            table = table_ref[0, half : half + 1, :]
            raw = dot_last(jnp.where(lane, query, jnp.zeros_like(query)), key)
            scores = scale * raw + bias_tile(table, start, BLOCK, keys)
            peak = jnp.max(scores, axis=-1, keepdims=True)
            lifted = jnp.exp(scores - peak)
            total = jnp.sum(lifted, axis=-1, keepdims=True)
            shares = low(lifted * (1.0 / total))
            part = dot(shares, value)
            tops = jnp.broadcast_to(peak + jnp.log(total), part.shape)
            mixed = part if mixed is None else jnp.where(lane, part, mixed)
            logs = tops if half == 0 else jnp.where(lane, tops, logs)
        mixed_ref[rows, :] = low(mixed)
        log_ref[rows, :] = logs


def attend_back(
    pair,
    scale,
    q_ref,
    k_ref,
    v_ref,
    table_ref,
    log_ref,
    back_ref,
    dq_ref,
    dk_ref,
    dv_ref,
    sums_ref,
    key_sum,
    value_sum,
):
    length = q_ref.shape[0]
    size = LANES // pair
    span = 2 * length
    order = list(range(0, length, BLOCK))[::-1]
    for turn, start in enumerate(order):
        keys = start + BLOCK
        rows = pl.ds(start, BLOCK)
        query = q_ref[rows, :]
        back = back_ref[rows, :]
        key = k_ref[pl.ds(0, keys), :]
        value = v_ref[pl.ds(0, keys), :]
        back_query = None
        for half in range(pair):
            lane = lane_of(half, pair)
            table = table_ref[0, half : half + 1, :]
            query_half = jnp.where(lane, query, jnp.zeros_like(query))
            back_half = jnp.where(lane, back, jnp.zeros_like(back))
            raw = dot_last(query_half, key)
            scores = scale * raw + bias_tile(table, start, BLOCK, keys)
            shares = jnp.exp(scores - log_ref[rows, half * size : half * size + 1])
            back_shares = dot_last(back_half, value)
            weighted = shares * back_shares
            back_scores = weighted - shares * jnp.sum(weighted, axis=-1, keepdims=True)
            back_raw = low(scale * back_scores)
            part = dot(back_raw, key)
            back_query = part if back_query is None else jnp.where(lane, part, back_query)
            key_part = dot_first(back_raw, query_half)
            value_part = dot_first(low(shares), back_half)
            if turn == 0 and half == 0:
                key_sum[pl.ds(0, keys), :] = key_part
                value_sum[pl.ds(0, keys), :] = value_part
            else:
                key_sum[pl.ds(0, keys), :] += key_part
                value_sum[pl.ds(0, keys), :] += value_part
            first = length - 1 - start
            lines = jnp.zeros((8, span), jnp.float32)
            wide = jnp.concatenate(
                [back_scores, jnp.zeros((BLOCK, span - keys), jnp.float32)], axis=1
            )
            for tile in range(BLOCK // 8):
                piece = wide[tile * 8 : tile * 8 + 8, :]
                lines = lines + pltpu.roll(piece, (first - tile * 8) % span, 1)
            line = lines[0:1, :]
            for step in range(1, 8):
                line = line + pltpu.roll(lines[step : step + 1, :], span - step, 1)
            if turn == 0:
                sums_ref[0, half : half + 1, :] = line
            else:
                sums_ref[0, half : half + 1, :] += line
        dq_ref[rows, :] = low(back_query)
    dk_ref[...] = low(key_sum[...])
    dv_ref[...] = low(value_sum[...])


def attention_specs(length, heads, size):
    pair = LANES // size
    groups = heads // pair

    def column(offset):
        return pl.BlockSpec((length, LANES), lambda g: (0, g + offset))

    table = pl.BlockSpec((1, pair, 2 * length), lambda g: (g, 0, 0))
    return pair, groups, column, table


def attention_forward(joined, table, heads):
    length, width = joined.shape[0], joined.shape[1] // 3
    size = width // heads
    pair, groups, column, table_spec = attention_specs(length, heads, size)
    return pl.pallas_call(
        functools.partial(attend, pair, size**-0.5),
        grid=(groups,),
        out_shape=(
            jax.ShapeDtypeStruct((length, width), jnp.bfloat16),
            jax.ShapeDtypeStruct((length, width), jnp.float32),
        ),
        in_specs=[column(0), column(groups), column(2 * groups), table_spec],
        out_specs=(column(0), column(0)),
        compiler_params=pltpu.CompilerParams(vmem_limit_bytes=32 << 20),
        cost_estimate=pl.CostEstimate(
            flops=4 * length * length * width,
            bytes_accessed=length * width * 12,
            transcendentals=length * length * heads,
        ),
        name="attend",
    )(joined, joined, joined, table.reshape(groups, pair, 2 * length))


def attention_backward(joined, table, log_total, back_mixed, heads):
    length, width = back_mixed.shape
    size = width // heads
    pair, groups, column, table_spec = attention_specs(length, heads, size)
    rows = jax.ShapeDtypeStruct((length, width), jnp.bfloat16)
    back_query, back_key, back_value, sums = pl.pallas_call(
        functools.partial(attend_back, pair, size**-0.5),
        grid=(groups,),
        out_shape=(
            rows,
            rows,
            rows,
            jax.ShapeDtypeStruct((groups, pair, 2 * length), jnp.float32),
        ),
        in_specs=[
            column(0),
            column(groups),
            column(2 * groups),
            table_spec,
            column(0),
            column(0),
        ],
        out_specs=(column(0), column(0), column(0), table_spec),
        scratch_shapes=[pltpu.VMEM((length, LANES), jnp.float32)] * 2,
        compiler_params=pltpu.CompilerParams(vmem_limit_bytes=32 << 20),
        cost_estimate=pl.CostEstimate(
            flops=10 * length * length * width,
            bytes_accessed=length * width * 20,
            transcendentals=length * length * heads,
        ),
        name="attend_back",
    )(joined, joined, joined, table.reshape(groups, pair, 2 * length), log_total, back_mixed)
    return back_query, back_key, back_value, sums.reshape(heads, 2 * length)


def mesh_copy(source, target, sends, receives, where, device):
    return pltpu.make_async_remote_copy(
        src_ref=source,
        dst_ref=target,
        send_sem=sends.at[where],
        recv_sem=receives.at[where],
        device_id=device,
        device_id_type=pl.DeviceIdType.MESH,
    )


def reduce_mixer(
    owners,
    chunks,
    q_ref,
    k_ref,
    v_ref,
    p_ref,
    small_ref,
    out_ref,
    core_in,
    side_out,
    side_in,
    keep,
    owner_in,
    small_in,
    part,
    whole_in,
    core_send,
    core_recv,
    side_send,
    side_recv,
    owner_send,
    owner_recv,
    small_send,
    small_recv,
    whole_send,
    whole_recv,
):
    me = lax.axis_index("dp")
    place = lax.axis_index("fsdp")
    core, side = lax.rem(place, 2), place // 2
    partner = 2 * side + (1 - core)
    across = 2 * (1 - side) + core
    refs = (q_ref, k_ref, v_ref, p_ref, small_ref)
    rows = q_ref.shape[1]
    spare = small_ref.shape[1]
    main = 4 * rows
    block = main // owners
    columns = q_ref.shape[2] // chunks
    spans = [(index * rows, ref.shape[1]) for index, ref in enumerate(refs)]

    barrier = pltpu.get_barrier_semaphore()
    for other in (partner, across):
        pl.semaphore_signal(
            barrier, inc=1, device_id={"fsdp": other}, device_id_type=pl.DeviceIdType.MESH
        )
    for step in range(1, owners):
        pl.semaphore_signal(
            barrier,
            inc=1,
            device_id={"dp": lax.rem(me + step, owners)},
            device_id_type=pl.DeviceIdType.MESH,
        )
    pl.semaphore_wait(barrier, owners + 1)

    waits = []
    core_copies = [[] for _ in range(chunks)]
    for chunk in range(chunks):
        lanes = pl.ds(chunk * columns, columns)
        for turn in range(2):
            there = 1 - side if turn == 0 else side
            for index, (start, count) in enumerate(spans):
                copy = mesh_copy(
                    refs[index].at[2 * there + 1 - core, :, lanes],
                    core_in.at[turn, pl.ds(start, count), lanes],
                    core_send,
                    core_recv,
                    (chunk * 2 + turn) * 5 + index,
                    {"fsdp": partner},
                )
                copy.start()
                core_copies[chunk].append(copy)

    side_copies = []
    for chunk in range(chunks):
        lanes = pl.ds(chunk * columns, columns)
        for copy in core_copies[chunk]:
            copy.wait()
        for turn in range(2):
            there = 1 - side if turn == 0 else side
            target = side_out if turn == 0 else keep
            for index, (start, count) in enumerate(spans):
                at = pl.ds(start, count)
                total = refs[index][2 * there + core, :, lanes].astype(jnp.float32)
                total = total + core_in[turn, at, lanes].astype(jnp.float32)
                target[at, lanes] = low(total)
            if turn == 0:
                copy = mesh_copy(
                    side_out.at[:, lanes],
                    side_in.at[:, lanes],
                    side_send,
                    side_recv,
                    chunk,
                    {"fsdp": across},
                )
                copy.start()
                side_copies.append(copy)

    owner_copies = []
    for chunk in range(chunks):
        lanes = pl.ds(chunk * columns, columns)
        side_copies[chunk].wait()
        keep[:, lanes] = low(
            keep[:, lanes].astype(jnp.float32) + side_in[:, lanes].astype(jnp.float32)
        )
        copies = []
        for step in range(1, owners):
            other = lax.rem(me + step, owners)
            where = chunk * owners + step
            at = pl.ds(pl.multiple_of(other * block, block), block)
            copies.append(
                mesh_copy(
                    keep.at[at, lanes],
                    owner_in.at[step, :, lanes],
                    owner_send,
                    owner_recv,
                    where,
                    {"dp": other},
                )
            )
            copies.append(
                mesh_copy(
                    keep.at[pl.ds(main, spare), lanes],
                    small_in.at[me, :, lanes],
                    small_send,
                    small_recv,
                    where,
                    {"dp": other},
                )
            )
            copies[-2].start()
            copies[-1].start()
        owner_copies.append(copies)

    mine = pl.ds(pl.multiple_of(me * block, block), block)
    whole_copies = []
    for chunk in range(chunks):
        lanes = pl.ds(chunk * columns, columns)
        for copy in owner_copies[chunk]:
            copy.wait()
        total = keep[mine, lanes].astype(jnp.float32)
        for step in range(1, owners):
            total = total + owner_in[step, :, lanes].astype(jnp.float32)
        part[:, lanes] = low(total)
        out_ref[mine, lanes] = low(total).astype(jnp.float32)
        copies = []
        for step in range(1, owners):
            copy = mesh_copy(
                part.at[:, lanes],
                whole_in.at[me, :, lanes],
                whole_send,
                whole_recv,
                chunk * owners + step,
                {"dp": lax.rem(me + step, owners)},
            )
            copy.start()
            copies.append(copy)
        whole_copies.append(copies)
        small_in[me, :, lanes] = keep[pl.ds(main, spare), lanes]
        narrow = small_in[0, :, lanes].astype(jnp.float32)
        for other in range(1, owners):
            narrow = narrow + small_in[other, :, lanes].astype(jnp.float32)
        out_ref[pl.ds(main, spare), lanes] = narrow

    for chunk in range(chunks):
        lanes = pl.ds(chunk * columns, columns)
        for copy in whole_copies[chunk]:
            copy.wait()
        for step in range(1, owners):
            other = lax.rem(me + step, owners)
            at = pl.ds(pl.multiple_of(other * block, block), block)
            out_ref[at, lanes] = whole_in[other, :, lanes].astype(jnp.float32)


def reduce_in_kernel(changes, small, owners):
    shards, rows, width = changes[0].shape
    spare = small.shape[1]
    main = 4 * rows
    total = main + spare
    block = main // owners
    chunks = 3
    low_type = jnp.bfloat16
    space = pl.BlockSpec(memory_space=pltpu.VMEM)
    return pl.pallas_call(
        functools.partial(reduce_mixer, owners, chunks),
        out_shape=jax.ShapeDtypeStruct((total, width), jnp.float32),
        in_specs=[space] * 5,
        out_specs=space,
        scratch_shapes=[
            pltpu.VMEM((2, total, width), low_type),
            pltpu.VMEM((total, width), low_type),
            pltpu.VMEM((total, width), low_type),
            pltpu.VMEM((total, width), low_type),
            pltpu.VMEM((owners, block, width), low_type),
            pltpu.VMEM((owners, spare, width), low_type),
            pltpu.VMEM((block, width), low_type),
            pltpu.VMEM((owners, block, width), low_type),
        ]
        + [pltpu.SemaphoreType.DMA((10 * chunks,))] * 2
        + [pltpu.SemaphoreType.DMA((chunks,))] * 2
        + [pltpu.SemaphoreType.DMA((chunks * owners,))] * 6,
        compiler_params=pltpu.CompilerParams(
            collective_id=1, has_side_effects=True, vmem_limit_bytes=40 << 20
        ),
        name="reduce_mixer",
    )(*changes, small)


def plan_routes(routes, experts, capacity):
    length = routes.shape[0]
    flat = routes.reshape(-1)
    selector = flat[:, None] == jnp.arange(experts, dtype=jnp.int32)[None, :]
    running = jnp.cumsum(selector.astype(jnp.int32), axis=0)
    rank = jnp.sum(jnp.where(selector, running, 0), axis=1) - 1
    slot = (flat * capacity + rank).reshape(length, TOP).T.reshape(-1)
    place = jnp.arange(experts * capacity, dtype=jnp.int32)
    taken = slot[None, :] == place[:, None]
    pick = low(taken)
    both = sum(pick[:, choice * length : (choice + 1) * length] for choice in range(TOP))
    chosen = routes[:, :, None] == jnp.arange(experts, dtype=jnp.int32)[None, None, :]
    return taken, pick, both, chosen


def exchange(values):
    return lax.all_to_all(values, "dp", split_axis=0, concat_axis=0, tiled=True)


def exchange_rows(values, experts):
    rows, width = values.shape
    return exchange(values.reshape(experts, rows // experts, width)).reshape(rows, width)


def exchange_numbers(values, experts):
    return exchange(values.reshape(experts, 1, -1)).reshape(-1)


def gather_rows(pick, returned, gates):
    length = gates.shape[0]
    routed = low(dot_first(pick, returned)).reshape(TOP, length, -1)
    update = sum(
        gates[:, choice : choice + 1] * routed[choice].astype(jnp.float32) for choice in range(TOP)
    )
    return routed, update


def pack_small(router, attention_gain, expert_gain, bias):
    rows = router.shape[0]
    flat = bias.reshape(-1)
    column = jnp.concatenate([flat, jnp.zeros((rows - flat.shape[0],), flat.dtype)])
    block = jnp.concatenate(
        [router, attention_gain[:, None], expert_gain[:, None], column[:, None]], axis=1
    )
    return jnp.pad(block, ((0, 0), (0, -block.shape[1] % LANES)))


def unpack_small(block, experts, shards, heads):
    router = block[:, :experts]
    attention_gain = block[:, experts]
    expert_gain = block[:, experts + 1]
    column = block[:, experts + 2].reshape(shards, -1)
    bias = column[:, : heads // shards * NB].reshape(heads, NB)
    return router, attention_gain, expert_gain, bias


def per_device(
    tokens,
    query_weight,
    key_weight,
    value_weight,
    projection,
    router_weight,
    attention_gain,
    expert_gain,
    position_bias,
    expert_up,
    expert_down,
    routes,
    cotangent,
):
    layers = query_weight.shape[0]
    length, width = tokens.shape
    shards = lax.axis_size("fsdp")
    owners = lax.axis_size("dp")
    experts = owners * EXP_DEV
    heads = position_bias.shape[1] * shards
    capacity = max(2, 9 * length * TOP // (8 * experts))
    taken, pick, both, chosen = plan_routes(routes, experts, capacity)
    offsets = offset_selector(length)

    mixers = []
    for layer in range(layers):
        small = pack_small(
            router_weight[layer], attention_gain[layer], expert_gain[layer], position_bias[layer]
        )
        first = jnp.concatenate(
            [query_weight[layer], key_weight[layer], value_weight[layer], small], axis=1
        )
        first = lax.all_gather(first, "fsdp", axis=0, tiled=True)
        second = lax.all_gather(projection[layer], "fsdp", axis=0, tiled=True)
        router, gain_attention, gain_expert, bias = unpack_small(
            first[:, 3 * width :], experts, shards, heads
        )
        table = lax.dot_general(
            bias.astype(jnp.float32), offsets, contract_last, precision=highest
        )
        mixers.append(
            (
                first[:, : 3 * width],
                second,
                router,
                gain_attention.astype(jnp.float32),
                gain_expert.astype(jnp.float32),
                table,
            )
        )

    early = exchange_rows(low(dot(both, cotangent)), experts)

    hidden = tokens.astype(jnp.float32)
    saved = []
    for layer in range(layers):
        joined_weight, projection_full, router, gain_attention, gain_expert, table = mixers[layer]
        up_matrix, down_matrix = expert_up[layer, 0], expert_down[layer, 0]
        scale = row_scale(hidden)
        normed = low(hidden * scale * gain_attention)
        joined = low(dot(normed, joined_weight))
        mixed, log_total = attention_forward(joined, table, heads)
        if layer == 0:
            mixed, early = lax.optimization_barrier((mixed, early))
        middle = hidden + dot(mixed, projection_full)
        scale_expert = row_scale(middle)
        normed_expert = low(middle * scale_expert * gain_expert)
        logits = dot(normed_expert, router)
        picked = jnp.sum(jnp.where(chosen, logits[:, None, :], 0.0), axis=-1)
        gates = jax.nn.softmax(picked, axis=-1)
        gate_line = gates.T.reshape(-1)
        received = exchange_rows(low(dot(both, normed_expert)), experts)
        if layer == layers - 1:
            gate_places = exchange_numbers(
                jnp.sum(jnp.where(taken, gate_line[None, :], 0.0), axis=1), experts
            )
            received, gate_places = lax.optimization_barrier((received, gate_places))
        inner = dot(received, up_matrix)
        activity, slope = smooth_pair(inner)
        activity = low(activity)
        result = low(dot(activity, down_matrix))
        if layer == layers - 1:
            back_places = jnp.sum(early.astype(jnp.float32) * result.astype(jnp.float32), axis=1)
            back_places = exchange_numbers(back_places, experts)
            back_sent = low(gate_places[:, None] * early.astype(jnp.float32))
            back_inner = low(dot_last(back_sent, down_matrix) * slope)
            back_rows, back_sent = lax.optimization_barrier(
                (low(dot_last(back_inner, up_matrix)), back_sent)
            )
            back_rows = exchange_rows(back_rows, experts)
            last = (back_places, back_sent, back_inner, back_rows)
        returned = exchange_rows(result, experts)
        routed = None
        if layer < layers - 1:
            routed, update = gather_rows(pick, returned, gates)
        saved.append(
            (
                hidden,
                scale,
                normed,
                joined,
                mixed,
                log_total,
                middle,
                scale_expert,
                normed_expert,
                gates,
                received,
                activity,
                slope,
                routed,
            )
        )
        if layer < layers - 1:
            hidden = middle + update

    back_out = cotangent.astype(jnp.float32)
    mixer_results = [None] * layers
    expert_results = [None] * layers
    above = None
    for layer in range(layers - 1, -1, -1):
        joined_weight, projection_full, router, gain_attention, gain_expert, table = mixers[layer]
        up_matrix, down_matrix = expert_up[layer, 0], expert_down[layer, 0]
        (
            hidden,
            scale,
            normed,
            joined,
            mixed,
            log_total,
            middle,
            scale_expert,
            normed_expert,
            gates,
            received,
            activity,
            slope,
            routed,
        ) = saved[layer]
        if layer == layers - 1:
            back_places, back_sent, back_inner, back_rows = last
            back_gates = jnp.sum(jnp.where(taken, back_places[:, None], 0.0), axis=0)
            back_gates = back_gates.reshape(TOP, length).T
        else:
            back_gates = jnp.stack(
                [
                    jnp.sum(back_out * routed[choice].astype(jnp.float32), axis=-1)
                    for choice in range(TOP)
                ],
                axis=1,
            )
            gated = jnp.concatenate(
                [low(gates[:, choice : choice + 1] * back_out) for choice in range(TOP)], axis=0
            )
            back_sent = exchange_rows(low(dot(pick, gated)), experts)
            up_above, down_above = expert_results[layer + 1]
            back_sent, up_above = lax.optimization_barrier((back_sent, up_above))
            expert_results[layer + 1] = (up_above, down_above)
            back_inner = low(dot_last(back_sent, down_matrix) * slope)
            back_inner, above = lax.optimization_barrier((back_inner, above))
            mixer_results[layer + 1] = lax.psum(above, "dp")
            back_rows, back_sent = lax.optimization_barrier(
                (low(dot_last(back_inner, up_matrix)), back_sent)
            )
            back_rows = exchange_rows(back_rows, experts)
        down_change = low(dot_first(activity, back_sent))
        up_change = low(dot_first(received, back_inner))
        expert_results[layer] = tuple(
            lax.psum_scatter(change, "fsdp", scatter_dimension=0, tiled=True)
            for change in (up_change, down_change)
        )
        back_rows, down_change, up_change = lax.optimization_barrier(
            (back_rows, down_change, up_change)
        )
        back_picked = gates * (back_gates - jnp.sum(gates * back_gates, axis=-1, keepdims=True))
        back_logits = low(jnp.sum(jnp.where(chosen, back_picked[:, :, None], 0.0), axis=1))
        router_change = dot_first(normed_expert, back_logits)
        back_expert = dot_first(both, back_rows) + dot_last(back_logits, router)
        rows, expert_gain_change = norm_back(middle, scale_expert, gain_expert, back_expert)
        back_middle = back_out + rows
        back_attended = low(back_middle)
        back_mixed = low(dot_last(back_attended, projection_full))
        back_query, back_key, back_value, sums = attention_backward(
            joined, table, log_total, back_mixed, heads
        )
        if layer == layers - 1:
            back_query, returned = lax.optimization_barrier((back_query, returned))
            output = low(middle + gather_rows(pick, returned, gates)[1])
        if layer > 0:
            up_shard, down_shard = expert_results[layer]
            back_query, back_key, back_value, down_shard = lax.optimization_barrier(
                (back_query, back_key, back_value, down_shard)
            )
            expert_results[layer] = (up_shard, down_shard)
        bias_change = jnp.dot(sums, offsets, precision=highest)
        projection_change = dot_first(mixed, back_attended)
        parts = (back_query, back_key, back_value)
        changes = [low(dot_first(normed, part)) for part in parts]
        back_normed = sum(
            dot_last(part, joined_weight[:, index * width : (index + 1) * width])
            for index, part in enumerate(parts)
        )
        rows, attention_gain_change = norm_back(hidden, scale, gain_attention, back_normed)
        back_out = back_middle + rows
        changes = [
            change.reshape(shards, width // shards, width)
            for change in changes + [low(projection_change)]
        ]
        small = jnp.concatenate(
            [
                change.reshape(shards, -1)
                for change in (
                    router_change,
                    attention_gain_change,
                    expert_gain_change,
                    bias_change,
                )
            ],
            axis=1,
        )
        small = low(jnp.pad(small, ((0, 0), (0, -small.shape[1] % (16 * width)))))
        small = small.reshape(shards, -1, width)
        if layer == 0 and shards == 4 and owners == 8:
            mixer_results[layer] = reduce_in_kernel(changes, small, owners)
        else:
            packed = jnp.concatenate(changes + [small], axis=1)
            above = lax.psum_scatter(packed, "fsdp", scatter_dimension=0)
            if layer == 0:
                mixer_results[layer] = lax.psum(above, "dp")

    mixer_results = lax.optimization_barrier(mixer_results)
    mixer_results = [result.astype(jnp.float32) for result in mixer_results]
    rows = width // shards
    counts = (rows * experts, rows, rows, heads // shards * NB)
    smalls = []
    for result in mixer_results:
        flat = result[4 * rows :].reshape(-1)
        ends = [sum(counts[: index + 1]) for index in range(4)]
        smalls.append([flat[end - count : end] for end, count in zip(ends, counts)])
    small_gradients = [jnp.stack([small[index] for small in smalls]) for index in range(4)]
    router_gradient = small_gradients[0].reshape(layers, rows, experts)
    bias_gradient = small_gradients[3].reshape(position_bias.shape)
    mixer_gradients = [
        jnp.stack([result[index * rows : (index + 1) * rows] for result in mixer_results])
        for index in range(4)
    ]
    up_stack, down_stack = (
        jnp.stack([results[index].astype(jnp.float32) for results in expert_results])[:, None]
        for index in range(2)
    )
    return (
        output,
        back_out,
        *mixer_gradients,
        router_gradient,
        small_gradients[1],
        small_gradients[2],
        bias_gradient,
        up_stack,
        down_stack,
    )


def solution(mesh):
    return jax.shard_map(
        per_device,
        mesh=mesh,
        in_specs=(
            P(("dp", "fsdp"), None),
            P(None, "fsdp", None),
            P(None, "fsdp", None),
            P(None, "fsdp", None),
            P(None, "fsdp", None),
            P(None, "fsdp", None),
            P(None, "fsdp"),
            P(None, "fsdp"),
            P(None, "fsdp", None),
            P(None, "dp", None, None),
            P(None, "dp", None, None),
            P(("dp", "fsdp"), None),
            P(("dp", "fsdp"), None),
        ),
        out_specs=(
            P(("dp", "fsdp"), None),
            P(("dp", "fsdp"), None),
            P(None, "fsdp", None),
            P(None, "fsdp", None),
            P(None, "fsdp", None),
            P(None, "fsdp", None),
            P(None, "fsdp", None),
            P(None, "fsdp"),
            P(None, "fsdp"),
            P(None, "fsdp", None),
            P(None, "dp", "fsdp", None),
            P(None, "dp", "fsdp", None),
        ),
        check_vma=False,
    )
```

```python
import functools

import jax
import jax.numpy as jnp
from jax import lax
from jax.experimental import pallas as pl
from jax.experimental.pallas import tpu as pltpu
from jax.sharding import PartitionSpec as P

EXP_DEV = 1
TOP = 2
BLOCK = 256
NB = 32
LANES = 128


epsilon = 1e-06
edges = (1, 2, 3, 4, 5, 6, 7, 8, 12, 16, 24, 32, 64, 128, 256)
highest = lax.Precision.HIGHEST
contract_first = (((0,), (0,)), ((), ()))
contract_last = (((1,), (1,)), ((), ()))
root = 0.7978845608028654
cubic = 0.044715


def dot(left, right):
    return jnp.dot(left, right, preferred_element_type=jnp.float32)


def dot_last(left, right):
    return lax.dot_general(left, right, contract_last, preferred_element_type=jnp.float32)


def dot_first(left, right):
    return lax.dot_general(left, right, contract_first, preferred_element_type=jnp.float32)


def low(values):
    return values.astype(jnp.bfloat16)


def row_scale(values):
    return lax.rsqrt(jnp.mean(values * values, axis=-1, keepdims=True) + epsilon)


def norm_back(values, scale, gain, back):
    lifted = back * gain
    inner = jnp.mean(lifted * values, axis=-1, keepdims=True)
    rows = scale * lifted - scale * scale * scale * values * inner
    return rows, jnp.sum(back * values * scale, axis=0)


def smooth_pair(values):
    tail = jnp.tanh(root * (values + cubic * values * values * values))
    half = 0.5 * (1.0 + tail)
    slope = half + 0.5 * values * (1.0 - tail * tail) * root * (1.0 + 3.0 * cubic * values * values)
    return values * half, slope


def offset_selector(length):
    offset = jnp.arange(2 * length, dtype=jnp.int32) - (length - 1)
    distance = jnp.abs(offset)
    bucket = jnp.zeros_like(offset)
    for edge in edges:
        bucket = bucket + (distance >= edge).astype(jnp.int32)
    bucket = bucket + NB // 2 * (offset > 0).astype(jnp.int32)
    return (bucket[:, None] == jnp.arange(NB, dtype=jnp.int32)[None, :]).astype(jnp.float32)


def lane_of(half, heads):
    lanes = lax.broadcasted_iota(jnp.int32, (1, LANES), 1)
    size = LANES // heads
    return (lanes >= half * size) & (lanes < (half + 1) * size)


def bias_tile(table, start, block, keys):
    span = table.shape[1]
    length = span // 2
    spread = jnp.broadcast_to(table, (block, span))
    shift = (start - (length - 1)) % span
    return pltpu.roll(spread, shift, 1, stride=1, stride_axis=0)[:, :keys]


def attend(pair, scale, q_ref, k_ref, v_ref, table_ref, mixed_ref, log_ref):
    length = q_ref.shape[0]
    for start in range(0, length, BLOCK):
        keys = start + BLOCK
        rows = pl.ds(start, BLOCK)
        query = q_ref[rows, :]
        key = k_ref[pl.ds(0, keys), :]
        value = v_ref[pl.ds(0, keys), :]
        mixed = None
        for half in range(pair):
            lane = lane_of(half, pair)
            table = table_ref[0, half : half + 1, :]
            raw = dot_last(jnp.where(lane, query, jnp.zeros_like(query)), key)
            scores = scale * raw + bias_tile(table, start, BLOCK, keys)
            peak = jnp.max(scores, axis=-1, keepdims=True)
            lifted = jnp.exp(scores - peak)
            total = jnp.sum(lifted, axis=-1, keepdims=True)
            shares = low(lifted * (1.0 / total))
            part = dot(shares, value)
            tops = jnp.broadcast_to(peak + jnp.log(total), part.shape)
            mixed = part if mixed is None else jnp.where(lane, part, mixed)
            logs = tops if half == 0 else jnp.where(lane, tops, logs)
        mixed_ref[rows, :] = low(mixed)
        log_ref[rows, :] = logs


def attend_back(
    pair,
    scale,
    q_ref,
    k_ref,
    v_ref,
    table_ref,
    log_ref,
    back_ref,
    dq_ref,
    dk_ref,
    dv_ref,
    sums_ref,
    key_sum,
    value_sum,
):
    length = q_ref.shape[0]
    size = LANES // pair
    span = 2 * length
    order = list(range(0, length, BLOCK))[::-1]
    for turn, start in enumerate(order):
        keys = start + BLOCK
        rows = pl.ds(start, BLOCK)
        query = q_ref[rows, :]
        back = back_ref[rows, :]
        key = k_ref[pl.ds(0, keys), :]
        value = v_ref[pl.ds(0, keys), :]
        back_query = None
        for half in range(pair):
            lane = lane_of(half, pair)
            table = table_ref[0, half : half + 1, :]
            query_half = jnp.where(lane, query, jnp.zeros_like(query))
            back_half = jnp.where(lane, back, jnp.zeros_like(back))
            raw = dot_last(query_half, key)
            scores = scale * raw + bias_tile(table, start, BLOCK, keys)
            shares = jnp.exp(scores - log_ref[rows, half * size : half * size + 1])
            back_shares = dot_last(back_half, value)
            weighted = shares * back_shares
            back_scores = weighted - shares * jnp.sum(weighted, axis=-1, keepdims=True)
            back_raw = low(scale * back_scores)
            part = dot(back_raw, key)
            back_query = part if back_query is None else jnp.where(lane, part, back_query)
            key_part = dot_first(back_raw, query_half)
            value_part = dot_first(low(shares), back_half)
            if turn == 0 and half == 0:
                key_sum[pl.ds(0, keys), :] = key_part
                value_sum[pl.ds(0, keys), :] = value_part
            else:
                key_sum[pl.ds(0, keys), :] += key_part
                value_sum[pl.ds(0, keys), :] += value_part
            first = length - 1 - start
            lines = jnp.zeros((8, span), jnp.float32)
            wide = jnp.concatenate(
                [back_scores, jnp.zeros((BLOCK, span - keys), jnp.float32)], axis=1
            )
            for tile in range(BLOCK // 8):
                piece = wide[tile * 8 : tile * 8 + 8, :]
                lines = lines + pltpu.roll(piece, (first - tile * 8) % span, 1)
            line = lines[0:1, :]
            for step in range(1, 8):
                line = line + pltpu.roll(lines[step : step + 1, :], span - step, 1)
            if turn == 0:
                sums_ref[0, half : half + 1, :] = line
            else:
                sums_ref[0, half : half + 1, :] += line
        dq_ref[rows, :] = low(back_query)
    dk_ref[...] = low(key_sum[...])
    dv_ref[...] = low(value_sum[...])


def attention_specs(length, heads, size):
    pair = LANES // size
    groups = heads // pair

    def column(offset):
        return pl.BlockSpec((length, LANES), lambda g: (0, g + offset))

    table = pl.BlockSpec((1, pair, 2 * length), lambda g: (g, 0, 0))
    return pair, groups, column, table


def attention_forward(joined, table, heads):
    length, width = joined.shape[0], joined.shape[1] // 3
    size = width // heads
    pair, groups, column, table_spec = attention_specs(length, heads, size)
    return pl.pallas_call(
        functools.partial(attend, pair, size**-0.5),
        grid=(groups,),
        out_shape=(
            jax.ShapeDtypeStruct((length, width), jnp.bfloat16),
            jax.ShapeDtypeStruct((length, width), jnp.float32),
        ),
        in_specs=[column(0), column(groups), column(2 * groups), table_spec],
        out_specs=(column(0), column(0)),
        compiler_params=pltpu.CompilerParams(vmem_limit_bytes=32 << 20),
        cost_estimate=pl.CostEstimate(
            flops=4 * length * length * width,
            bytes_accessed=length * width * 12,
            transcendentals=length * length * heads,
        ),
        name="attend",
    )(joined, joined, joined, table.reshape(groups, pair, 2 * length))


def attention_backward(joined, table, log_total, back_mixed, heads):
    length, width = back_mixed.shape
    size = width // heads
    pair, groups, column, table_spec = attention_specs(length, heads, size)
    rows = jax.ShapeDtypeStruct((length, width), jnp.bfloat16)
    back_query, back_key, back_value, sums = pl.pallas_call(
        functools.partial(attend_back, pair, size**-0.5),
        grid=(groups,),
        out_shape=(
            rows,
            rows,
            rows,
            jax.ShapeDtypeStruct((groups, pair, 2 * length), jnp.float32),
        ),
        in_specs=[
            column(0),
            column(groups),
            column(2 * groups),
            table_spec,
            column(0),
            column(0),
        ],
        out_specs=(column(0), column(0), column(0), table_spec),
        scratch_shapes=[pltpu.VMEM((length, LANES), jnp.float32)] * 2,
        compiler_params=pltpu.CompilerParams(vmem_limit_bytes=32 << 20),
        cost_estimate=pl.CostEstimate(
            flops=10 * length * length * width,
            bytes_accessed=length * width * 20,
            transcendentals=length * length * heads,
        ),
        name="attend_back",
    )(joined, joined, joined, table.reshape(groups, pair, 2 * length), log_total, back_mixed)
    return back_query, back_key, back_value, sums.reshape(heads, 2 * length)


def mesh_copy(source, target, sends, receives, where, device):
    return pltpu.make_async_remote_copy(
        src_ref=source,
        dst_ref=target,
        send_sem=sends.at[where],
        recv_sem=receives.at[where],
        device_id=device,
        device_id_type=pl.DeviceIdType.MESH,
    )


def reduce_mixer(
    owners,
    chunks,
    q_ref,
    k_ref,
    v_ref,
    p_ref,
    small_ref,
    out_ref,
    core_in,
    side_out,
    side_in,
    keep,
    owner_in,
    small_in,
    part,
    whole_in,
    core_send,
    core_recv,
    side_send,
    side_recv,
    owner_send,
    owner_recv,
    small_send,
    small_recv,
    whole_send,
    whole_recv,
):
    me = lax.axis_index("dp")
    place = lax.axis_index("fsdp")
    core, side = lax.rem(place, 2), place // 2
    partner = 2 * side + (1 - core)
    across = 2 * (1 - side) + core
    refs = (q_ref, k_ref, v_ref, p_ref, small_ref)
    rows = q_ref.shape[1]
    spare = small_ref.shape[1]
    main = 4 * rows
    block = main // owners
    columns = q_ref.shape[2] // chunks
    spans = [(index * rows, ref.shape[1]) for index, ref in enumerate(refs)]

    barrier = pltpu.get_barrier_semaphore()
    for other in (partner, across):
        pl.semaphore_signal(
            barrier, inc=1, device_id={"fsdp": other}, device_id_type=pl.DeviceIdType.MESH
        )
    for step in range(1, owners):
        pl.semaphore_signal(
            barrier,
            inc=1,
            device_id={"dp": lax.rem(me + step, owners)},
            device_id_type=pl.DeviceIdType.MESH,
        )
    pl.semaphore_wait(barrier, owners + 1)

    waits = []
    core_copies = [[] for _ in range(chunks)]
    for chunk in range(chunks):
        lanes = pl.ds(chunk * columns, columns)
        for turn in range(2):
            there = 1 - side if turn == 0 else side
            for index, (start, count) in enumerate(spans):
                copy = mesh_copy(
                    refs[index].at[2 * there + 1 - core, :, lanes],
                    core_in.at[turn, pl.ds(start, count), lanes],
                    core_send,
                    core_recv,
                    (chunk * 2 + turn) * 5 + index,
                    {"fsdp": partner},
                )
                copy.start()
                core_copies[chunk].append(copy)

    side_copies = []
    for chunk in range(chunks):
        lanes = pl.ds(chunk * columns, columns)
        for copy in core_copies[chunk]:
            copy.wait()
        for turn in range(2):
            there = 1 - side if turn == 0 else side
            target = side_out if turn == 0 else keep
            for index, (start, count) in enumerate(spans):
                at = pl.ds(start, count)
                total = refs[index][2 * there + core, :, lanes].astype(jnp.float32)
                total = total + core_in[turn, at, lanes].astype(jnp.float32)
                target[at, lanes] = low(total)
            if turn == 0:
                copy = mesh_copy(
                    side_out.at[:, lanes],
                    side_in.at[:, lanes],
                    side_send,
                    side_recv,
                    chunk,
                    {"fsdp": across},
                )
                copy.start()
                side_copies.append(copy)

    owner_copies = []
    for chunk in range(chunks):
        lanes = pl.ds(chunk * columns, columns)
        side_copies[chunk].wait()
        keep[:, lanes] = low(
            keep[:, lanes].astype(jnp.float32) + side_in[:, lanes].astype(jnp.float32)
        )
        copies = []
        for step in range(1, owners):
            other = lax.rem(me + step, owners)
            where = chunk * owners + step
            at = pl.ds(pl.multiple_of(other * block, block), block)
            copies.append(
                mesh_copy(
                    keep.at[at, lanes],
                    owner_in.at[step, :, lanes],
                    owner_send,
                    owner_recv,
                    where,
                    {"dp": other},
                )
            )
            copies.append(
                mesh_copy(
                    keep.at[pl.ds(main, spare), lanes],
                    small_in.at[me, :, lanes],
                    small_send,
                    small_recv,
                    where,
                    {"dp": other},
                )
            )
            copies[-2].start()
            copies[-1].start()
        owner_copies.append(copies)

    mine = pl.ds(pl.multiple_of(me * block, block), block)
    whole_copies = []
    for chunk in range(chunks):
        lanes = pl.ds(chunk * columns, columns)
        for copy in owner_copies[chunk]:
            copy.wait()
        total = keep[mine, lanes].astype(jnp.float32)
        for step in range(1, owners):
            total = total + owner_in[step, :, lanes].astype(jnp.float32)
        part[:, lanes] = low(total)
        out_ref[mine, lanes] = low(total).astype(jnp.float32)
        copies = []
        for step in range(1, owners):
            copy = mesh_copy(
                part.at[:, lanes],
                whole_in.at[me, :, lanes],
                whole_send,
                whole_recv,
                chunk * owners + step,
                {"dp": lax.rem(me + step, owners)},
            )
            copy.start()
            copies.append(copy)
        whole_copies.append(copies)
        small_in[me, :, lanes] = keep[pl.ds(main, spare), lanes]
        narrow = small_in[0, :, lanes].astype(jnp.float32)
        for other in range(1, owners):
            narrow = narrow + small_in[other, :, lanes].astype(jnp.float32)
        out_ref[pl.ds(main, spare), lanes] = narrow

    for chunk in range(chunks):
        lanes = pl.ds(chunk * columns, columns)
        for copy in whole_copies[chunk]:
            copy.wait()
        for step in range(1, owners):
            other = lax.rem(me + step, owners)
            at = pl.ds(pl.multiple_of(other * block, block), block)
            out_ref[at, lanes] = whole_in[other, :, lanes].astype(jnp.float32)


def reduce_in_kernel(changes, small, owners):
    shards, rows, width = changes[0].shape
    spare = small.shape[1]
    main = 4 * rows
    total = main + spare
    block = main // owners
    chunks = 3
    low_type = jnp.bfloat16
    space = pl.BlockSpec(memory_space=pltpu.VMEM)
    return pl.pallas_call(
        functools.partial(reduce_mixer, owners, chunks),
        out_shape=jax.ShapeDtypeStruct((total, width), jnp.float32),
        in_specs=[space] * 5,
        out_specs=space,
        scratch_shapes=[
            pltpu.VMEM((2, total, width), low_type),
            pltpu.VMEM((total, width), low_type),
            pltpu.VMEM((total, width), low_type),
            pltpu.VMEM((total, width), low_type),
            pltpu.VMEM((owners, block, width), low_type),
            pltpu.VMEM((owners, spare, width), low_type),
            pltpu.VMEM((block, width), low_type),
            pltpu.VMEM((owners, block, width), low_type),
        ]
        + [pltpu.SemaphoreType.DMA((10 * chunks,))] * 2
        + [pltpu.SemaphoreType.DMA((chunks,))] * 2
        + [pltpu.SemaphoreType.DMA((chunks * owners,))] * 6,
        compiler_params=pltpu.CompilerParams(
            collective_id=1, has_side_effects=True, vmem_limit_bytes=40 << 20
        ),
        name="reduce_mixer",
    )(*changes, small)


def partner_of(me, index):
    other = me
    for bit, weight in ((1, 1), (2, 4), (4, 2)):
        if index & bit:
            other = other + weight * (1 - 2 * (lax.rem(me // weight, 2)))
    return other


def flip_row(row):
    count = row.shape[1]
    down = lax.broadcasted_iota(jnp.int32, (count, count), 0)
    along = lax.broadcasted_iota(jnp.int32, (count, count), 1)
    return jnp.sum(jnp.where(down == along, row, 0.0), axis=1, keepdims=True)


def flip_column(column):
    count = column.shape[0]
    down = lax.broadcasted_iota(jnp.int32, (count, count), 0)
    along = lax.broadcasted_iota(jnp.int32, (count, count), 1)
    return jnp.sum(jnp.where(down == along, column, 0.0), axis=0, keepdims=True)


def run_experts(mode, tile, *refs):
    refs = list(refs)

    def take(count):
        taken = refs[:count]
        del refs[:count]
        return taken

    sent, up_any, down_any = take(3)
    if mode == "forward":
        home, rows_in, activity_any, slope_any = take(4)
    elif mode == "backward":
        (slope_any,) = take(1)
        home, rows_in, inner_any = take(3)
    else:
        gates, early = take(2)
        home, rows_in, activity_any, inner_any, scaled, result, places = take(7)
    up, down, ready = take(3)
    if mode == "forward":
        activity, slope = take(2)
        outs = [(activity, activity_any), (slope, slope_any)]
    elif mode == "backward":
        slope, inner = take(2)
        outs = [(inner, inner_any)]
    else:
        activity, inner, gates_in, place_out = take(4)
        outs = [(activity, activity_any), (inner, inner_any)]
    load, own, stores, go_send, go_recv, back_send, back_recv = take(7)
    if mode == "both":
        gate_send, gate_recv, place_send, place_recv = take(4)

    owners, capacity, width = sent.shape
    hidden = up.shape[1]
    me = lax.axis_index("dp")
    barrier = pltpu.get_barrier_semaphore()
    for index in range(1, owners):
        pl.semaphore_signal(
            barrier,
            inc=1,
            device_id={"dp": partner_of(me, index)},
            device_id_type=pl.DeviceIdType.MESH,
        )
    pl.semaphore_wait(barrier, owners - 1)

    going = {}
    gate_going = {}
    for index in range(1, owners):
        other = partner_of(me, index)
        copy = mesh_copy(
            sent.at[other], rows_in.at[index], go_send, go_recv, index, {"dp": other}
        )
        copy.start()
        going[index] = copy
        if mode == "both":
            copy = mesh_copy(
                gates.at[other], gates_in.at[index], gate_send, gate_recv, index, {"dp": other}
            )
            copy.start()
            gate_going[index] = copy
    first = [pltpu.make_async_copy(sent.at[me], rows_in.at[0], own.at[0])]
    if mode == "both":
        first.append(pltpu.make_async_copy(gates.at[me], gates_in.at[0], own.at[1]))
    first.append(pltpu.make_async_copy(up_any, up, load.at[0]))
    first.append(pltpu.make_async_copy(down_any, down, load.at[1]))
    if mode == "backward":
        first.append(pltpu.make_async_copy(slope_any, slope, load.at[2]))
    for copy in first:
        copy.start()

    coming = []
    for pair in range(owners // 2):
        blocks = (2 * pair, 2 * pair + 1)
        both = pl.ds(2 * pair, 2)
        count = 2 * capacity
        if pair == 0:
            for copy in first:
                copy.wait()
        for index in blocks:
            if index:
                going[index].wait_recv()
                if mode == "both":
                    gate_going[index].wait_recv()
        if mode == "both":
            for index in blocks:
                gate = flip_row(gates_in[index][:, :capacity])
                rows = early[partner_of(me, index)].astype(jnp.float32)
                scaled[index] = low(gate * rows)

        def widen(step, carry):
            columns = pl.ds(pl.multiple_of(step * tile, tile), tile)
            rows = rows_in[both].reshape(count, width)
            if mode == "backward":
                back = dot_last(rows, down[columns, :])
                inner[pair, :, columns] = low(back * slope[pair, :, columns].astype(jnp.float32))
                return carry
            value, steep = smooth_pair(dot(rows, up[:, columns]))
            activity[pair, :, columns] = low(value)
            if mode == "forward":
                slope[pair, :, columns] = low(steep)
            else:
                back = dot_last(scaled[both].reshape(count, width), down[columns, :])
                inner[pair, :, columns] = low(back * steep)
            return carry

        lax.fori_loop(0, hidden // tile, widen, 0)
        for at, (source, target) in enumerate(outs):
            copy = pltpu.make_async_copy(
                source.at[pair], target.at[pair], stores.at[at * (owners // 2) + pair]
            )
            copy.start()
            coming.append(copy)

        def narrow(step, carry):
            columns = pl.ds(pl.multiple_of(step * 256, 256), 256)
            if mode == "forward":
                rows = dot(activity[pair], down[:, columns])
            else:
                rows = dot_last(inner[pair], up[columns, :])
            ready[both, :, columns] = low(rows).reshape(2, capacity, 256)
            return carry

        lax.fori_loop(0, width // 256, narrow, 0)
        for index in blocks:
            other = partner_of(me, index)
            if index:
                copy = mesh_copy(
                    ready.at[index], home.at[me], back_send, back_recv, index, {"dp": other}
                )
            else:
                copy = pltpu.make_async_copy(ready.at[index], home.at[me], own.at[2])
            copy.start()
            coming.append(copy)

        if mode == "both":

            def finish(step, carry):
                columns = pl.ds(pl.multiple_of(step * 256, 256), 256)
                rows = low(dot(activity[pair], down[:, columns])).reshape(2, capacity, 256)
                sums = []
                for at, index in enumerate(blocks):
                    other = partner_of(me, index)
                    result[other, :, columns] = rows[at]
                    sums.append(
                        jnp.sum(
                            early[other, :, columns].astype(jnp.float32)
                            * rows[at].astype(jnp.float32),
                            axis=1,
                            keepdims=True,
                        )
                    )
                return tuple(old + new for old, new in zip(carry, sums))

            zero = jnp.zeros((capacity, 1), jnp.float32)
            totals = lax.fori_loop(0, width // 256, finish, (zero, zero))
            for at, index in enumerate(blocks):
                other = partner_of(me, index)
                place_out[index, :, :capacity] = flip_column(totals[at])
                if index:
                    copy = mesh_copy(
                        place_out.at[index],
                        places.at[me],
                        place_send,
                        place_recv,
                        index,
                        {"dp": other},
                    )
                else:
                    copy = pltpu.make_async_copy(place_out.at[index], places.at[me], own.at[3])
                copy.start()
                coming.append(copy)

    for index in range(1, owners):
        going[index].wait_send()
        if mode == "both":
            gate_going[index].wait_send()
    for copy in coming:
        copy.wait()


def experts_in_kernel(mode, sent, up_matrix, down_matrix, extra=()):
    owners, capacity, width = sent.shape
    hidden = up_matrix.shape[1]
    pairs = owners // 2
    low_type = jnp.bfloat16
    near = pl.BlockSpec(memory_space=pltpu.VMEM)
    far = pl.BlockSpec(memory_space=pl.ANY)
    rows = jax.ShapeDtypeStruct((owners, capacity, width), low_type)
    wide = jax.ShapeDtypeStruct((pairs, 2 * capacity, hidden), low_type)
    wide_scratch = pltpu.VMEM((pairs, 2 * capacity, hidden), low_type)
    lines = -(-capacity // LANES) * LANES
    line = jax.ShapeDtypeStruct((owners, 1, lines), jnp.float32)
    line_scratch = pltpu.VMEM((owners, 1, lines), jnp.float32)
    many = pltpu.SemaphoreType.DMA((owners,))
    if mode == "forward":
        ins, outs = [near, far, far], [(rows, near), (rows, near), (wide, far), (wide, far)]
        scratch = [wide_scratch] * 2
    elif mode == "backward":
        ins, outs = [near, far, far, far], [(rows, near), (rows, near), (wide, far)]
        scratch = [wide_scratch] * 2
    else:
        ins = [near, far, far, near, near]
        outs = [(rows, near), (rows, near), (wide, far), (wide, far)]
        outs += [(rows, near), (rows, near), (line, near)]
        scratch = [wide_scratch] * 2 + [line_scratch] * 2
    return pl.pallas_call(
        functools.partial(run_experts, mode, 512),
        out_shape=tuple(shape for shape, _ in outs),
        in_specs=ins,
        out_specs=tuple(spec for _, spec in outs),
        scratch_shapes=[
            pltpu.VMEM(up_matrix.shape, low_type),
            pltpu.VMEM(down_matrix.shape, low_type),
            pltpu.VMEM((owners, capacity, width), low_type),
        ]
        + scratch
        + [
            pltpu.SemaphoreType.DMA((3,)),
            pltpu.SemaphoreType.DMA((4,)),
            pltpu.SemaphoreType.DMA((2 * pairs,)),
        ]
        + [many] * (8 if mode == "both" else 4),
        compiler_params=pltpu.CompilerParams(
            collective_id={"forward": 2, "backward": 3, "both": 4}[mode],
            has_side_effects=True,
            vmem_limit_bytes=56 << 20,
        ),
        name="experts_" + mode,
    )(sent, up_matrix, down_matrix, *extra)


def plan_routes(routes, experts, capacity):
    length = routes.shape[0]
    flat = routes.reshape(-1)
    selector = flat[:, None] == jnp.arange(experts, dtype=jnp.int32)[None, :]
    running = jnp.cumsum(selector.astype(jnp.int32), axis=0)
    rank = jnp.sum(jnp.where(selector, running, 0), axis=1) - 1
    slot = (flat * capacity + rank).reshape(length, TOP).T.reshape(-1)
    place = jnp.arange(experts * capacity, dtype=jnp.int32)
    taken = slot[None, :] == place[:, None]
    pick = low(taken)
    both = sum(pick[:, choice * length : (choice + 1) * length] for choice in range(TOP))
    chosen = routes[:, :, None] == jnp.arange(experts, dtype=jnp.int32)[None, None, :]
    return taken, pick, both, chosen


def exchange(values):
    return lax.all_to_all(values, "dp", split_axis=0, concat_axis=0, tiled=True)


def exchange_rows(values, experts):
    rows, width = values.shape
    return exchange(values.reshape(experts, rows // experts, width)).reshape(rows, width)


def exchange_numbers(values, experts):
    return exchange(values.reshape(experts, 1, -1)).reshape(-1)


def gather_rows(pick, returned, gates):
    length = gates.shape[0]
    routed = low(dot_first(pick, returned)).reshape(TOP, length, -1)
    update = sum(
        gates[:, choice : choice + 1] * routed[choice].astype(jnp.float32) for choice in range(TOP)
    )
    return routed, update


def pack_small(router, attention_gain, expert_gain, bias):
    rows = router.shape[0]
    flat = bias.reshape(-1)
    column = jnp.concatenate([flat, jnp.zeros((rows - flat.shape[0],), flat.dtype)])
    block = jnp.concatenate(
        [router, attention_gain[:, None], expert_gain[:, None], column[:, None]], axis=1
    )
    return jnp.pad(block, ((0, 0), (0, -block.shape[1] % LANES)))


def unpack_small(block, experts, shards, heads):
    router = block[:, :experts]
    attention_gain = block[:, experts]
    expert_gain = block[:, experts + 1]
    column = block[:, experts + 2].reshape(shards, -1)
    bias = column[:, : heads // shards * NB].reshape(heads, NB)
    return router, attention_gain, expert_gain, bias


def per_device(
    tokens,
    query_weight,
    key_weight,
    value_weight,
    projection,
    router_weight,
    attention_gain,
    expert_gain,
    position_bias,
    expert_up,
    expert_down,
    routes,
    cotangent,
):
    layers = query_weight.shape[0]
    length, width = tokens.shape
    shards = lax.axis_size("fsdp")
    owners = lax.axis_size("dp")
    experts = owners * EXP_DEV
    heads = position_bias.shape[1] * shards
    capacity = max(2, 9 * length * TOP // (8 * experts))
    fused = shards == 4 and owners == 8 and capacity % 16 == 0
    taken, pick, both, chosen = plan_routes(routes, experts, capacity)
    offsets = offset_selector(length)

    mixers = []
    for layer in range(layers):
        small = pack_small(
            router_weight[layer], attention_gain[layer], expert_gain[layer], position_bias[layer]
        )
        first = jnp.concatenate(
            [query_weight[layer], key_weight[layer], value_weight[layer], small], axis=1
        )
        first = lax.all_gather(first, "fsdp", axis=0, tiled=True)
        second = lax.all_gather(projection[layer], "fsdp", axis=0, tiled=True)
        router, gain_attention, gain_expert, bias = unpack_small(
            first[:, 3 * width :], experts, shards, heads
        )
        table = lax.dot_general(
            bias.astype(jnp.float32), offsets, contract_last, precision=highest
        )
        mixers.append(
            (
                first[:, : 3 * width],
                second,
                router,
                gain_attention.astype(jnp.float32),
                gain_expert.astype(jnp.float32),
                table,
            )
        )

    early = exchange_rows(low(dot(both, cotangent)), experts)

    hidden = tokens.astype(jnp.float32)
    saved = []
    for layer in range(layers):
        joined_weight, projection_full, router, gain_attention, gain_expert, table = mixers[layer]
        up_matrix, down_matrix = expert_up[layer, 0], expert_down[layer, 0]
        scale = row_scale(hidden)
        normed = low(hidden * scale * gain_attention)
        joined = low(dot(normed, joined_weight))
        mixed, log_total = attention_forward(joined, table, heads)
        if layer == 0:
            mixed, early = lax.optimization_barrier((mixed, early))
        middle = hidden + dot(mixed, projection_full)
        scale_expert = row_scale(middle)
        normed_expert = low(middle * scale_expert * gain_expert)
        logits = dot(normed_expert, router)
        picked = jnp.sum(jnp.where(chosen, logits[:, None, :], 0.0), axis=-1)
        gates = jax.nn.softmax(picked, axis=-1)
        gate_line = gates.T.reshape(-1)
        sent = low(dot(both, normed_expert))
        slope = None
        if fused and layer < layers - 1:
            returned, received, activity, slope = experts_in_kernel(
                "forward", sent.reshape(experts, capacity, width), up_matrix, down_matrix
            )
            returned = returned.reshape(-1, width)
            received = received.reshape(-1, width)
            activity = activity.reshape(received.shape[0], -1)
        elif fused:
            gate_places = jnp.sum(jnp.where(taken, gate_line[None, :], 0.0), axis=1)
            gate_places = gate_places.reshape(experts, 1, capacity)
            gate_places = jnp.pad(gate_places, ((0, 0), (0, 0), (0, -capacity % LANES)))
            back_rows, received, activity, back_inner, back_sent, result, back_places = (
                experts_in_kernel(
                    "both",
                    sent.reshape(experts, capacity, width),
                    up_matrix,
                    down_matrix,
                    (gate_places, early.reshape(experts, capacity, width)),
                )
            )
            count = experts * capacity
            last = (
                back_places[:, 0, :capacity].reshape(-1),
                back_sent.reshape(count, width),
                back_inner.reshape(count, -1),
                back_rows.reshape(count, width),
            )
            received = received.reshape(count, width)
            activity = activity.reshape(count, -1)
            returned = exchange_rows(result.reshape(count, width), experts)
        else:
            received = exchange_rows(sent, experts)
            if layer == layers - 1:
                gate_places = exchange_numbers(
                    jnp.sum(jnp.where(taken, gate_line[None, :], 0.0), axis=1), experts
                )
                received, gate_places = lax.optimization_barrier((received, gate_places))
            inner = dot(received, up_matrix)
            activity, slope = smooth_pair(inner)
            activity = low(activity)
            result = low(dot(activity, down_matrix))
            if layer == layers - 1:
                back_places = jnp.sum(early.astype(jnp.float32) * result.astype(jnp.float32), axis=1)
                back_places = exchange_numbers(back_places, experts)
                back_sent = low(gate_places[:, None] * early.astype(jnp.float32))
                back_inner = low(dot_last(back_sent, down_matrix) * slope)
                back_rows, back_sent = lax.optimization_barrier(
                    (low(dot_last(back_inner, up_matrix)), back_sent)
                )
                back_rows = exchange_rows(back_rows, experts)
                last = (back_places, back_sent, back_inner, back_rows)
            returned = exchange_rows(result, experts)
        routed = None
        if layer < layers - 1:
            routed, update = gather_rows(pick, returned, gates)
        saved.append(
            (
                hidden,
                scale,
                normed,
                joined,
                mixed,
                log_total,
                middle,
                scale_expert,
                normed_expert,
                gates,
                received,
                activity,
                slope,
                routed,
            )
        )
        if layer < layers - 1:
            hidden = middle + update

    back_out = cotangent.astype(jnp.float32)
    mixer_results = [None] * layers
    expert_results = [None] * layers
    above = None
    for layer in range(layers - 1, -1, -1):
        joined_weight, projection_full, router, gain_attention, gain_expert, table = mixers[layer]
        up_matrix, down_matrix = expert_up[layer, 0], expert_down[layer, 0]
        (
            hidden,
            scale,
            normed,
            joined,
            mixed,
            log_total,
            middle,
            scale_expert,
            normed_expert,
            gates,
            received,
            activity,
            slope,
            routed,
        ) = saved[layer]
        if layer == layers - 1:
            back_places, back_sent, back_inner, back_rows = last
            back_gates = jnp.sum(jnp.where(taken, back_places[:, None], 0.0), axis=0)
            back_gates = back_gates.reshape(TOP, length).T
        else:
            back_gates = jnp.stack(
                [
                    jnp.sum(back_out * routed[choice].astype(jnp.float32), axis=-1)
                    for choice in range(TOP)
                ],
                axis=1,
            )
            gated = jnp.concatenate(
                [low(gates[:, choice : choice + 1] * back_out) for choice in range(TOP)], axis=0
            )
            back_sent = low(dot(pick, gated))
            up_above, down_above = expert_results[layer + 1]
            if fused:
                back_rows, back_sent, back_inner = experts_in_kernel(
                    "backward",
                    back_sent.reshape(experts, capacity, width),
                    up_matrix,
                    down_matrix,
                    (slope,),
                )
                back_rows, back_sent, up_above, above = lax.optimization_barrier(
                    (back_rows, back_sent, up_above, above)
                )
                back_rows = back_rows.reshape(-1, width)
                back_sent = back_sent.reshape(-1, width)
                back_inner = back_inner.reshape(back_sent.shape[0], -1)
            else:
                back_sent = exchange_rows(back_sent, experts)
                back_sent, up_above = lax.optimization_barrier((back_sent, up_above))
                back_inner = low(dot_last(back_sent, down_matrix) * slope)
                back_inner, above = lax.optimization_barrier((back_inner, above))
                back_rows, back_sent = lax.optimization_barrier(
                    (low(dot_last(back_inner, up_matrix)), back_sent)
                )
                back_rows = exchange_rows(back_rows, experts)
            expert_results[layer + 1] = (up_above, down_above)
            mixer_results[layer + 1] = lax.psum(above, "dp")
        down_change = low(dot_first(activity, back_sent))
        up_change = low(dot_first(received, back_inner))
        expert_results[layer] = tuple(
            lax.psum_scatter(change, "fsdp", scatter_dimension=0, tiled=True)
            for change in (up_change, down_change)
        )
        back_rows, down_change, up_change = lax.optimization_barrier(
            (back_rows, down_change, up_change)
        )
        back_picked = gates * (back_gates - jnp.sum(gates * back_gates, axis=-1, keepdims=True))
        back_logits = low(jnp.sum(jnp.where(chosen, back_picked[:, :, None], 0.0), axis=1))
        router_change = dot_first(normed_expert, back_logits)
        back_expert = dot_first(both, back_rows) + dot_last(back_logits, router)
        rows, expert_gain_change = norm_back(middle, scale_expert, gain_expert, back_expert)
        back_middle = back_out + rows
        back_attended = low(back_middle)
        back_mixed = low(dot_last(back_attended, projection_full))
        back_query, back_key, back_value, sums = attention_backward(
            joined, table, log_total, back_mixed, heads
        )
        if layer == layers - 1:
            back_query, returned = lax.optimization_barrier((back_query, returned))
            output = low(middle + gather_rows(pick, returned, gates)[1])
        if layer > 0:
            up_shard, down_shard = expert_results[layer]
            back_query, back_key, back_value, down_shard = lax.optimization_barrier(
                (back_query, back_key, back_value, down_shard)
            )
            expert_results[layer] = (up_shard, down_shard)
        bias_change = jnp.dot(sums, offsets, precision=highest)
        projection_change = dot_first(mixed, back_attended)
        parts = (back_query, back_key, back_value)
        changes = [low(dot_first(normed, part)) for part in parts]
        back_normed = sum(
            dot_last(part, joined_weight[:, index * width : (index + 1) * width])
            for index, part in enumerate(parts)
        )
        rows, attention_gain_change = norm_back(hidden, scale, gain_attention, back_normed)
        back_out = back_middle + rows
        changes = [
            change.reshape(shards, width // shards, width)
            for change in changes + [low(projection_change)]
        ]
        small = jnp.concatenate(
            [
                change.reshape(shards, -1)
                for change in (
                    router_change,
                    attention_gain_change,
                    expert_gain_change,
                    bias_change,
                )
            ],
            axis=1,
        )
        small = low(jnp.pad(small, ((0, 0), (0, -small.shape[1] % (16 * width)))))
        small = small.reshape(shards, -1, width)
        if layer == 0 and shards == 4 and owners == 8:
            mixer_results[layer] = reduce_in_kernel(changes, small, owners)
        else:
            packed = jnp.concatenate(changes + [small], axis=1)
            above = lax.psum_scatter(packed, "fsdp", scatter_dimension=0)
            if layer == 0:
                mixer_results[layer] = lax.psum(above, "dp")

    mixer_results = lax.optimization_barrier(mixer_results)
    mixer_results = [result.astype(jnp.float32) for result in mixer_results]
    rows = width // shards
    counts = (rows * experts, rows, rows, heads // shards * NB)
    smalls = []
    for result in mixer_results:
        flat = result[4 * rows :].reshape(-1)
        ends = [sum(counts[: index + 1]) for index in range(4)]
        smalls.append([flat[end - count : end] for end, count in zip(ends, counts)])
    small_gradients = [jnp.stack([small[index] for small in smalls]) for index in range(4)]
    router_gradient = small_gradients[0].reshape(layers, rows, experts)
    bias_gradient = small_gradients[3].reshape(position_bias.shape)
    mixer_gradients = [
        jnp.stack([result[index * rows : (index + 1) * rows] for result in mixer_results])
        for index in range(4)
    ]
    up_stack, down_stack = (
        jnp.stack([results[index].astype(jnp.float32) for results in expert_results])[:, None]
        for index in range(2)
    )
    return (
        output,
        back_out,
        *mixer_gradients,
        router_gradient,
        small_gradients[1],
        small_gradients[2],
        bias_gradient,
        up_stack,
        down_stack,
    )


def solution(mesh):
    return jax.shard_map(
        per_device,
        mesh=mesh,
        in_specs=(
            P(("dp", "fsdp"), None),
            P(None, "fsdp", None),
            P(None, "fsdp", None),
            P(None, "fsdp", None),
            P(None, "fsdp", None),
            P(None, "fsdp", None),
            P(None, "fsdp"),
            P(None, "fsdp"),
            P(None, "fsdp", None),
            P(None, "dp", None, None),
            P(None, "dp", None, None),
            P(("dp", "fsdp"), None),
            P(("dp", "fsdp"), None),
        ),
        out_specs=(
            P(("dp", "fsdp"), None),
            P(("dp", "fsdp"), None),
            P(None, "fsdp", None),
            P(None, "fsdp", None),
            P(None, "fsdp", None),
            P(None, "fsdp", None),
            P(None, "fsdp", None),
            P(None, "fsdp"),
            P(None, "fsdp"),
            P(None, "fsdp", None),
            P(None, "dp", "fsdp", None),
            P(None, "dp", "fsdp", None),
        ),
        check_vma=False,
    )
```

```python
import functools

import jax
import jax.numpy as jnp
from jax import lax
from jax.experimental import pallas as pl
from jax.experimental.pallas import tpu as pltpu
from jax.sharding import PartitionSpec as P

EXP_DEV = 1
TOP = 2
BLOCK = 256
NB = 32
LANES = 128


epsilon = 1e-06
edges = (1, 2, 3, 4, 5, 6, 7, 8, 12, 16, 24, 32, 64, 128, 256)
highest = lax.Precision.HIGHEST
contract_first = (((0,), (0,)), ((), ()))
contract_last = (((1,), (1,)), ((), ()))
root = 0.7978845608028654
cubic = 0.044715


def dot(left, right):
    return jnp.dot(left, right, preferred_element_type=jnp.float32)


def dot_last(left, right):
    return lax.dot_general(left, right, contract_last, preferred_element_type=jnp.float32)


def dot_first(left, right):
    return lax.dot_general(left, right, contract_first, preferred_element_type=jnp.float32)


def low(values):
    return values.astype(jnp.bfloat16)


def row_scale(values):
    return lax.rsqrt(jnp.mean(values * values, axis=-1, keepdims=True) + epsilon)


def norm_back(values, scale, gain, back):
    lifted = back * gain
    inner = jnp.mean(lifted * values, axis=-1, keepdims=True)
    rows = scale * lifted - scale * scale * scale * values * inner
    return rows, jnp.sum(back * values * scale, axis=0)


def smooth_pair(values):
    tail = jnp.tanh(root * (values + cubic * values * values * values))
    half = 0.5 * (1.0 + tail)
    slope = half + 0.5 * values * (1.0 - tail * tail) * root * (1.0 + 3.0 * cubic * values * values)
    return values * half, slope


def offset_selector(length):
    offset = jnp.arange(2 * length, dtype=jnp.int32) - (length - 1)
    distance = jnp.abs(offset)
    bucket = jnp.zeros_like(offset)
    for edge in edges:
        bucket = bucket + (distance >= edge).astype(jnp.int32)
    bucket = bucket + NB // 2 * (offset > 0).astype(jnp.int32)
    return (bucket[:, None] == jnp.arange(NB, dtype=jnp.int32)[None, :]).astype(jnp.float32)


def lane_of(half, heads):
    lanes = lax.broadcasted_iota(jnp.int32, (1, LANES), 1)
    size = LANES // heads
    return (lanes >= half * size) & (lanes < (half + 1) * size)


def bias_tile(table, start, block, keys):
    span = table.shape[1]
    length = span // 2
    spread = jnp.broadcast_to(table, (block, span))
    shift = (start - (length - 1)) % span
    return pltpu.roll(spread, shift, 1, stride=1, stride_axis=0)[:, :keys]


def attend(pair, scale, q_ref, k_ref, v_ref, table_ref, mixed_ref, log_ref):
    length = q_ref.shape[0]
    for start in range(0, length, BLOCK):
        keys = start + BLOCK
        rows = pl.ds(start, BLOCK)
        query = q_ref[rows, :]
        key = k_ref[pl.ds(0, keys), :]
        value = v_ref[pl.ds(0, keys), :]
        mixed = None
        for half in range(pair):
            lane = lane_of(half, pair)
            table = table_ref[0, half : half + 1, :]
            raw = dot_last(jnp.where(lane, query, jnp.zeros_like(query)), key)
            scores = scale * raw + bias_tile(table, start, BLOCK, keys)
            peak = jnp.max(scores, axis=-1, keepdims=True)
            lifted = jnp.exp(scores - peak)
            total = jnp.sum(lifted, axis=-1, keepdims=True)
            shares = low(lifted * (1.0 / total))
            part = dot(shares, value)
            tops = jnp.broadcast_to(peak + jnp.log(total), part.shape)
            mixed = part if mixed is None else jnp.where(lane, part, mixed)
            logs = tops if half == 0 else jnp.where(lane, tops, logs)
        mixed_ref[rows, :] = low(mixed)
        log_ref[rows, :] = logs


def attend_back(
    pair,
    scale,
    q_ref,
    k_ref,
    v_ref,
    table_ref,
    log_ref,
    back_ref,
    dq_ref,
    dk_ref,
    dv_ref,
    sums_ref,
    key_sum,
    value_sum,
):
    length = q_ref.shape[0]
    size = LANES // pair
    span = 2 * length
    order = list(range(0, length, BLOCK))[::-1]
    for turn, start in enumerate(order):
        keys = start + BLOCK
        rows = pl.ds(start, BLOCK)
        query = q_ref[rows, :]
        back = back_ref[rows, :]
        key = k_ref[pl.ds(0, keys), :]
        value = v_ref[pl.ds(0, keys), :]
        back_query = None
        for half in range(pair):
            lane = lane_of(half, pair)
            table = table_ref[0, half : half + 1, :]
            query_half = jnp.where(lane, query, jnp.zeros_like(query))
            back_half = jnp.where(lane, back, jnp.zeros_like(back))
            raw = dot_last(query_half, key)
            scores = scale * raw + bias_tile(table, start, BLOCK, keys)
            shares = jnp.exp(scores - log_ref[rows, half * size : half * size + 1])
            back_shares = dot_last(back_half, value)
            weighted = shares * back_shares
            back_scores = weighted - shares * jnp.sum(weighted, axis=-1, keepdims=True)
            back_raw = low(scale * back_scores)
            part = dot(back_raw, key)
            back_query = part if back_query is None else jnp.where(lane, part, back_query)
            key_part = dot_first(back_raw, query_half)
            value_part = dot_first(low(shares), back_half)
            if turn == 0 and half == 0:
                key_sum[pl.ds(0, keys), :] = key_part
                value_sum[pl.ds(0, keys), :] = value_part
            else:
                key_sum[pl.ds(0, keys), :] += key_part
                value_sum[pl.ds(0, keys), :] += value_part
            first = length - 1 - start
            lines = jnp.zeros((8, span), jnp.float32)
            wide = jnp.concatenate(
                [back_scores, jnp.zeros((BLOCK, span - keys), jnp.float32)], axis=1
            )
            for tile in range(BLOCK // 8):
                piece = wide[tile * 8 : tile * 8 + 8, :]
                lines = lines + pltpu.roll(piece, (first - tile * 8) % span, 1)
            line = lines[0:1, :]
            for step in range(1, 8):
                line = line + pltpu.roll(lines[step : step + 1, :], span - step, 1)
            if turn == 0:
                sums_ref[0, half : half + 1, :] = line
            else:
                sums_ref[0, half : half + 1, :] += line
        dq_ref[rows, :] = low(back_query)
    dk_ref[...] = low(key_sum[...])
    dv_ref[...] = low(value_sum[...])


def attention_specs(length, heads, size):
    pair = LANES // size
    groups = heads // pair

    def column(offset):
        return pl.BlockSpec((length, LANES), lambda g: (0, g + offset))

    table = pl.BlockSpec((1, pair, 2 * length), lambda g: (g, 0, 0))
    return pair, groups, column, table


def attention_forward(joined, table, heads):
    length, width = joined.shape[0], joined.shape[1] // 3
    size = width // heads
    pair, groups, column, table_spec = attention_specs(length, heads, size)
    return pl.pallas_call(
        functools.partial(attend, pair, size**-0.5),
        grid=(groups,),
        out_shape=(
            jax.ShapeDtypeStruct((length, width), jnp.bfloat16),
            jax.ShapeDtypeStruct((length, width), jnp.float32),
        ),
        in_specs=[column(0), column(groups), column(2 * groups), table_spec],
        out_specs=(column(0), column(0)),
        compiler_params=pltpu.CompilerParams(vmem_limit_bytes=32 << 20),
        cost_estimate=pl.CostEstimate(
            flops=4 * length * length * width,
            bytes_accessed=length * width * 12,
            transcendentals=length * length * heads,
        ),
        name="attend",
    )(joined, joined, joined, table.reshape(groups, pair, 2 * length))


def attention_backward(joined, table, log_total, back_mixed, heads):
    length, width = back_mixed.shape
    size = width // heads
    pair, groups, column, table_spec = attention_specs(length, heads, size)
    rows = jax.ShapeDtypeStruct((length, width), jnp.bfloat16)
    back_query, back_key, back_value, sums = pl.pallas_call(
        functools.partial(attend_back, pair, size**-0.5),
        grid=(groups,),
        out_shape=(
            rows,
            rows,
            rows,
            jax.ShapeDtypeStruct((groups, pair, 2 * length), jnp.float32),
        ),
        in_specs=[
            column(0),
            column(groups),
            column(2 * groups),
            table_spec,
            column(0),
            column(0),
        ],
        out_specs=(column(0), column(0), column(0), table_spec),
        scratch_shapes=[pltpu.VMEM((length, LANES), jnp.float32)] * 2,
        compiler_params=pltpu.CompilerParams(vmem_limit_bytes=32 << 20),
        cost_estimate=pl.CostEstimate(
            flops=10 * length * length * width,
            bytes_accessed=length * width * 20,
            transcendentals=length * length * heads,
        ),
        name="attend_back",
    )(joined, joined, joined, table.reshape(groups, pair, 2 * length), log_total, back_mixed)
    return back_query, back_key, back_value, sums.reshape(heads, 2 * length)


def mesh_copy(source, target, sends, receives, where, device):
    return pltpu.make_async_remote_copy(
        src_ref=source,
        dst_ref=target,
        send_sem=sends.at[where],
        recv_sem=receives.at[where],
        device_id=device,
        device_id_type=pl.DeviceIdType.MESH,
    )


def reduce_mixer(chunks, *refs):
    q_ref, k_ref, v_ref, p_ref, small_ref, above, out_ref, narrow_ref = refs[:8]
    core_in, side_out, side_in, keep, cross_in, half, line_in, whole, other_half, small_in = refs[
        8:18
    ]
    core_send, core_recv, side_send, side_recv = refs[18:22]
    x1_send, x1_recv, z1_send, z1_recv, z2_send, z2_recv, x2_send, x2_recv = refs[22:30]
    small_send, small_recv = refs[30:32]
    owners = small_in.shape[1]
    me = lax.axis_index("dp")
    place = lax.axis_index("fsdp")
    core, side = lax.rem(place, 2), place // 2
    partner = 2 * side + (1 - core)
    across = 2 * (1 - side) + core
    x, z = lax.rem(me, 2), me // 2
    x_peer = me + 1 - 2 * x
    depth = owners // 2
    inputs = (q_ref, k_ref, v_ref, p_ref, small_ref)
    rows = q_ref.shape[1]
    spare = small_ref.shape[1]
    main = 4 * rows
    quarter = main // 2
    block = quarter // depth
    columns = q_ref.shape[2] // chunks
    spans = [(index * rows, ref.shape[1]) for index, ref in enumerate(inputs)]
    sources = (keep, above)

    barrier = pltpu.get_barrier_semaphore()
    for other in (partner, across):
        pl.semaphore_signal(
            barrier, inc=1, device_id={"fsdp": other}, device_id_type=pl.DeviceIdType.MESH
        )
    for step in range(1, owners):
        pl.semaphore_signal(
            barrier,
            inc=1,
            device_id={"dp": lax.rem(me + step, owners)},
            device_id_type=pl.DeviceIdType.MESH,
        )
    pl.semaphore_wait(barrier, owners + 1)

    def lanes_of(chunk):
        return pl.ds(chunk * columns, columns)

    def half_at(index):
        return pl.ds(pl.multiple_of(index * quarter, quarter), quarter)

    def block_at(index):
        return pl.ds(pl.multiple_of(index * block, block), block)

    live = {}

    def start(key, copies):
        for copy in copies:
            copy.start()
        live[key] = copies

    def finish(key):
        for copy in live.pop(key):
            copy.wait()

    def start_core(chunk):
        lanes = lanes_of(chunk)
        copies = []
        for turn in range(2):
            there = 1 - side if turn == 0 else side
            for index, (first, count) in enumerate(spans):
                copies.append(
                    mesh_copy(
                        inputs[index].at[2 * there + 1 - core, :, lanes],
                        core_in.at[turn, pl.ds(first, count), lanes],
                        core_send,
                        core_recv,
                        (chunk * 2 + turn) * 5 + index,
                        {"fsdp": partner},
                    )
                )
        start(("core", chunk), copies)

    def add_core(chunk):
        lanes = lanes_of(chunk)
        finish(("core", chunk))
        for turn in range(2):
            there = 1 - side if turn == 0 else side
            target = side_out if turn == 0 else keep
            for index, (first, count) in enumerate(spans):
                at = pl.ds(first, count)
                total = inputs[index][2 * there + core, :, lanes].astype(jnp.float32)
                total = total + core_in[turn, at, lanes].astype(jnp.float32)
                target[at, lanes] = low(total)
            if turn == 0:
                copy = mesh_copy(
                    side_out.at[:, lanes],
                    side_in.at[:, lanes],
                    side_send,
                    side_recv,
                    chunk,
                    {"fsdp": across},
                )
                start(("side", chunk), [copy])

    def start_cross(layer, chunk):
        lanes = lanes_of(chunk)
        unit = layer * chunks + chunk
        if layer == 0:
            finish(("side", chunk))
            keep[:, lanes] = low(
                keep[:, lanes].astype(jnp.float32) + side_in[:, lanes].astype(jnp.float32)
            )
        source = sources[layer]
        copies = [
            mesh_copy(
                source.at[half_at(1 - x), lanes],
                cross_in.at[layer, :, lanes],
                x1_send,
                x1_recv,
                unit,
                {"dp": x_peer},
            )
        ]
        start(("x1", unit), copies)
        copies = [
            mesh_copy(
                source.at[pl.ds(main, spare), lanes],
                small_in.at[layer, me, :, lanes],
                small_send,
                small_recv,
                unit * owners + step,
                {"dp": lax.rem(me + step, owners)},
            )
            for step in range(1, owners)
        ]
        start(("small", unit), copies)

    def add_cross(layer, chunk):
        lanes = lanes_of(chunk)
        unit = layer * chunks + chunk
        finish(("x1", unit))
        half[layer, :, lanes] = low(
            sources[layer][half_at(x), lanes].astype(jnp.float32)
            + cross_in[layer, :, lanes].astype(jnp.float32)
        )
        copies = []
        for step in range(1, depth):
            there = lax.rem(z + step, depth)
            copies.append(
                mesh_copy(
                    half.at[layer, block_at(there), lanes],
                    line_in.at[layer, step, :, lanes],
                    z1_send,
                    z1_recv,
                    unit * depth + step,
                    {"dp": 2 * there + x},
                )
            )
        start(("z1", unit), copies)

    def add_line(layer, chunk):
        lanes = lanes_of(chunk)
        unit = layer * chunks + chunk
        finish(("z1", unit))
        total = half[layer, block_at(z), lanes].astype(jnp.float32)
        for step in range(1, depth):
            total = total + line_in[layer, step, :, lanes].astype(jnp.float32)
        whole[layer, block_at(z), lanes] = low(total)
        copies = []
        for step in range(1, depth):
            there = lax.rem(z + step, depth)
            copies.append(
                mesh_copy(
                    whole.at[layer, block_at(z), lanes],
                    whole.at[layer, block_at(z), lanes],
                    z2_send,
                    z2_recv,
                    unit * depth + step,
                    {"dp": 2 * there + x},
                )
            )
        start(("z2", unit), copies)

    def return_cross(layer, chunk):
        lanes = lanes_of(chunk)
        unit = layer * chunks + chunk
        finish(("z2", unit))
        copy = mesh_copy(
            whole.at[layer, :, lanes],
            other_half.at[layer, :, lanes],
            x2_send,
            x2_recv,
            unit,
            {"dp": x_peer},
        )
        start(("x2", unit), [copy])

    def write(layer, chunk):
        lanes = lanes_of(chunk)
        unit = layer * chunks + chunk
        finish(("x2", unit))
        for index in range(2):
            at = pl.ds(index * rows, rows)
            out_ref[2 * x + index, layer, :, lanes] = whole[layer, at, lanes].astype(jnp.float32)
            out_ref[2 * (1 - x) + index, layer, :, lanes] = other_half[layer, at, lanes].astype(
                jnp.float32
            )
        finish(("small", unit))
        small_in[layer, me, :, lanes] = sources[layer][pl.ds(main, spare), lanes]
        narrow = small_in[layer, 0, :, lanes].astype(jnp.float32)
        for other in range(1, owners):
            narrow = narrow + small_in[layer, other, :, lanes].astype(jnp.float32)
        narrow_ref[layer, :, lanes] = narrow

    for chunk in range(chunks):
        start_core(chunk)
    for chunk in range(chunks):
        start_cross(1, chunk)
    for chunk in range(chunks):
        add_core(chunk)
        add_cross(1, chunk)
    for chunk in range(chunks):
        add_line(1, chunk)
    start_cross(0, 0)
    return_cross(1, 0)
    add_cross(0, 0)
    return_cross(1, 1)
    start_cross(0, 1)
    return_cross(1, 2)
    add_line(0, 0)
    add_cross(0, 1)
    for chunk in range(chunks):
        write(1, chunk)
    start_cross(0, 2)
    add_line(0, 1)
    add_cross(0, 2)
    return_cross(0, 0)
    return_cross(0, 1)
    add_line(0, 2)
    write(0, 0)
    return_cross(0, 2)
    write(0, 1)
    write(0, 2)


def reduce_in_kernel(changes, small, above, owners):
    shards, rows, width = changes[0].shape
    spare = small.shape[1]
    main = 4 * rows
    total = main + spare
    block = main // owners
    chunks = 3
    units = 2 * chunks
    low_type = jnp.bfloat16
    space = pl.BlockSpec(memory_space=pltpu.VMEM)
    return pl.pallas_call(
        functools.partial(reduce_mixer, chunks),
        out_shape=(
            jax.ShapeDtypeStruct((4, 2, rows, width), jnp.float32),
            jax.ShapeDtypeStruct((2, spare, width), jnp.float32),
        ),
        in_specs=[space] * 6,
        out_specs=(space, space),
        scratch_shapes=[
            pltpu.VMEM((2, total, width), low_type),
            pltpu.VMEM((total, width), low_type),
            pltpu.VMEM((total, width), low_type),
            pltpu.VMEM((total, width), low_type),
            pltpu.VMEM((2, main // 2, width), low_type),
            pltpu.VMEM((2, main // 2, width), low_type),
            pltpu.VMEM((2, owners // 2, block, width), low_type),
            pltpu.VMEM((2, main // 2, width), low_type),
            pltpu.VMEM((2, main // 2, width), low_type),
            pltpu.VMEM((2, owners, spare, width), low_type),
        ]
        + [pltpu.SemaphoreType.DMA((10 * chunks,))] * 2
        + [pltpu.SemaphoreType.DMA((chunks,))] * 2
        + [pltpu.SemaphoreType.DMA((units,))] * 2
        + [pltpu.SemaphoreType.DMA((units * owners // 2,))] * 4
        + [pltpu.SemaphoreType.DMA((units,))] * 2
        + [pltpu.SemaphoreType.DMA((units * owners,))] * 2,
        compiler_params=pltpu.CompilerParams(
            collective_id=1, has_side_effects=True, vmem_limit_bytes=48 << 20
        ),
        name="reduce_mixer",
    )(*changes, small, above)


def partner_of(me, index):
    other = me
    for bit, weight in ((1, 1), (2, 4), (4, 2)):
        if index & bit:
            other = other + weight * (1 - 2 * (lax.rem(me // weight, 2)))
    return other


def flip_row(row):
    count = row.shape[1]
    down = lax.broadcasted_iota(jnp.int32, (count, count), 0)
    along = lax.broadcasted_iota(jnp.int32, (count, count), 1)
    return jnp.sum(jnp.where(down == along, row, 0.0), axis=1, keepdims=True)


def flip_column(column):
    count = column.shape[0]
    down = lax.broadcasted_iota(jnp.int32, (count, count), 0)
    along = lax.broadcasted_iota(jnp.int32, (count, count), 1)
    return jnp.sum(jnp.where(down == along, column, 0.0), axis=0, keepdims=True)


def run_experts(mode, tile, *refs):
    refs = list(refs)

    def take(count):
        taken = refs[:count]
        del refs[:count]
        return taken

    sent, up_any, down_any = take(3)
    if mode == "forward":
        home, rows_in, activity_any, slope_any = take(4)
    elif mode == "backward":
        (slope_any,) = take(1)
        home, rows_in, inner_any = take(3)
    else:
        gates, early = take(2)
        home, rows_in, activity_any, inner_any, scaled, result, places = take(7)
    up, down, ready = take(3)
    if mode == "forward":
        activity, slope = take(2)
        outs = [(activity, activity_any), (slope, slope_any)]
    elif mode == "backward":
        slope, inner = take(2)
        outs = [(inner, inner_any)]
    else:
        activity, inner, gates_in, place_out = take(4)
        outs = [(activity, activity_any), (inner, inner_any)]
    load, own, stores, go_send, go_recv, back_send, back_recv = take(7)
    if mode == "both":
        gate_send, gate_recv, place_send, place_recv = take(4)

    owners, capacity, width = sent.shape
    hidden = up.shape[1]
    me = lax.axis_index("dp")
    barrier = pltpu.get_barrier_semaphore()
    for index in range(1, owners):
        pl.semaphore_signal(
            barrier,
            inc=1,
            device_id={"dp": partner_of(me, index)},
            device_id_type=pl.DeviceIdType.MESH,
        )
    pl.semaphore_wait(barrier, owners - 1)

    going = {}
    gate_going = {}
    for index in range(1, owners):
        other = partner_of(me, index)
        copy = mesh_copy(
            sent.at[other], rows_in.at[index], go_send, go_recv, index, {"dp": other}
        )
        copy.start()
        going[index] = copy
        if mode == "both":
            copy = mesh_copy(
                gates.at[other], gates_in.at[index], gate_send, gate_recv, index, {"dp": other}
            )
            copy.start()
            gate_going[index] = copy
    first = [pltpu.make_async_copy(sent.at[me], rows_in.at[0], own.at[0])]
    if mode == "both":
        first.append(pltpu.make_async_copy(gates.at[me], gates_in.at[0], own.at[1]))
    first.append(pltpu.make_async_copy(up_any, up, load.at[0]))
    first.append(pltpu.make_async_copy(down_any, down, load.at[1]))
    if mode == "backward":
        first.append(pltpu.make_async_copy(slope_any, slope, load.at[2]))
    for copy in first:
        copy.start()

    coming = []
    for pair in range(owners // 2):
        blocks = (2 * pair, 2 * pair + 1)
        both = pl.ds(2 * pair, 2)
        count = 2 * capacity
        if pair == 0:
            for copy in first:
                copy.wait()
        for index in blocks:
            if index:
                going[index].wait_recv()
                if mode == "both":
                    gate_going[index].wait_recv()
        if mode == "both":
            for index in blocks:
                gate = flip_row(gates_in[index][:, :capacity])
                rows = early[partner_of(me, index)].astype(jnp.float32)
                scaled[index] = low(gate * rows)

        def widen(step, carry):
            columns = pl.ds(pl.multiple_of(step * tile, tile), tile)
            rows = rows_in[both].reshape(count, width)
            if mode == "backward":
                back = dot_last(rows, down[columns, :])
                inner[pair, :, columns] = low(back * slope[pair, :, columns].astype(jnp.float32))
                return carry
            value, steep = smooth_pair(dot(rows, up[:, columns]))
            activity[pair, :, columns] = low(value)
            if mode == "forward":
                slope[pair, :, columns] = low(steep)
            else:
                back = dot_last(scaled[both].reshape(count, width), down[columns, :])
                inner[pair, :, columns] = low(back * steep)
            return carry

        lax.fori_loop(0, hidden // tile, widen, 0)
        for at, (source, target) in enumerate(outs):
            copy = pltpu.make_async_copy(
                source.at[pair], target.at[pair], stores.at[at * (owners // 2) + pair]
            )
            copy.start()
            coming.append(copy)

        def narrow(step, carry):
            columns = pl.ds(pl.multiple_of(step * 256, 256), 256)
            if mode == "forward":
                rows = dot(activity[pair], down[:, columns])
            else:
                rows = dot_last(inner[pair], up[columns, :])
            ready[both, :, columns] = low(rows).reshape(2, capacity, 256)
            return carry

        lax.fori_loop(0, width // 256, narrow, 0)
        for index in blocks:
            other = partner_of(me, index)
            if index:
                copy = mesh_copy(
                    ready.at[index], home.at[me], back_send, back_recv, index, {"dp": other}
                )
            else:
                copy = pltpu.make_async_copy(ready.at[index], home.at[me], own.at[2])
            copy.start()
            coming.append(copy)

        if mode == "both":

            def finish(step, carry):
                columns = pl.ds(pl.multiple_of(step * 256, 256), 256)
                rows = low(dot(activity[pair], down[:, columns])).reshape(2, capacity, 256)
                sums = []
                for at, index in enumerate(blocks):
                    other = partner_of(me, index)
                    result[other, :, columns] = rows[at]
                    sums.append(
                        jnp.sum(
                            early[other, :, columns].astype(jnp.float32)
                            * rows[at].astype(jnp.float32),
                            axis=1,
                            keepdims=True,
                        )
                    )
                return tuple(old + new for old, new in zip(carry, sums))

            zero = jnp.zeros((capacity, 1), jnp.float32)
            totals = lax.fori_loop(0, width // 256, finish, (zero, zero))
            for at, index in enumerate(blocks):
                other = partner_of(me, index)
                place_out[index, :, :capacity] = flip_column(totals[at])
                if index:
                    copy = mesh_copy(
                        place_out.at[index],
                        places.at[me],
                        place_send,
                        place_recv,
                        index,
                        {"dp": other},
                    )
                else:
                    copy = pltpu.make_async_copy(place_out.at[index], places.at[me], own.at[3])
                copy.start()
                coming.append(copy)

    for index in range(1, owners):
        going[index].wait_send()
        if mode == "both":
            gate_going[index].wait_send()
    for copy in coming:
        copy.wait()


def experts_in_kernel(mode, sent, up_matrix, down_matrix, extra=()):
    owners, capacity, width = sent.shape
    hidden = up_matrix.shape[1]
    pairs = owners // 2
    low_type = jnp.bfloat16
    near = pl.BlockSpec(memory_space=pltpu.VMEM)
    far = pl.BlockSpec(memory_space=pl.ANY)
    rows = jax.ShapeDtypeStruct((owners, capacity, width), low_type)
    wide = jax.ShapeDtypeStruct((pairs, 2 * capacity, hidden), low_type)
    wide_scratch = pltpu.VMEM((pairs, 2 * capacity, hidden), low_type)
    lines = -(-capacity // LANES) * LANES
    line = jax.ShapeDtypeStruct((owners, 1, lines), jnp.float32)
    line_scratch = pltpu.VMEM((owners, 1, lines), jnp.float32)
    many = pltpu.SemaphoreType.DMA((owners,))
    if mode == "forward":
        ins, outs = [near, far, far], [(rows, near), (rows, near), (wide, far), (wide, far)]
        scratch = [wide_scratch] * 2
    elif mode == "backward":
        ins, outs = [near, far, far, far], [(rows, near), (rows, near), (wide, far)]
        scratch = [wide_scratch] * 2
    else:
        ins = [near, far, far, near, near]
        outs = [(rows, near), (rows, near), (wide, far), (wide, far)]
        outs += [(rows, near), (rows, near), (line, near)]
        scratch = [wide_scratch] * 2 + [line_scratch] * 2
    return pl.pallas_call(
        functools.partial(run_experts, mode, 512),
        out_shape=tuple(shape for shape, _ in outs),
        in_specs=ins,
        out_specs=tuple(spec for _, spec in outs),
        scratch_shapes=[
            pltpu.VMEM(up_matrix.shape, low_type),
            pltpu.VMEM(down_matrix.shape, low_type),
            pltpu.VMEM((owners, capacity, width), low_type),
        ]
        + scratch
        + [
            pltpu.SemaphoreType.DMA((3,)),
            pltpu.SemaphoreType.DMA((4,)),
            pltpu.SemaphoreType.DMA((2 * pairs,)),
        ]
        + [many] * (8 if mode == "both" else 4),
        compiler_params=pltpu.CompilerParams(
            collective_id={"forward": 2, "backward": 3, "both": 4}[mode],
            has_side_effects=True,
            vmem_limit_bytes=56 << 20,
        ),
        name="experts_" + mode,
    )(sent, up_matrix, down_matrix, *extra)


def plan_routes(routes, experts, capacity):
    length = routes.shape[0]
    flat = routes.reshape(-1)
    selector = flat[:, None] == jnp.arange(experts, dtype=jnp.int32)[None, :]
    running = jnp.cumsum(selector.astype(jnp.int32), axis=0)
    rank = jnp.sum(jnp.where(selector, running, 0), axis=1) - 1
    slot = (flat * capacity + rank).reshape(length, TOP).T.reshape(-1)
    place = jnp.arange(experts * capacity, dtype=jnp.int32)
    taken = slot[None, :] == place[:, None]
    pick = low(taken)
    both = sum(pick[:, choice * length : (choice + 1) * length] for choice in range(TOP))
    chosen = routes[:, :, None] == jnp.arange(experts, dtype=jnp.int32)[None, None, :]
    return taken, pick, both, chosen


def exchange(values):
    return lax.all_to_all(values, "dp", split_axis=0, concat_axis=0, tiled=True)


def exchange_rows(values, experts):
    rows, width = values.shape
    return exchange(values.reshape(experts, rows // experts, width)).reshape(rows, width)


def exchange_numbers(values, experts):
    return exchange(values.reshape(experts, 1, -1)).reshape(-1)


def gather_rows(pick, returned, gates):
    length = gates.shape[0]
    routed = low(dot_first(pick, returned)).reshape(TOP, length, -1)
    update = sum(
        gates[:, choice : choice + 1] * routed[choice].astype(jnp.float32) for choice in range(TOP)
    )
    return routed, update


def pack_small(router, attention_gain, expert_gain, bias):
    rows = router.shape[0]
    flat = bias.reshape(-1)
    column = jnp.concatenate([flat, jnp.zeros((rows - flat.shape[0],), flat.dtype)])
    block = jnp.concatenate(
        [router, attention_gain[:, None], expert_gain[:, None], column[:, None]], axis=1
    )
    return jnp.pad(block, ((0, 0), (0, -block.shape[1] % LANES)))


def unpack_small(block, experts, shards, heads):
    router = block[:, :experts]
    attention_gain = block[:, experts]
    expert_gain = block[:, experts + 1]
    column = block[:, experts + 2].reshape(shards, -1)
    bias = column[:, : heads // shards * NB].reshape(heads, NB)
    return router, attention_gain, expert_gain, bias


def per_device(
    tokens,
    query_weight,
    key_weight,
    value_weight,
    projection,
    router_weight,
    attention_gain,
    expert_gain,
    position_bias,
    expert_up,
    expert_down,
    routes,
    cotangent,
):
    layers = query_weight.shape[0]
    length, width = tokens.shape
    shards = lax.axis_size("fsdp")
    owners = lax.axis_size("dp")
    experts = owners * EXP_DEV
    heads = position_bias.shape[1] * shards
    capacity = max(2, 9 * length * TOP // (8 * experts))
    fused = shards == 4 and owners == 8 and capacity % 16 == 0 and layers == 2
    taken, pick, both, chosen = plan_routes(routes, experts, capacity)
    offsets = offset_selector(length)

    gathered = []
    for layer in range(layers):
        small = pack_small(
            router_weight[layer], attention_gain[layer], expert_gain[layer], position_bias[layer]
        )
        first = jnp.concatenate(
            [query_weight[layer], key_weight[layer], value_weight[layer], small], axis=1
        )
        first = lax.all_gather(first, "fsdp", axis=0, tiled=True)
        second = lax.all_gather(projection[layer], "fsdp", axis=0, tiled=True)
        gathered.append((first, second))

    early = exchange_rows(low(dot(both, cotangent)), experts)

    hidden = tokens.astype(jnp.float32)
    mixers = []
    saved = []
    for layer in range(layers):
        first, projection_full = gathered[layer]
        if layer:
            hidden, first, projection_full = lax.optimization_barrier(
                (hidden, first, projection_full)
            )
        router, gain_attention, gain_expert, bias = unpack_small(
            first[:, 3 * width :], experts, shards, heads
        )
        gain_attention = gain_attention.astype(jnp.float32)
        gain_expert = gain_expert.astype(jnp.float32)
        table = lax.dot_general(
            bias.astype(jnp.float32), offsets, contract_last, precision=highest
        )
        joined_weight = first[:, : 3 * width]
        mixers.append((joined_weight, projection_full, router, gain_attention, gain_expert, table))
        up_matrix, down_matrix = expert_up[layer, 0], expert_down[layer, 0]
        scale = row_scale(hidden)
        normed = low(hidden * scale * gain_attention)
        joined = low(dot(normed, joined_weight))
        mixed, log_total = attention_forward(joined, table, heads)
        if layer == 0:
            mixed, early = lax.optimization_barrier((mixed, early))
        middle = hidden + dot(mixed, projection_full)
        scale_expert = row_scale(middle)
        normed_expert = low(middle * scale_expert * gain_expert)
        logits = dot(normed_expert, router)
        picked = jnp.sum(jnp.where(chosen, logits[:, None, :], 0.0), axis=-1)
        gates = jax.nn.softmax(picked, axis=-1)
        gate_line = gates.T.reshape(-1)
        sent = low(dot(both, normed_expert))
        slope = None
        if fused and layer < layers - 1:
            returned, received, activity, slope = experts_in_kernel(
                "forward", sent.reshape(experts, capacity, width), up_matrix, down_matrix
            )
            returned = returned.reshape(-1, width)
            received = received.reshape(-1, width)
            activity = activity.reshape(received.shape[0], -1)
        elif fused:
            gate_places = jnp.sum(jnp.where(taken, gate_line[None, :], 0.0), axis=1)
            gate_places = gate_places.reshape(experts, 1, capacity)
            gate_places = jnp.pad(gate_places, ((0, 0), (0, 0), (0, -capacity % LANES)))
            back_rows, received, activity, back_inner, back_sent, result, back_places = (
                experts_in_kernel(
                    "both",
                    sent.reshape(experts, capacity, width),
                    up_matrix,
                    down_matrix,
                    (gate_places, early.reshape(experts, capacity, width)),
                )
            )
            count = experts * capacity
            last = (
                back_places[:, 0, :capacity].reshape(-1),
                back_sent.reshape(count, width),
                back_inner.reshape(count, -1),
                back_rows.reshape(count, width),
            )
            received = received.reshape(count, width)
            activity = activity.reshape(count, -1)
            returned = exchange_rows(result.reshape(count, width), experts)
        else:
            received = exchange_rows(sent, experts)
            if layer == layers - 1:
                gate_places = exchange_numbers(
                    jnp.sum(jnp.where(taken, gate_line[None, :], 0.0), axis=1), experts
                )
                received, gate_places = lax.optimization_barrier((received, gate_places))
            inner = dot(received, up_matrix)
            activity, slope = smooth_pair(inner)
            activity = low(activity)
            result = low(dot(activity, down_matrix))
            if layer == layers - 1:
                back_places = jnp.sum(early.astype(jnp.float32) * result.astype(jnp.float32), axis=1)
                back_places = exchange_numbers(back_places, experts)
                back_sent = low(gate_places[:, None] * early.astype(jnp.float32))
                back_inner = low(dot_last(back_sent, down_matrix) * slope)
                back_rows, back_sent = lax.optimization_barrier(
                    (low(dot_last(back_inner, up_matrix)), back_sent)
                )
                back_rows = exchange_rows(back_rows, experts)
                last = (back_places, back_sent, back_inner, back_rows)
            returned = exchange_rows(result, experts)
        routed = None
        if layer < layers - 1:
            routed, update = gather_rows(pick, returned, gates)
        saved.append(
            (
                hidden,
                scale,
                normed,
                joined,
                mixed,
                log_total,
                middle,
                scale_expert,
                normed_expert,
                gates,
                received,
                activity,
                slope,
                routed,
            )
        )
        if layer < layers - 1:
            hidden = middle + update

    back_out = cotangent.astype(jnp.float32)
    mixer_results = [None] * layers
    expert_results = [None] * layers
    above = None
    for layer in range(layers - 1, -1, -1):
        joined_weight, projection_full, router, gain_attention, gain_expert, table = mixers[layer]
        up_matrix, down_matrix = expert_up[layer, 0], expert_down[layer, 0]
        (
            hidden,
            scale,
            normed,
            joined,
            mixed,
            log_total,
            middle,
            scale_expert,
            normed_expert,
            gates,
            received,
            activity,
            slope,
            routed,
        ) = saved[layer]
        if layer == layers - 1:
            back_places, back_sent, back_inner, back_rows = last
            back_gates = jnp.sum(jnp.where(taken, back_places[:, None], 0.0), axis=0)
            back_gates = back_gates.reshape(TOP, length).T
        else:
            back_gates = jnp.stack(
                [
                    jnp.sum(back_out * routed[choice].astype(jnp.float32), axis=-1)
                    for choice in range(TOP)
                ],
                axis=1,
            )
            gated = jnp.concatenate(
                [low(gates[:, choice : choice + 1] * back_out) for choice in range(TOP)], axis=0
            )
            back_sent = low(dot(pick, gated))
            up_above, down_above = expert_results[layer + 1]
            if fused:
                back_rows, back_sent, back_inner = experts_in_kernel(
                    "backward",
                    back_sent.reshape(experts, capacity, width),
                    up_matrix,
                    down_matrix,
                    (slope,),
                )
                back_rows, back_sent, up_above, above = lax.optimization_barrier(
                    (back_rows, back_sent, up_above, above)
                )
                back_rows = back_rows.reshape(-1, width)
                back_sent = back_sent.reshape(-1, width)
                back_inner = back_inner.reshape(back_sent.shape[0], -1)
            else:
                back_sent = exchange_rows(back_sent, experts)
                back_sent, up_above = lax.optimization_barrier((back_sent, up_above))
                back_inner = low(dot_last(back_sent, down_matrix) * slope)
                back_inner, above = lax.optimization_barrier((back_inner, above))
                back_rows, back_sent = lax.optimization_barrier(
                    (low(dot_last(back_inner, up_matrix)), back_sent)
                )
                back_rows = exchange_rows(back_rows, experts)
            expert_results[layer + 1] = (up_above, down_above)
            if not fused:
                mixer_results[layer + 1] = lax.psum(above, "dp")
        down_change = low(dot_first(activity, back_sent))
        up_change = low(dot_first(received, back_inner))
        expert_results[layer] = tuple(
            lax.psum_scatter(change, "fsdp", scatter_dimension=0, tiled=True)
            for change in (up_change, down_change)
        )
        back_rows, down_change, up_change = lax.optimization_barrier(
            (back_rows, down_change, up_change)
        )
        back_picked = gates * (back_gates - jnp.sum(gates * back_gates, axis=-1, keepdims=True))
        back_logits = low(jnp.sum(jnp.where(chosen, back_picked[:, :, None], 0.0), axis=1))
        router_change = dot_first(normed_expert, back_logits)
        back_expert = dot_first(both, back_rows) + dot_last(back_logits, router)
        rows, expert_gain_change = norm_back(middle, scale_expert, gain_expert, back_expert)
        back_middle = back_out + rows
        back_attended = low(back_middle)
        back_mixed = low(dot_last(back_attended, projection_full))
        back_query, back_key, back_value, sums = attention_backward(
            joined, table, log_total, back_mixed, heads
        )
        if layer == layers - 1:
            back_query, returned = lax.optimization_barrier((back_query, returned))
            output = low(middle + gather_rows(pick, returned, gates)[1])
        if layer > 0:
            up_shard, down_shard = expert_results[layer]
            back_query, back_key, back_value, down_shard = lax.optimization_barrier(
                (back_query, back_key, back_value, down_shard)
            )
            expert_results[layer] = (up_shard, down_shard)
        bias_change = jnp.dot(sums, offsets, precision=highest)
        projection_change = dot_first(mixed, back_attended)
        parts = (back_query, back_key, back_value)
        changes = [low(dot_first(normed, part)) for part in parts]
        back_normed = sum(
            dot_last(part, joined_weight[:, index * width : (index + 1) * width])
            for index, part in enumerate(parts)
        )
        rows, attention_gain_change = norm_back(hidden, scale, gain_attention, back_normed)
        back_out = back_middle + rows
        changes = [
            change.reshape(shards, width // shards, width)
            for change in changes + [low(projection_change)]
        ]
        small = jnp.concatenate(
            [
                change.reshape(shards, -1)
                for change in (
                    router_change,
                    attention_gain_change,
                    expert_gain_change,
                    bias_change,
                )
            ],
            axis=1,
        )
        small = low(jnp.pad(small, ((0, 0), (0, -small.shape[1] % (16 * width)))))
        small = small.reshape(shards, -1, width)
        if layer == 0 and fused:
            summed, narrow = reduce_in_kernel(changes, small, above, owners)
        else:
            packed = jnp.concatenate(changes + [small], axis=1)
            above = lax.psum_scatter(packed, "fsdp", scatter_dimension=0)
            if layer == 0:
                mixer_results[layer] = lax.psum(above, "dp")

    rows = width // shards
    counts = (rows * experts, rows, rows, heads // shards * NB)
    if fused:
        mixer_gradients = [summed[index] for index in range(4)]
        flat = narrow.reshape(layers, -1)
    else:
        mixer_results = jnp.stack(lax.optimization_barrier(mixer_results)).astype(jnp.float32)
        mixer_gradients = [
            mixer_results[:, index * rows : (index + 1) * rows] for index in range(4)
        ]
        flat = mixer_results[:, 4 * rows :].reshape(layers, -1)
    ends = [sum(counts[: index + 1]) for index in range(4)]
    small_gradients = [flat[:, end - count : end] for end, count in zip(ends, counts)]
    router_gradient = small_gradients[0].reshape(layers, rows, experts)
    bias_gradient = small_gradients[3].reshape(position_bias.shape)
    up_stack, down_stack = (
        jnp.stack([results[index].astype(jnp.float32) for results in expert_results])[:, None]
        for index in range(2)
    )
    return (
        output,
        back_out,
        *mixer_gradients,
        router_gradient,
        small_gradients[1],
        small_gradients[2],
        bias_gradient,
        up_stack,
        down_stack,
    )


def solution(mesh):
    return jax.shard_map(
        per_device,
        mesh=mesh,
        in_specs=(
            P(("dp", "fsdp"), None),
            P(None, "fsdp", None),
            P(None, "fsdp", None),
            P(None, "fsdp", None),
            P(None, "fsdp", None),
            P(None, "fsdp", None),
            P(None, "fsdp"),
            P(None, "fsdp"),
            P(None, "fsdp", None),
            P(None, "dp", None, None),
            P(None, "dp", None, None),
            P(("dp", "fsdp"), None),
            P(("dp", "fsdp"), None),
        ),
        out_specs=(
            P(("dp", "fsdp"), None),
            P(("dp", "fsdp"), None),
            P(None, "fsdp", None),
            P(None, "fsdp", None),
            P(None, "fsdp", None),
            P(None, "fsdp", None),
            P(None, "fsdp", None),
            P(None, "fsdp"),
            P(None, "fsdp"),
            P(None, "fsdp", None),
            P(None, "dp", "fsdp", None),
            P(None, "dp", "fsdp", None),
        ),
        check_vma=False,
    )
```

```python
import functools

import jax
import jax.numpy as jnp
from jax import lax
from jax.experimental import pallas as pl
from jax.experimental.pallas import tpu as pltpu
from jax.sharding import PartitionSpec as P


EXP_DEV = 1
TOP = 2
BLOCK = 256
NB = 32
LANES = 128


epsilon = 1e-06
edges = (1, 2, 3, 4, 5, 6, 7, 8, 12, 16, 24, 32, 64, 128, 256)
highest = lax.Precision.HIGHEST
contract_first = (((0,), (0,)), ((), ()))
contract_last = (((1,), (1,)), ((), ()))
root = 0.7978845608028654
cubic = 0.044715


def dot(left, right):
    return jnp.dot(left, right, preferred_element_type=jnp.float32)


def dot_last(left, right):
    return lax.dot_general(left, right, contract_last, preferred_element_type=jnp.float32)


def dot_first(left, right):
    return lax.dot_general(left, right, contract_first, preferred_element_type=jnp.float32)


def low(values):
    return values.astype(jnp.bfloat16)


def row_scale(values):
    return lax.rsqrt(jnp.mean(values * values, axis=-1, keepdims=True) + epsilon)


def norm_back(values, scale, gain, back):
    lifted = back * gain
    inner = jnp.mean(lifted * values, axis=-1, keepdims=True)
    rows = scale * lifted - scale * scale * scale * values * inner
    return rows, jnp.sum(back * values * scale, axis=0)


def smooth_pair(values):
    tail = jnp.tanh(root * (values + cubic * values * values * values))
    half = 0.5 * (1.0 + tail)
    slope = half + 0.5 * values * (1.0 - tail * tail) * root * (1.0 + 3.0 * cubic * values * values)
    return values * half, slope


def offset_selector(length):
    offset = jnp.arange(2 * length, dtype=jnp.int32) - (length - 1)
    distance = jnp.abs(offset)
    bucket = jnp.zeros_like(offset)
    for edge in edges:
        bucket = bucket + (distance >= edge).astype(jnp.int32)
    bucket = bucket + NB // 2 * (offset > 0).astype(jnp.int32)
    return (bucket[:, None] == jnp.arange(NB, dtype=jnp.int32)[None, :]).astype(jnp.float32)


def lane_of(half, heads):
    lanes = lax.broadcasted_iota(jnp.int32, (1, LANES), 1)
    size = LANES // heads
    return (lanes >= half * size) & (lanes < (half + 1) * size)


def bias_tile(table, start, block, keys):
    span = table.shape[1]
    length = span // 2
    spread = jnp.broadcast_to(table, (block, span))
    shift = (start - (length - 1)) % span
    return pltpu.roll(spread, shift, 1, stride=1, stride_axis=0)[:, :keys]


def attend(pair, scale, q_ref, k_ref, v_ref, table_ref, mixed_ref, log_ref):
    length = q_ref.shape[0]
    for start in range(0, length, BLOCK):
        keys = start + BLOCK
        rows = pl.ds(start, BLOCK)
        query = q_ref[rows, :]
        key = k_ref[pl.ds(0, keys), :]
        value = v_ref[pl.ds(0, keys), :]
        mixed = None
        for half in range(pair):
            lane = lane_of(half, pair)
            table = table_ref[0, half : half + 1, :]
            raw = dot_last(jnp.where(lane, query, jnp.zeros_like(query)), key)
            scores = scale * raw + bias_tile(table, start, BLOCK, keys)
            peak = jnp.max(scores, axis=-1, keepdims=True)
            lifted = jnp.exp(scores - peak)
            total = jnp.sum(lifted, axis=-1, keepdims=True)
            shares = low(lifted * (1.0 / total))
            part = dot(shares, value)
            tops = jnp.broadcast_to(peak + jnp.log(total), part.shape)
            mixed = part if mixed is None else jnp.where(lane, part, mixed)
            logs = tops if half == 0 else jnp.where(lane, tops, logs)
        mixed_ref[rows, :] = low(mixed)
        log_ref[rows, :] = logs


def attend_back(
    pair,
    scale,
    q_ref,
    k_ref,
    v_ref,
    table_ref,
    log_ref,
    back_ref,
    dq_ref,
    dk_ref,
    dv_ref,
    sums_ref,
    key_sum,
    value_sum,
):
    length = q_ref.shape[0]
    size = LANES // pair
    span = 2 * length
    order = list(range(0, length, BLOCK))[::-1]
    for turn, start in enumerate(order):
        keys = start + BLOCK
        rows = pl.ds(start, BLOCK)
        query = q_ref[rows, :]
        back = back_ref[rows, :]
        key = k_ref[pl.ds(0, keys), :]
        value = v_ref[pl.ds(0, keys), :]
        back_query = None
        for half in range(pair):
            lane = lane_of(half, pair)
            table = table_ref[0, half : half + 1, :]
            query_half = jnp.where(lane, query, jnp.zeros_like(query))
            back_half = jnp.where(lane, back, jnp.zeros_like(back))
            raw = dot_last(query_half, key)
            scores = scale * raw + bias_tile(table, start, BLOCK, keys)
            shares = jnp.exp(scores - log_ref[rows, half * size : half * size + 1])
            back_shares = dot_last(back_half, value)
            weighted = shares * back_shares
            back_scores = weighted - shares * jnp.sum(weighted, axis=-1, keepdims=True)
            back_raw = low(scale * back_scores)
            part = dot(back_raw, key)
            back_query = part if back_query is None else jnp.where(lane, part, back_query)
            key_part = dot_first(back_raw, query_half)
            value_part = dot_first(low(shares), back_half)
            if turn == 0 and half == 0:
                key_sum[pl.ds(0, keys), :] = key_part
                value_sum[pl.ds(0, keys), :] = value_part
            else:
                key_sum[pl.ds(0, keys), :] += key_part
                value_sum[pl.ds(0, keys), :] += value_part
            first = length - 1 - start
            lines = jnp.zeros((8, span), jnp.float32)
            wide = jnp.concatenate(
                [back_scores, jnp.zeros((BLOCK, span - keys), jnp.float32)], axis=1
            )
            for tile in range(BLOCK // 8):
                piece = wide[tile * 8 : tile * 8 + 8, :]
                lines = lines + pltpu.roll(piece, (first - tile * 8) % span, 1)
            line = lines[0:1, :]
            for step in range(1, 8):
                line = line + pltpu.roll(lines[step : step + 1, :], span - step, 1)
            if turn == 0:
                sums_ref[0, half : half + 1, :] = line
            else:
                sums_ref[0, half : half + 1, :] += line
        dq_ref[rows, :] = low(back_query)
    dk_ref[...] = low(key_sum[...])
    dv_ref[...] = low(value_sum[...])


def attention_specs(length, heads, size):
    pair = LANES // size
    groups = heads // pair

    def column(offset):
        return pl.BlockSpec((length, LANES), lambda g: (0, g + offset))

    table = pl.BlockSpec((1, pair, 2 * length), lambda g: (g, 0, 0))
    return pair, groups, column, table


def attention_forward(joined, table, heads):
    length, width = joined.shape[0], joined.shape[1] // 3
    size = width // heads
    pair, groups, column, table_spec = attention_specs(length, heads, size)
    return pl.pallas_call(
        functools.partial(attend, pair, size**-0.5),
        grid=(groups,),
        out_shape=(
            jax.ShapeDtypeStruct((length, width), jnp.bfloat16),
            jax.ShapeDtypeStruct((length, width), jnp.float32),
        ),
        in_specs=[column(0), column(groups), column(2 * groups), table_spec],
        out_specs=(column(0), column(0)),
        compiler_params=pltpu.CompilerParams(vmem_limit_bytes=32 << 20),
        cost_estimate=pl.CostEstimate(
            flops=4 * length * length * width,
            bytes_accessed=length * width * 12,
            transcendentals=length * length * heads,
        ),
        name="attend",
    )(joined, joined, joined, table.reshape(groups, pair, 2 * length))


def attention_backward(joined, table, log_total, back_mixed, heads):
    length, width = back_mixed.shape
    size = width // heads
    pair, groups, column, table_spec = attention_specs(length, heads, size)
    rows = jax.ShapeDtypeStruct((length, width), jnp.bfloat16)
    back_query, back_key, back_value, sums = pl.pallas_call(
        functools.partial(attend_back, pair, size**-0.5),
        grid=(groups,),
        out_shape=(
            rows,
            rows,
            rows,
            jax.ShapeDtypeStruct((groups, pair, 2 * length), jnp.float32),
        ),
        in_specs=[
            column(0),
            column(groups),
            column(2 * groups),
            table_spec,
            column(0),
            column(0),
        ],
        out_specs=(column(0), column(0), column(0), table_spec),
        scratch_shapes=[pltpu.VMEM((length, LANES), jnp.float32)] * 2,
        compiler_params=pltpu.CompilerParams(vmem_limit_bytes=32 << 20),
        cost_estimate=pl.CostEstimate(
            flops=10 * length * length * width,
            bytes_accessed=length * width * 20,
            transcendentals=length * length * heads,
        ),
        name="attend_back",
    )(joined, joined, joined, table.reshape(groups, pair, 2 * length), log_total, back_mixed)
    return back_query, back_key, back_value, sums.reshape(heads, 2 * length)


def mesh_copy(source, target, sends, receives, where, device):
    return pltpu.make_async_remote_copy(
        src_ref=source,
        dst_ref=target,
        send_sem=sends.at[where],
        recv_sem=receives.at[where],
        device_id=device,
        device_id_type=pl.DeviceIdType.MESH,
    )


def reduce_mixer(chunks, *refs):
    q_ref, k_ref, v_ref, p_ref, small_ref, above, out_ref, narrow_ref = refs[:8]
    core_in, side_out, side_in, keep, cross_in, half, line_in, whole, other_half, small_in = refs[
        8:18
    ]
    core_send, core_recv, side_send, side_recv = refs[18:22]
    x1_send, x1_recv, z1_send, z1_recv, z2_send, z2_recv, x2_send, x2_recv = refs[22:30]
    small_send, small_recv = refs[30:32]
    owners = small_in.shape[1]
    me = lax.axis_index("dp")
    place = lax.axis_index("fsdp")
    core, side = lax.rem(place, 2), place // 2
    partner = 2 * side + (1 - core)
    across = 2 * (1 - side) + core
    x, z = lax.rem(me, 2), me // 2
    x_peer = me + 1 - 2 * x
    depth = owners // 2
    inputs = (q_ref, k_ref, v_ref, p_ref, small_ref)
    rows = q_ref.shape[1]
    spare = small_ref.shape[1]
    main = 4 * rows
    quarter = main // 2
    block = quarter // depth
    columns = q_ref.shape[2] // chunks
    spans = [(index * rows, ref.shape[1]) for index, ref in enumerate(inputs)]
    sources = (keep, above)

    barrier = pltpu.get_barrier_semaphore()
    for other in (partner, across):
        pl.semaphore_signal(
            barrier, inc=1, device_id={"fsdp": other}, device_id_type=pl.DeviceIdType.MESH
        )
    for step in range(1, owners):
        pl.semaphore_signal(
            barrier,
            inc=1,
            device_id={"dp": lax.rem(me + step, owners)},
            device_id_type=pl.DeviceIdType.MESH,
        )
    pl.semaphore_wait(barrier, owners + 1)

    def lanes_of(chunk):
        return pl.ds(chunk * columns, columns)

    def half_at(index):
        return pl.ds(pl.multiple_of(index * quarter, quarter), quarter)

    def block_at(index):
        return pl.ds(pl.multiple_of(index * block, block), block)

    live = {}

    def start(key, copies):
        for copy in copies:
            copy.start()
        live[key] = copies

    def finish(key):
        for copy in live.pop(key):
            copy.wait()

    def start_core(chunk):
        lanes = lanes_of(chunk)
        copies = []
        for turn in range(2):
            there = 1 - side if turn == 0 else side
            for index, (first, count) in enumerate(spans):
                copies.append(
                    mesh_copy(
                        inputs[index].at[2 * there + 1 - core, :, lanes],
                        core_in.at[turn, pl.ds(first, count), lanes],
                        core_send,
                        core_recv,
                        (chunk * 2 + turn) * 5 + index,
                        {"fsdp": partner},
                    )
                )
        start(("core", chunk), copies)

    def add_core(chunk):
        lanes = lanes_of(chunk)
        finish(("core", chunk))
        for turn in range(2):
            there = 1 - side if turn == 0 else side
            target = side_out if turn == 0 else keep
            for index, (first, count) in enumerate(spans):
                at = pl.ds(first, count)
                total = inputs[index][2 * there + core, :, lanes].astype(jnp.float32)
                total = total + core_in[turn, at, lanes].astype(jnp.float32)
                target[at, lanes] = low(total)
            if turn == 0:
                copy = mesh_copy(
                    side_out.at[:, lanes],
                    side_in.at[:, lanes],
                    side_send,
                    side_recv,
                    chunk,
                    {"fsdp": across},
                )
                start(("side", chunk), [copy])

    def start_cross(layer, chunk):
        lanes = lanes_of(chunk)
        unit = layer * chunks + chunk
        if layer == 0:
            finish(("side", chunk))
            keep[:, lanes] = low(
                keep[:, lanes].astype(jnp.float32) + side_in[:, lanes].astype(jnp.float32)
            )
        source = sources[layer]
        copies = [
            mesh_copy(
                source.at[half_at(1 - x), lanes],
                cross_in.at[layer, :, lanes],
                x1_send,
                x1_recv,
                unit,
                {"dp": x_peer},
            )
        ]
        start(("x1", unit), copies)
        copies = [
            mesh_copy(
                source.at[pl.ds(main, spare), lanes],
                small_in.at[layer, me, :, lanes],
                small_send,
                small_recv,
                unit * owners + step,
                {"dp": lax.rem(me + step, owners)},
            )
            for step in range(1, owners)
        ]
        start(("small", unit), copies)

    def add_cross(layer, chunk):
        lanes = lanes_of(chunk)
        unit = layer * chunks + chunk
        finish(("x1", unit))
        half[layer, :, lanes] = low(
            sources[layer][half_at(x), lanes].astype(jnp.float32)
            + cross_in[layer, :, lanes].astype(jnp.float32)
        )
        copies = []
        for step in range(1, depth):
            there = lax.rem(z + step, depth)
            copies.append(
                mesh_copy(
                    half.at[layer, block_at(there), lanes],
                    line_in.at[layer, step, :, lanes],
                    z1_send,
                    z1_recv,
                    unit * depth + step,
                    {"dp": 2 * there + x},
                )
            )
        start(("z1", unit), copies)

    def add_line(layer, chunk):
        lanes = lanes_of(chunk)
        unit = layer * chunks + chunk
        finish(("z1", unit))
        total = half[layer, block_at(z), lanes].astype(jnp.float32)
        for step in range(1, depth):
            total = total + line_in[layer, step, :, lanes].astype(jnp.float32)
        whole[layer, block_at(z), lanes] = low(total)
        copies = []
        for step in range(1, depth):
            there = lax.rem(z + step, depth)
            copies.append(
                mesh_copy(
                    whole.at[layer, block_at(z), lanes],
                    whole.at[layer, block_at(z), lanes],
                    z2_send,
                    z2_recv,
                    unit * depth + step,
                    {"dp": 2 * there + x},
                )
            )
        start(("z2", unit), copies)

    def return_cross(layer, chunk):
        lanes = lanes_of(chunk)
        unit = layer * chunks + chunk
        finish(("z2", unit))
        copy = mesh_copy(
            whole.at[layer, :, lanes],
            other_half.at[layer, :, lanes],
            x2_send,
            x2_recv,
            unit,
            {"dp": x_peer},
        )
        start(("x2", unit), [copy])

    def write(layer, chunk):
        lanes = lanes_of(chunk)
        unit = layer * chunks + chunk
        finish(("x2", unit))
        for index in range(2):
            at = pl.ds(index * rows, rows)
            out_ref[2 * x + index, layer, :, lanes] = whole[layer, at, lanes].astype(jnp.float32)
            out_ref[2 * (1 - x) + index, layer, :, lanes] = other_half[layer, at, lanes].astype(
                jnp.float32
            )
        finish(("small", unit))
        small_in[layer, me, :, lanes] = sources[layer][pl.ds(main, spare), lanes]
        narrow = small_in[layer, 0, :, lanes].astype(jnp.float32)
        for other in range(1, owners):
            narrow = narrow + small_in[layer, other, :, lanes].astype(jnp.float32)
        narrow_ref[layer, :, lanes] = narrow

    for chunk in range(chunks):
        start_core(chunk)
    for chunk in range(chunks):
        start_cross(1, chunk)
    for chunk in range(chunks):
        add_core(chunk)
        add_cross(1, chunk)
    for chunk in range(chunks):
        add_line(1, chunk)
    start_cross(0, 0)
    return_cross(1, 0)
    add_cross(0, 0)
    return_cross(1, 1)
    start_cross(0, 1)
    return_cross(1, 2)
    add_line(0, 0)
    add_cross(0, 1)
    for chunk in range(chunks):
        write(1, chunk)
    start_cross(0, 2)
    add_line(0, 1)
    add_cross(0, 2)
    return_cross(0, 0)
    return_cross(0, 1)
    add_line(0, 2)
    write(0, 0)
    return_cross(0, 2)
    write(0, 1)
    write(0, 2)


def reduce_in_kernel(changes, small, above, owners):
    _, rows, width = changes[0].shape
    spare = small.shape[1]
    main = 4 * rows
    total = main + spare
    block = main // owners
    chunks = 3
    units = 2 * chunks
    low_type = jnp.bfloat16
    space = pl.BlockSpec(memory_space=pltpu.VMEM)
    return pl.pallas_call(
        functools.partial(reduce_mixer, chunks),
        out_shape=(
            jax.ShapeDtypeStruct((4, 2, rows, width), jnp.float32),
            jax.ShapeDtypeStruct((2, spare, width), jnp.float32),
        ),
        in_specs=[space] * 6,
        out_specs=(space, space),
        scratch_shapes=[
            pltpu.VMEM((2, total, width), low_type),
            pltpu.VMEM((total, width), low_type),
            pltpu.VMEM((total, width), low_type),
            pltpu.VMEM((total, width), low_type),
            pltpu.VMEM((2, main // 2, width), low_type),
            pltpu.VMEM((2, main // 2, width), low_type),
            pltpu.VMEM((2, owners // 2, block, width), low_type),
            pltpu.VMEM((2, main // 2, width), low_type),
            pltpu.VMEM((2, main // 2, width), low_type),
            pltpu.VMEM((2, owners, spare, width), low_type),
        ]
        + [pltpu.SemaphoreType.DMA((10 * chunks,))] * 2
        + [pltpu.SemaphoreType.DMA((chunks,))] * 2
        + [pltpu.SemaphoreType.DMA((units,))] * 2
        + [pltpu.SemaphoreType.DMA((units * owners // 2,))] * 4
        + [pltpu.SemaphoreType.DMA((units,))] * 2
        + [pltpu.SemaphoreType.DMA((units * owners,))] * 2,
        compiler_params=pltpu.CompilerParams(
            collective_id=1, has_side_effects=True, vmem_limit_bytes=48 << 20
        ),
        name="reduce_mixer",
    )(*changes, small, above)


def partner_of(me, index):
    other = me
    for bit, weight in ((1, 1), (2, 4), (4, 2)):
        if index & bit:
            other = other + weight * (1 - 2 * (lax.rem(me // weight, 2)))
    return other


def flip_row(row):
    count = row.shape[1]
    down = lax.broadcasted_iota(jnp.int32, (count, count), 0)
    along = lax.broadcasted_iota(jnp.int32, (count, count), 1)
    return jnp.sum(jnp.where(down == along, row, 0.0), axis=1, keepdims=True)


def flip_column(column):
    count = column.shape[0]
    down = lax.broadcasted_iota(jnp.int32, (count, count), 0)
    along = lax.broadcasted_iota(jnp.int32, (count, count), 1)
    return jnp.sum(jnp.where(down == along, column, 0.0), axis=0, keepdims=True)


def run_experts(mode, tile, *refs):
    refs = list(refs)

    def take(count):
        taken = refs[:count]
        del refs[:count]
        return taken

    sent, up_any, down_any = take(3)
    if mode == "forward":
        home, rows_in, activity_any, slope_any = take(4)
    elif mode == "backward":
        slope_any, activity_any, rows_before = take(3)
        home, rows_in, up_any_out, down_any_out = take(4)
    else:
        gates, early = take(2)
        home, rows_in, result, places, up_any_out, down_any_out = take(6)
    up, down, ready = take(3)
    if mode == "forward":
        activity, slope = take(2)
        outs = [(activity, activity_any), (slope, slope_any)]
    elif mode == "backward":
        slope, inner, activity, up_out, down_out = take(5)
        outs = []
    else:
        activity, inner, gates_in, place_out, scaled, up_out, down_out = take(7)
        outs = []
    load, own, stores, go_send, go_recv, back_send, back_recv = take(7)
    if mode == "both":
        gate_send, gate_recv, place_send, place_recv = take(4)

    owners, capacity, width = sent.shape
    hidden = up.shape[1]
    me = lax.axis_index("dp")
    barrier = pltpu.get_barrier_semaphore()
    for index in range(1, owners):
        pl.semaphore_signal(
            barrier,
            inc=1,
            device_id={"dp": partner_of(me, index)},
            device_id_type=pl.DeviceIdType.MESH,
        )
    pl.semaphore_wait(barrier, owners - 1)

    going = {}
    gate_going = {}
    for index in range(1, owners):
        other = partner_of(me, index)
        copy = mesh_copy(
            sent.at[other], rows_in.at[index], go_send, go_recv, index, {"dp": other}
        )
        copy.start()
        going[index] = copy
        if mode == "both":
            copy = mesh_copy(
                gates.at[other], gates_in.at[index], gate_send, gate_recv, index, {"dp": other}
            )
            copy.start()
            gate_going[index] = copy
    first = [pltpu.make_async_copy(sent.at[me], rows_in.at[0], own.at[0])]
    if mode == "both":
        first.append(pltpu.make_async_copy(gates.at[me], gates_in.at[0], own.at[1]))
    first.append(pltpu.make_async_copy(up_any, up, load.at[0]))
    first.append(pltpu.make_async_copy(down_any, down, load.at[1]))
    if mode == "backward":
        first.append(pltpu.make_async_copy(slope_any, slope, load.at[2]))
        first.append(pltpu.make_async_copy(activity_any, activity, load.at[3]))
    for copy in first:
        copy.start()

    coming = []
    for pair in range(owners // 2):
        blocks = (2 * pair, 2 * pair + 1)
        both = pl.ds(2 * pair, 2)
        count = 2 * capacity
        if pair == 0:
            for copy in first:
                copy.wait()
        for index in blocks:
            if index:
                going[index].wait_recv()
                if mode == "both":
                    gate_going[index].wait_recv()
        if mode == "both":
            for index in blocks:
                gate = flip_row(gates_in[index][:, :capacity])
                rows = early[partner_of(me, index)].astype(jnp.float32)
                scaled[index] = low(gate * rows)

        def widen(step, carry):
            columns = pl.ds(pl.multiple_of(step * tile, tile), tile)
            rows = rows_in[both].reshape(count, width)
            if mode == "backward":
                back = dot_last(rows, down[columns, :])
                inner[pair, :, columns] = low(back * slope[pair, :, columns].astype(jnp.float32))
                return carry
            value, steep = smooth_pair(dot(rows, up[:, columns]))
            activity[pair, :, columns] = low(value)
            if mode == "forward":
                slope[pair, :, columns] = low(steep)
            else:
                back = dot_last(scaled[both].reshape(count, width), down[columns, :])
                inner[pair, :, columns] = low(back * steep)
            return carry

        lax.fori_loop(0, hidden // tile, widen, 0)
        for at, (source, target) in enumerate(outs):
            copy = pltpu.make_async_copy(
                source.at[pair], target.at[pair], stores.at[at * (owners // 2) + pair]
            )
            copy.start()
            coming.append(copy)

        def narrow(step, carry):
            columns = pl.ds(pl.multiple_of(step * 256, 256), 256)
            if mode == "forward":
                rows = dot(activity[pair], down[:, columns])
            else:
                rows = dot_last(inner[pair], up[columns, :])
            ready[both, :, columns] = low(rows).reshape(2, capacity, 256)
            return carry

        lax.fori_loop(0, width // 256, narrow, 0)
        for index in blocks:
            other = partner_of(me, index)
            if index:
                copy = mesh_copy(
                    ready.at[index], home.at[me], back_send, back_recv, index, {"dp": other}
                )
            else:
                copy = pltpu.make_async_copy(ready.at[index], home.at[me], own.at[2])
            copy.start()
            coming.append(copy)

        if mode == "both":

            def finish(step, carry):
                columns = pl.ds(pl.multiple_of(step * 256, 256), 256)
                rows = low(dot(activity[pair], down[:, columns])).reshape(2, capacity, 256)
                sums = []
                for at, index in enumerate(blocks):
                    other = partner_of(me, index)
                    result[other, :, columns] = rows[at]
                    sums.append(
                        jnp.sum(
                            early[other, :, columns].astype(jnp.float32)
                            * rows[at].astype(jnp.float32),
                            axis=1,
                            keepdims=True,
                        )
                    )
                return tuple(old + new for old, new in zip(carry, sums))

            zero = jnp.zeros((capacity, 1), jnp.float32)
            totals = lax.fori_loop(0, width // 256, finish, (zero, zero))
            for at, index in enumerate(blocks):
                other = partner_of(me, index)
                place_out[index, :, :capacity] = flip_column(totals[at])
                if index:
                    copy = mesh_copy(
                        place_out.at[index],
                        places.at[me],
                        place_send,
                        place_recv,
                        index,
                        {"dp": other},
                    )
                else:
                    copy = pltpu.make_async_copy(place_out.at[index], places.at[me], own.at[3])
                copy.start()
                coming.append(copy)

    if mode != "forward":
        before = rows_before if mode == "backward" else rows_in
        back = rows_in if mode == "backward" else scaled
        part = hidden // 3

        for third in range(3):

            def change(step, carry):
                start = pl.multiple_of(third * part + step * 256, 256)
                columns = pl.ds(start, 256)
                count = owners * capacity
                down_out[columns, :] = low(
                    dot_first(
                        activity[:, :, columns].reshape(count, 256),
                        back[...].reshape(count, width),
                    )
                )
                up_out[:, columns] = low(
                    dot_first(
                        before[...].reshape(count, width),
                        inner[:, :, columns].reshape(count, 256),
                    )
                )
                return carry

            lax.fori_loop(0, part // 256, change, 0)
            some = pl.ds(third * part, part)
            for at, (source, target) in enumerate(
                (
                    (down_out.at[some, :], down_any_out.at[some, :]),
                    (up_out.at[:, some], up_any_out.at[:, some]),
                )
            ):
                copy = pltpu.make_async_copy(source, target, stores.at[2 * third + at])
                copy.start()
                coming.append(copy)

    for index in range(1, owners):
        going[index].wait_send()
        if mode == "both":
            gate_going[index].wait_send()
    for copy in coming:
        copy.wait()


def experts_in_kernel(mode, sent, up_matrix, down_matrix, extra=()):
    owners, capacity, width = sent.shape
    hidden = up_matrix.shape[1]
    pairs = owners // 2
    low_type = jnp.bfloat16
    near = pl.BlockSpec(memory_space=pltpu.VMEM)
    far = pl.BlockSpec(memory_space=pl.ANY)
    rows = jax.ShapeDtypeStruct((owners, capacity, width), low_type)
    wide = jax.ShapeDtypeStruct((pairs, 2 * capacity, hidden), low_type)
    wide_scratch = pltpu.VMEM((pairs, 2 * capacity, hidden), low_type)
    lines = -(-capacity // LANES) * LANES
    line = jax.ShapeDtypeStruct((owners, 1, lines), jnp.float32)
    line_scratch = pltpu.VMEM((owners, 1, lines), jnp.float32)
    many = pltpu.SemaphoreType.DMA((owners,))
    changes = [
        (jax.ShapeDtypeStruct(matrix.shape, low_type), far) for matrix in (up_matrix, down_matrix)
    ]
    change_scratch = [pltpu.VMEM(matrix.shape, low_type) for matrix in (up_matrix, down_matrix)]
    rows_scratch = pltpu.VMEM((owners, capacity, width), low_type)
    if mode == "forward":
        ins, outs = [near, far, far], [(rows, near), (rows, near), (wide, far), (wide, far)]
        scratch = [wide_scratch] * 2
    elif mode == "backward":
        ins, outs = [near, far, far, far, far, near], [(rows, near), (rows, near)] + changes
        scratch = [wide_scratch] * 3 + change_scratch
    else:
        ins = [near, far, far, near, near]
        outs = [(rows, near), (rows, near), (rows, near), (line, near)] + changes
        scratch = [wide_scratch] * 2 + [line_scratch] * 2 + [rows_scratch] + change_scratch
    return pl.pallas_call(
        functools.partial(run_experts, mode, 512),
        out_shape=tuple(shape for shape, _ in outs),
        in_specs=ins,
        out_specs=tuple(spec for _, spec in outs),
        scratch_shapes=[
            pltpu.VMEM(up_matrix.shape, low_type),
            pltpu.VMEM(down_matrix.shape, low_type),
            rows_scratch,
        ]
        + scratch
        + [
            pltpu.SemaphoreType.DMA((4,)),
            pltpu.SemaphoreType.DMA((4,)),
            pltpu.SemaphoreType.DMA((2 * pairs,)),
        ]
        + [many] * (8 if mode == "both" else 4),
        compiler_params=pltpu.CompilerParams(
            collective_id={"forward": 2, "backward": 3, "both": 4}[mode],
            has_side_effects=True,
            vmem_limit_bytes=60 << 20,
        ),
        cost_estimate=pl.CostEstimate(
            flops=80 * owners * capacity * width * hidden // 2,
            bytes_accessed=12 * width * hidden,
            transcendentals=0,
        ),
    )(sent, up_matrix, down_matrix, *extra)


def plan_routes(routes, experts, capacity):
    length = routes.shape[0]
    flat = routes.reshape(-1)
    selector = flat[:, None] == jnp.arange(experts, dtype=jnp.int32)[None, :]
    running = jnp.cumsum(selector.astype(jnp.int32), axis=0)
    rank = jnp.sum(jnp.where(selector, running, 0), axis=1) - 1
    slot = (flat * capacity + rank).reshape(length, TOP).T.reshape(-1)
    place = jnp.arange(experts * capacity, dtype=jnp.int32)
    taken = slot[None, :] == place[:, None]
    pick = low(taken)
    both = sum(pick[:, choice * length : (choice + 1) * length] for choice in range(TOP))
    chosen = routes[:, :, None] == jnp.arange(experts, dtype=jnp.int32)[None, None, :]
    return taken, pick, both, chosen


def exchange(values):
    return lax.all_to_all(values, "dp", split_axis=0, concat_axis=0, tiled=True)


def exchange_rows(values, experts):
    rows, width = values.shape
    return exchange(values.reshape(experts, rows // experts, width)).reshape(rows, width)


def exchange_numbers(values, experts):
    return exchange(values.reshape(experts, 1, -1)).reshape(-1)


def gather_rows(pick, returned, gates):
    length = gates.shape[0]
    routed = low(dot_first(pick, returned)).reshape(TOP, length, -1)
    update = sum(
        gates[:, choice : choice + 1] * routed[choice].astype(jnp.float32) for choice in range(TOP)
    )
    return routed, update


def pack_small(router, attention_gain, expert_gain, bias):
    rows = router.shape[0]
    flat = bias.reshape(-1)
    column = jnp.concatenate([flat, jnp.zeros((rows - flat.shape[0],), flat.dtype)])
    block = jnp.concatenate(
        [router, attention_gain[:, None], expert_gain[:, None], column[:, None]], axis=1
    )
    return jnp.pad(block, ((0, 0), (0, -block.shape[1] % LANES)))


def unpack_small(block, experts, shards, heads):
    router = block[:, :experts]
    attention_gain = block[:, experts]
    expert_gain = block[:, experts + 1]
    column = block[:, experts + 2].reshape(shards, -1)
    bias = column[:, : heads // shards * NB].reshape(heads, NB)
    return router, attention_gain, expert_gain, bias


def per_device(
    tokens,
    query_weight,
    key_weight,
    value_weight,
    projection,
    router_weight,
    attention_gain,
    expert_gain,
    position_bias,
    expert_up,
    expert_down,
    routes,
    cotangent,
):
    layers = query_weight.shape[0]
    length, width = tokens.shape
    shards = lax.axis_size("fsdp")
    owners = lax.axis_size("dp")
    experts = owners * EXP_DEV
    heads = position_bias.shape[1] * shards
    capacity = max(2, 9 * length * TOP // (8 * experts))
    fused = shards == 4 and owners == 8 and capacity % 16 == 0 and layers == 2
    taken, pick, both, chosen = plan_routes(routes, experts, capacity)
    offsets = offset_selector(length)

    gathered = []
    for layer in range(layers):
        small = pack_small(
            router_weight[layer], attention_gain[layer], expert_gain[layer], position_bias[layer]
        )
        first = jnp.concatenate(
            [query_weight[layer], key_weight[layer], value_weight[layer], small], axis=1
        )
        first = lax.all_gather(first, "fsdp", axis=0, tiled=True)
        second = lax.all_gather(projection[layer], "fsdp", axis=0, tiled=True)
        gathered.append((first, second))

    early = exchange_rows(low(dot(both, cotangent)), experts)

    hidden = tokens.astype(jnp.float32)
    mixers = []
    saved = []
    for layer in range(layers):
        first, projection_full = gathered[layer]
        if layer:
            hidden, first, projection_full = lax.optimization_barrier(
                (hidden, first, projection_full)
            )
        router, gain_attention, gain_expert, bias = unpack_small(
            first[:, 3 * width :], experts, shards, heads
        )
        gain_attention = gain_attention.astype(jnp.float32)
        gain_expert = gain_expert.astype(jnp.float32)
        table = lax.dot_general(
            bias.astype(jnp.float32), offsets, contract_last, precision=highest
        )
        joined_weight = first[:, : 3 * width]
        mixers.append((joined_weight, projection_full, router, gain_attention, gain_expert, table))
        up_matrix, down_matrix = expert_up[layer, 0], expert_down[layer, 0]
        scale = row_scale(hidden)
        normed = low(hidden * scale * gain_attention)
        joined = low(dot(normed, joined_weight))
        mixed, log_total = attention_forward(joined, table, heads)
        if layer == 0:
            mixed, early = lax.optimization_barrier((mixed, early))
        middle = hidden + dot(mixed, projection_full)
        scale_expert = row_scale(middle)
        normed_expert = low(middle * scale_expert * gain_expert)
        logits = dot(normed_expert, router)
        picked = jnp.sum(jnp.where(chosen, logits[:, None, :], 0.0), axis=-1)
        gates = jax.nn.softmax(picked, axis=-1)
        gate_line = gates.T.reshape(-1)
        sent = low(dot(both, normed_expert))
        slope = None
        if fused and layer < layers - 1:
            returned, received, activity, slope = experts_in_kernel(
                "forward", sent.reshape(experts, capacity, width), up_matrix, down_matrix
            )
            returned = returned.reshape(-1, width)
        elif fused:
            gate_places = jnp.sum(jnp.where(taken, gate_line[None, :], 0.0), axis=1)
            gate_places = gate_places.reshape(experts, 1, capacity)
            gate_places = jnp.pad(gate_places, ((0, 0), (0, 0), (0, -capacity % LANES)))
            back_rows, received, result, back_places, up_change, down_change = (
                experts_in_kernel(
                    "both",
                    sent.reshape(experts, capacity, width),
                    up_matrix,
                    down_matrix,
                    (gate_places, early.reshape(experts, capacity, width)),
                )
            )
            count = experts * capacity
            last = (
                back_places[:, 0, :capacity].reshape(-1),
                up_change,
                down_change,
                back_rows.reshape(count, width),
            )
            activity = None
            returned = exchange_rows(result.reshape(count, width), experts)
        else:
            received = exchange_rows(sent, experts)
            if layer == layers - 1:
                gate_places = exchange_numbers(
                    jnp.sum(jnp.where(taken, gate_line[None, :], 0.0), axis=1), experts
                )
                received, gate_places = lax.optimization_barrier((received, gate_places))
            inner = dot(received, up_matrix)
            activity, slope = smooth_pair(inner)
            activity = low(activity)
            result = low(dot(activity, down_matrix))
            if layer == layers - 1:
                back_places = jnp.sum(early.astype(jnp.float32) * result.astype(jnp.float32), axis=1)
                back_places = exchange_numbers(back_places, experts)
                back_sent = low(gate_places[:, None] * early.astype(jnp.float32))
                back_inner = low(dot_last(back_sent, down_matrix) * slope)
                back_rows, back_sent = lax.optimization_barrier(
                    (low(dot_last(back_inner, up_matrix)), back_sent)
                )
                back_rows = exchange_rows(back_rows, experts)
                last = (back_places, back_sent, back_inner, back_rows)
            returned = exchange_rows(result, experts)
        routed = None
        if layer < layers - 1:
            routed, update = gather_rows(pick, returned, gates)
        saved.append(
            (
                hidden,
                scale,
                normed,
                joined,
                mixed,
                log_total,
                middle,
                scale_expert,
                normed_expert,
                gates,
                received,
                activity,
                slope,
                routed,
            )
        )
        if layer < layers - 1:
            hidden = middle + update

    back_out = cotangent.astype(jnp.float32)
    mixer_results = [None] * layers
    expert_results = [None] * layers
    above = None
    for layer in range(layers - 1, -1, -1):
        joined_weight, projection_full, router, gain_attention, gain_expert, table = mixers[layer]
        up_matrix, down_matrix = expert_up[layer, 0], expert_down[layer, 0]
        (
            hidden,
            scale,
            normed,
            joined,
            mixed,
            log_total,
            middle,
            scale_expert,
            normed_expert,
            gates,
            received,
            activity,
            slope,
            routed,
        ) = saved[layer]
        if layer == layers - 1:
            if fused:
                back_places, up_change, down_change, back_rows = last
            else:
                back_places, back_sent, back_inner, back_rows = last
            back_gates = jnp.sum(jnp.where(taken, back_places[:, None], 0.0), axis=0)
            back_gates = back_gates.reshape(TOP, length).T
        else:
            back_gates = jnp.stack(
                [
                    jnp.sum(back_out * routed[choice].astype(jnp.float32), axis=-1)
                    for choice in range(TOP)
                ],
                axis=1,
            )
            gated = jnp.concatenate(
                [low(gates[:, choice : choice + 1] * back_out) for choice in range(TOP)], axis=0
            )
            back_sent = low(dot(pick, gated))
            up_above, down_above = expert_results[layer + 1]
            if fused:
                back_rows, _, up_change, down_change = experts_in_kernel(
                    "backward",
                    back_sent.reshape(experts, capacity, width),
                    up_matrix,
                    down_matrix,
                    (slope, activity, received),
                )
                back_rows, up_above, above = lax.optimization_barrier(
                    (back_rows, up_above, above)
                )
                back_rows = back_rows.reshape(-1, width)
            else:
                back_sent = exchange_rows(back_sent, experts)
                back_sent, up_above = lax.optimization_barrier((back_sent, up_above))
                back_inner = low(dot_last(back_sent, down_matrix) * slope)
                back_inner, above = lax.optimization_barrier((back_inner, above))
                back_rows, back_sent = lax.optimization_barrier(
                    (low(dot_last(back_inner, up_matrix)), back_sent)
                )
                back_rows = exchange_rows(back_rows, experts)
            expert_results[layer + 1] = (up_above, down_above)
            if not fused:
                mixer_results[layer + 1] = lax.psum(above, "dp")
        if not fused:
            down_change = low(dot_first(activity, back_sent))
            up_change = low(dot_first(received, back_inner))
        shards_of = []
        for change in (up_change, down_change):
            shards_of.append(
                lax.psum_scatter(change, "fsdp", scatter_dimension=0, tiled=True)
            )
        expert_results[layer] = tuple(shards_of)
        if not fused:
            back_rows, down_change, up_change = lax.optimization_barrier(
                (back_rows, down_change, up_change)
            )
        back_picked = gates * (back_gates - jnp.sum(gates * back_gates, axis=-1, keepdims=True))
        back_logits = low(jnp.sum(jnp.where(chosen, back_picked[:, :, None], 0.0), axis=1))
        router_change = dot_first(normed_expert, back_logits)
        back_expert = dot_first(both, back_rows) + dot_last(back_logits, router)
        rows, expert_gain_change = norm_back(middle, scale_expert, gain_expert, back_expert)
        back_middle = back_out + rows
        back_attended = low(back_middle)
        back_mixed = low(dot_last(back_attended, projection_full))
        back_query, back_key, back_value, sums = attention_backward(
            joined, table, log_total, back_mixed, heads
        )
        if layer == layers - 1:
            back_query, returned = lax.optimization_barrier((back_query, returned))
            output = low(middle + gather_rows(pick, returned, gates)[1])
        if layer > 0:
            up_shard, down_shard = expert_results[layer]
            back_query, back_key, back_value, down_shard = lax.optimization_barrier(
                (back_query, back_key, back_value, down_shard)
            )
            expert_results[layer] = (up_shard, down_shard)
        bias_change = jnp.dot(sums, offsets, precision=highest)
        projection_change = dot_first(mixed, back_attended)
        parts = (back_query, back_key, back_value)
        changes = [low(dot_first(normed, part)) for part in parts]
        back_normed = sum(
            dot_last(part, joined_weight[:, index * width : (index + 1) * width])
            for index, part in enumerate(parts)
        )
        rows, attention_gain_change = norm_back(hidden, scale, gain_attention, back_normed)
        back_out = back_middle + rows
        changes = [
            change.reshape(shards, width // shards, width)
            for change in changes + [low(projection_change)]
        ]
        small = jnp.concatenate(
            [
                change.reshape(shards, -1)
                for change in (
                    router_change,
                    attention_gain_change,
                    expert_gain_change,
                    bias_change,
                )
            ],
            axis=1,
        )
        small = low(jnp.pad(small, ((0, 0), (0, -small.shape[1] % (16 * width)))))
        small = small.reshape(shards, -1, width)
        if layer == 0 and fused:
            summed, narrow = reduce_in_kernel(changes, small, above, owners)
        else:
            packed = jnp.concatenate(changes + [small], axis=1)
            above = lax.psum_scatter(packed, "fsdp", scatter_dimension=0)
            if layer == 0:
                mixer_results[layer] = lax.psum(above, "dp")

    rows = width // shards
    counts = (rows * experts, rows, rows, heads // shards * NB)
    if fused:
        mixer_gradients = [summed[index] for index in range(4)]
        flat = narrow.reshape(layers, -1)
    else:
        mixer_results = jnp.stack(lax.optimization_barrier(mixer_results)).astype(jnp.float32)
        mixer_gradients = [
            mixer_results[:, index * rows : (index + 1) * rows] for index in range(4)
        ]
        flat = mixer_results[:, 4 * rows :].reshape(layers, -1)
    ends = [sum(counts[: index + 1]) for index in range(4)]
    small_gradients = [flat[:, end - count : end] for end, count in zip(ends, counts)]
    router_gradient = small_gradients[0].reshape(layers, rows, experts)
    bias_gradient = small_gradients[3].reshape(position_bias.shape)
    up_stack, down_stack = (
        jnp.stack([results[index].astype(jnp.float32) for results in expert_results])[:, None]
        for index in range(2)
    )
    return (
        output,
        back_out,
        *mixer_gradients,
        router_gradient,
        small_gradients[1],
        small_gradients[2],
        bias_gradient,
        up_stack,
        down_stack,
    )


def solution(mesh):
    return jax.shard_map(
        per_device,
        mesh=mesh,
        in_specs=(
            P(("dp", "fsdp"), None),
            P(None, "fsdp", None),
            P(None, "fsdp", None),
            P(None, "fsdp", None),
            P(None, "fsdp", None),
            P(None, "fsdp", None),
            P(None, "fsdp"),
            P(None, "fsdp"),
            P(None, "fsdp", None),
            P(None, "dp", None, None),
            P(None, "dp", None, None),
            P(("dp", "fsdp"), None),
            P(("dp", "fsdp"), None),
        ),
        out_specs=(
            P(("dp", "fsdp"), None),
            P(("dp", "fsdp"), None),
            P(None, "fsdp", None),
            P(None, "fsdp", None),
            P(None, "fsdp", None),
            P(None, "fsdp", None),
            P(None, "fsdp", None),
            P(None, "fsdp"),
            P(None, "fsdp"),
            P(None, "fsdp", None),
            P(None, "dp", "fsdp", None),
            P(None, "dp", "fsdp", None),
        ),
        check_vma=False,
    )
```
